32 devices in a mesh: groups: 2 (over y), dom: 4 (over z), ens: 4 (over x, core).
Axes of the slice: x: 2, y: 2, z: 4, core: 2. Of those that a mesh axis runs over, the one named last changes fastest.
Arguments:
- state: float32 [16, 256, 512], P('ens', ('groups', 'dom')), parts along dimension 1, may hold values from -8 to 8, as said below
- coords: float32 [3, 2048], P(None, ('groups', 'dom')), parts along dimension 1, may hold values from -1 to 1
- owner_local: int32 [2048], P(('groups', 'dom')), parts along dimension 0, may hold values from 0 to 31
- counts: int32 [8, 4], P(('groups', 'dom')), parts along dimension 0, may hold values from 32 to 64, as said below
- obs_value: float32 [2048], P(('groups', 'dom')), parts along dimension 0, may hold values from 0.5 to 3.5
- obs_weight: float32 [2048], P(('groups', 'dom')), parts along dimension 0, as said below
Outputs:
- analysis: float32 [16, 256, 512], P('ens', ('groups', 'dom')), parts along dimension 1
The draws below stay inside these ranges and needn't reach their ends.
There are 2 independent parts, one for each index of `groups`. The reference program is written for one: setup_inputs(seed, part) draws one part's arguments, and reference() takes and returns one part's arrays. A program takes and returns all parts, laid end to end along the dimension named above; each array names one. Nothing has to cross between parts.
Inputs may be any that keep to these rules, and one draw needn't show every extreme that they name: `state`: each member is an independent field plus an offset of its own. The sensors of one block are stored in order of owner block: the first counts[d, 0] slots belong to owner block 0, the next counts[d, 1] to block 1, and so on; slots after the last of them are unused. For one owner block, chosen by the draw, every row holds exactly 64. `obs_weight`: Positive.
All inputs are finite; a program needn't handle non-finite values.
Results may differ from the reference program's by a relative error of at most 0.00028.
Values sent between devices are 32-bit elements; how exact they have to be, the bound alone decides.
No kernel may reach another device: no remote copies, remote signals or barrier semaphores. Data moves between devices by JAX's collectives and lax.ppermute only.
A program may use at most 64 MiB of HBM per device.

```python
import math
import jax
import jax.numpy as jnp
from jax import lax

NODES = 512
MEMBERS = 16
ELEM_DEV = 32
ELEMENTS = 128
CAP = 64
OBS_DEV = 256
OBS_TOTAL = 1024
NS_ITERS = 8
N_DOM = 4


def draw_state(key, part):
    noise_key, offset_key = jax.random.split(jax.random.fold_in(key, 11))
    noise = jnp.clip(jax.random.normal(noise_key, (MEMBERS, ELEMENTS, NODES), jnp.float32), -5.0, 5.0)
    offset = jnp.clip(jax.random.normal(offset_key, (MEMBERS, 1, 1), jnp.float32), -3.0, 3.0)
    return noise + offset


def draw_counts(key, part):
    hot_key, count_key = jax.random.split(jax.random.fold_in(key, 23))
    hot_owner = jax.random.randint(hot_key, (), 0, N_DOM)
    base_counts = jax.random.randint(count_key, (N_DOM, N_DOM), CAP // 2, CAP + 1)
    column = jnp.arange(N_DOM, dtype=jnp.int32)
    return jnp.where(column[None, :] == hot_owner, CAP, base_counts).astype(jnp.int32)


def draw_obs_weight(key, part):
    base_key = jax.random.fold_in(key, 37)
    block_number = jnp.arange(OBS_TOTAL, dtype=jnp.int32) // OBS_DEV
    rising = 1.0 + 2.0 * block_number.astype(jnp.float32) / max(N_DOM - 1, 1)
    scale_value = 50.0 / (N_DOM * (3 * N_DOM + 1) * CAP)
    base_weight = jnp.exp(jax.random.uniform(base_key, (OBS_TOTAL,), jnp.float32, 0.0, math.log(10.0)))
    return (base_weight * rising * scale_value).astype(jnp.float32)


def with_ends(array, key, smallest, top_value):
    longest = array.shape.index(max(array.shape))
    spots = []
    for shift in (0, 1):
        where = [jax.random.randint(jax.random.fold_in(key, axis), (), 0, length) for axis, length in enumerate(array.shape)]
        where[longest] = (where[longest] + shift) % array.shape[longest]
        spots.append(tuple(where))
    return array.at[spots[0]].set(smallest).at[spots[1]].set(top_value)


def shard_levels(own_key, dims, cuts, low, high):
    factor_of, own = 1.0, jax.random.fold_in(own_key, 6)
    for dim, parts in cuts:
        draws = jnp.exp(jax.random.uniform(jax.random.fold_in(own, dim), (parts,), jnp.float32, low / len(cuts), high / len(cuts)))
        factor_of = factor_of * jnp.repeat(draws, dims[dim] // parts).reshape([-1 if axis == dim else 1 for axis in range(len(dims))])
    return factor_of


def setup_inputs(seed: int = 0, part: int = 0) -> dict:
    streams_of = jax.random.split(jax.random.key(seed), 7)
    part_keys = jax.random.split(jax.random.fold_in(streams_of[6], part), 7)
    return {
        "state": draw_state(jax.random.fold_in(jax.random.fold_in(streams_of[6], part), 71), part),
        "coords": jnp.clip(jax.random.uniform(part_keys[1], (3, OBS_TOTAL), jnp.float32, -1.0, 1.0) * shard_levels(part_keys[1], (3, OBS_TOTAL), ((1, 4),), -0.4, 0.0), -1.0, 1.0),
        "owner_local": with_ends(jax.random.randint(part_keys[2], (OBS_TOTAL,), 0, ELEM_DEV), jax.random.fold_in(part_keys[2], 1), 0, ELEM_DEV - 1).astype(jnp.int32),
        "counts": draw_counts(jax.random.fold_in(jax.random.fold_in(streams_of[6], part), 71), part),
        "obs_value": jnp.clip(0.5 + 3.0 * jax.random.uniform(part_keys[4], (OBS_TOTAL,), jnp.float32) ** shard_levels(part_keys[4], (OBS_TOTAL,), ((0, 4),), -0.2, 0.2), 0.5, 3.5),
        "obs_weight": draw_obs_weight(jax.random.fold_in(jax.random.fold_in(streams_of[6], part), 71), part),
    }


GLL_POINTS = (-1.0, -0.8717401485096066, -0.5917001814331423, -0.2092992179024789, 0.2092992179024789, 0.5917001814331423, 0.8717401485096066, 1.0)
INFLATION = 1.1

def lagrange(position):
    basis_rows = []
    for node_index in range(8):
        product = jnp.ones_like(position)
        for other_node in range(8):
            if other_node != node_index:
                product = product * (position - GLL_POINTS[other_node]) / (GLL_POINTS[node_index] - GLL_POINTS[other_node])
        basis_rows.append(product)
    return jnp.stack(basis_rows, 0)

def node_weights(sensor_coords):
    along_r = lagrange(sensor_coords[0]).T
    along_s = lagrange(sensor_coords[1]).T
    along_t = lagrange(sensor_coords[2]).T
    node_table = along_t[:, :, None, None] * along_s[:, None, :, None] * along_r[:, None, None, :]
    return node_table.reshape(sensor_coords.shape[1], 512)

def analysis_weights(cross_terms, project):
    highest = lax.Precision.HIGHEST
    members = cross_terms.shape[0]
    identity = jnp.eye(members, dtype=jnp.float32)
    system = cross_terms + (members - 1) / INFLATION * identity
    trace_value = jnp.trace(system)
    iterate = system / trace_value
    inverse_root = identity
    for sweep in range(NS_ITERS):
        middle = 0.5 * (3.0 * identity - jnp.dot(inverse_root, iterate, precision=highest))
        iterate = jnp.dot(iterate, middle, precision=highest)
        inverse_root = jnp.dot(middle, inverse_root, precision=highest)
    mean_weights = jnp.dot(inverse_root, jnp.dot(inverse_root, project, precision=highest), precision=highest) / trace_value
    transform = inverse_root * jnp.sqrt((members - 1) / trace_value) + mean_weights[:, None]
    return transform - lax.optimization_barrier(jnp.mean(transform, axis=0, keepdims=True)) + 1.0 / members

def reference(state, coords, owner_local, counts, obs_value, obs_weight):
    highest = lax.Precision.HIGHEST
    members = state.shape[0]
    segment_ends = jnp.cumsum(counts, axis=1)
    slot_index = jnp.arange(OBS_DEV, dtype=jnp.int32)
    destination = lax.optimization_barrier(jnp.sum((slot_index[None, :, None] >= segment_ends[:, None, :]).astype(jnp.int32), axis=2))
    in_use = destination < N_DOM
    element = jnp.minimum(destination, N_DOM - 1) * ELEM_DEV + owner_local.reshape(N_DOM, OBS_DEV)
    used_weight = jnp.where(in_use.reshape(-1), obs_weight, jnp.zeros_like(obs_weight))

    def interpolate(inputs):
        block_coords, block_element = inputs
        node_table = node_weights(block_coords)
        element_rows = jnp.take(state, block_element, axis=1)
        return jnp.einsum('sn,ksn->ks', node_table, element_rows, precision=highest)
    block_coords = coords.reshape(3, N_DOM, OBS_DEV).transpose(1, 0, 2)
    model_value = lax.map(interpolate, (block_coords, element))
    model_value = model_value.transpose(1, 0, 2).reshape(members, N_DOM * OBS_DEV)
    mean_value = lax.optimization_barrier(jnp.mean(model_value, axis=0))
    anomaly = model_value - mean_value[None, :]
    weighted = anomaly * used_weight[None, :]
    cross_terms = jnp.dot(weighted, anomaly.T, precision=highest)
    project = jnp.dot(weighted, obs_value - mean_value, precision=highest)
    mixing = analysis_weights(cross_terms, project)
    flat_state = state.reshape(members, -1)
    return jnp.dot(mixing.T, flat_state, precision=highest).reshape(state.shape)
```

```python
import jax
import jax.numpy as jnp
from jax import lax
from jax.experimental import pallas as pl
from jax.experimental.pallas import tpu as pltpu
from jax.sharding import PartitionSpec as P

CAP = 64
NS_ITERS = 8


GLL_POINTS = (
    -1.0,
    -0.8717401485096066,
    -0.5917001814331423,
    -0.2092992179024789,
    0.2092992179024789,
    0.5917001814331423,
    0.8717401485096066,
    1.0,
)
INFLATION = 1.1
ORDER = len(GLL_POINTS)
F32 = jnp.float32
BF16 = jnp.bfloat16
DIRECT_DOM = 8


def lagrange_scale(index):
    product = 1.0
    for other in range(ORDER):
        if other != index:
            product *= GLL_POINTS[index] - GLL_POINTS[other]
    return 1.0 / product


def lagrange_rows(position):
    shape = (ORDER, position.shape[1])
    node = lax.broadcasted_iota(jnp.int32, shape, 0)
    product = jnp.full(shape, lagrange_scale(0), F32)
    for index in range(1, ORDER):
        product = jnp.where(node == index, lagrange_scale(index), product)
    for other in range(ORDER):
        product = product * jnp.where(node == other, 1.0, position - GLL_POINTS[other])
    return product


def split(value):
    high = value.astype(BF16)
    low = (value - high.astype(F32)).astype(BF16)
    return high, low


def pack_kernel(direct, counts, coords, owner, obs, weight, *rest):
    outs, block = rest[:-1], rest[-1]
    n_dom = counts.shape[1]
    slots = coords.shape[1]
    here = lax.axis_index("dom")
    block[...] = jnp.zeros(block.shape, F32)
    block[0:3, :] = coords[...]
    block[3:4, :] = owner[...].astype(F32)
    block[4:5, :] = obs[...]
    block[5:6, :] = weight[...]
    rows = block[...]
    column = lax.broadcasted_iota(jnp.int32, (8, 2 * CAP), 1)

    def tile(target, half):
        start = jnp.int32(0)
        for other in range(n_dom):
            start = start + jnp.where(other < target, counts[0, other], 0)
        count = counts[0, target]
        turned = pltpu.roll(rows, lax.rem(half - start + slots, slots), axis=1)[:, : 2 * CAP]
        return jnp.where((column >= half) & (column < half + count), turned, 0.0)

    if direct:
        for shift in range(n_dom):
            outs[shift][...] = tile(lax.rem(here + shift, n_dom), (shift % 2) * CAP)
    else:
        half = lax.rem(here, 2) * CAP

        def step(target, carry):
            outs[0][target] = tile(target, half)
            return carry

        lax.fori_loop(0, n_dom, step, 0)


def pick(state_rows, members, elements, high, low, chosen):
    rows_high, rows_low = split(state_rows)
    partial = (
        jnp.dot(rows_high, high, preferred_element_type=F32)
        + jnp.dot(rows_low, high, preferred_element_type=F32)
        + jnp.dot(rows_high, low, preferred_element_type=F32)
    )
    partial = partial.reshape(members, elements, partial.shape[1])
    return jnp.sum(jnp.where(chosen[None], partial, 0.0), axis=1)


def chosen_mask(sensors, elements):
    ids = lax.broadcasted_iota(jnp.int32, (elements, sensors.shape[1]), 0).astype(F32)
    return ids == sensors[3:4, :]


def values_kernel(tile_count, *refs):
    tiles, state_refs = refs[:tile_count], refs[tile_count:-4]
    sensors_out, high_out, low_out, values_out = refs[-4:]
    pairs = []
    for first in range(0, tile_count, 2):
        pair = tiles[first][...]
        if first + 1 < tile_count:
            pair = pair + tiles[first + 1][...]
        pairs.append(pair)
    sensors = jnp.concatenate(pairs, axis=1) if len(pairs) > 1 else pairs[0]
    sensors_out[...] = sensors
    along_r = lagrange_rows(sensors[0:1, :])
    along_s = lagrange_rows(sensors[1:2, :])
    along_t = lagrange_rows(sensors[2:3, :])
    for t in range(ORDER):
        for s in range(0, ORDER, 2):
            rows = [along_r * (along_t[t : t + 1, :] * along_s[k : k + 1, :]) for k in (s, s + 1)]
            high, low = split(jnp.concatenate(rows, axis=0))
            base = ORDER * ORDER * t + ORDER * s
            high_out[base : base + 2 * ORDER, :] = high
            low_out[base : base + 2 * ORDER, :] = low
    high, low = high_out[...], low_out[...]
    for index, ref in enumerate(state_refs):
        members, elements, nodes = ref.shape
        chosen = chosen_mask(sensors, elements)
        rows = ref[...].reshape(members * elements, nodes)
        values_out[index * members : (index + 1) * members, :] = pick(
            rows, members, elements, high, low, chosen
        )


def cross_kernel(sensors_ref, high_ref, low_ref, values_ref, *refs):
    state_refs, out = refs[:-1], refs[-1]
    high, low = high_ref[...], low_ref[...]
    sensors = sensors_ref[...]
    parts = [values_ref[...]]
    for ref in state_refs:
        members, elements, nodes = ref.shape
        chosen = chosen_mask(sensors, elements)
        rows = ref[...].reshape(members * elements, nodes)
        parts.append(pick(rows, members, elements, high, low, chosen))
    values = jnp.concatenate(parts, axis=0)
    total = values.shape[0]
    mean_value = jnp.sum(values, axis=0, keepdims=True) * (1.0 / total)
    anomaly = values - mean_value
    weighted = anomaly * sensors[5:6, :]
    innovation = sensors[4:5, :] - mean_value
    pad = jnp.zeros((out.shape[1] - total - 1, values.shape[1]), F32)
    right = jnp.concatenate([anomaly, innovation, pad], axis=0)
    out[...] = lax.dot_general(
        weighted,
        right,
        (((1,), (1,)), ((), ())),
        precision=lax.Precision.HIGHEST,
        preferred_element_type=F32,
    )


def mix_kernel(sum_count, *refs):
    sums, state_refs, out, splats = refs[:sum_count], refs[sum_count:-2], refs[-2], refs[-1]
    highest = lax.Precision.HIGHEST
    total_sum = sums[0][...]
    for ref in sums[1:]:
        total_sum = total_sum + ref[...]
    local_members, elements, nodes = out.shape
    members = local_members * len(state_refs)
    row = lax.broadcasted_iota(jnp.int32, (members, members), 0)
    col = lax.broadcasted_iota(jnp.int32, (members, members), 1)
    identity = (row == col).astype(F32)
    system = total_sum[:, :members] + (members - 1) / INFLATION * identity
    project = total_sum[:, members : members + 1]
    trace_value = jnp.sum(
        jnp.sum(jnp.where(row == col, system, 0.0), axis=1, keepdims=True), axis=0, keepdims=True
    )
    iterate = system / trace_value
    inverse_root = identity
    for sweep in range(NS_ITERS):
        if sweep:
            product = jnp.dot(inverse_root, iterate, precision=highest)
        else:
            product = iterate
        middle = 0.5 * (3.0 * identity - product)
        if sweep + 1 < NS_ITERS:
            iterate = jnp.dot(iterate, middle, precision=highest)
        inverse_root = jnp.dot(middle, inverse_root, precision=highest) if sweep else middle
    mean_weights = (
        jnp.dot(inverse_root, jnp.dot(inverse_root, project, precision=highest), precision=highest)
        / trace_value
    )
    transform = inverse_root * jnp.sqrt((members - 1) / trace_value) + mean_weights
    mixing = transform - jnp.mean(transform, axis=0, keepdims=True) + 1.0 / members
    for j in range(members):
        for k in range(local_members):
            splats[j * local_members + k] = jnp.broadcast_to(mixing[j : j + 1, k : k + 1], (8, 128))
    for block in range(elements // 8):
        span = slice(8 * block, 8 * block + 8)
        for lane in range(nodes // 128):
            lanes = slice(128 * lane, 128 * lane + 128)
            totals = [None] * local_members
            for j in range(members):
                value = state_refs[j // local_members][j % local_members, span, lanes]
                for k in range(local_members):
                    term = splats[j * local_members + k] * value
                    totals[k] = term if totals[k] is None else totals[k] + term
            for k in range(local_members):
                out[k, span, lanes] = totals[k]


def exchange(value, axis, pairs):
    return lax.ppermute(value, axis, pairs)


def gather_members(state, n_ens):
    pieces = {0: state}
    if n_ens & (n_ens - 1) == 0:
        bit = n_ens >> 1
        while bit:
            pairs = [(e, e ^ bit) for e in range(n_ens)]
            for key in list(pieces):
                pieces[key ^ bit] = exchange(pieces[key], "ens", pairs)
            bit >>= 1
    else:
        for shift in range(1, n_ens):
            pairs = [(e, (e + shift) % n_ens) for e in range(n_ens)]
            pieces[shift] = exchange(state, "ens", pairs)
    return [pieces[key] for key in sorted(pieces)]


def make_on_device(n_dom, n_ens):
    vmem = pl.BlockSpec(memory_space=pltpu.VMEM)
    smem = pl.BlockSpec(memory_space=pltpu.SMEM)
    direct = n_dom <= DIRECT_DOM

    def call(kernel, name, out_shape, operands, specs=None, scratch=()):
        many = isinstance(out_shape, (list, tuple))
        return pl.pallas_call(
            kernel,
            name=name,
            out_shape=out_shape,
            in_specs=specs or [vmem] * len(operands),
            out_specs=[vmem] * len(out_shape) if many else vmem,
            scratch_shapes=list(scratch),
        )(*operands)

    def shape(dims, dtype=F32):
        return jax.ShapeDtypeStruct(dims, dtype)

    def on_device(state, coords, owner_local, counts, obs_value, obs_weight):
        local_members, elements, nodes = state.shape
        slots = coords.shape[1]
        members = local_members * n_ens
        pieces = gather_members(state, n_ens)
        tile_shape = (8, 2 * CAP)
        tiles = list(call(
            lambda *refs: pack_kernel(direct, *refs),
            "pack",
            [shape(tile_shape)] * n_dom if direct else [shape((n_dom,) + tile_shape)],
            [counts, coords, owner_local[None], obs_value[None], obs_weight[None]],
            [smem] + [vmem] * 4,
            [pltpu.VMEM((8, slots), F32)],
        ))
        if direct:
            for shift in range(1, n_dom):
                pairs = [(d, (d + shift) % n_dom) for d in range(n_dom)]
                tiles[shift] = exchange(tiles[shift], "dom", pairs)
        else:
            moved = lax.all_to_all(tiles[0], "dom", split_axis=0, concat_axis=0, tiled=True)
            tiles = [moved[d] for d in range(n_dom)]
        sensor_count = CAP * (n_dom + n_dom % 2)
        early = max(1, n_ens // 2)
        sensors, high, low, values = call(
            lambda *refs: values_kernel(n_dom, *refs),
            "values",
            [
                shape((8, sensor_count)),
                shape((nodes, sensor_count), BF16),
                shape((nodes, sensor_count), BF16),
                shape((early * local_members, sensor_count)),
            ],
            list(tiles) + pieces[:early],
        )
        partial_sum = call(
            cross_kernel,
            "cross",
            shape((members, members + 8)),
            [sensors, high, low, values] + pieces[early:],
        )
        if direct:
            sums = [partial_sum]
            for shift in range(1, n_dom):
                pairs = [(d, (d + shift) % n_dom) for d in range(n_dom)]
                sums.append(exchange(partial_sum, "dom", pairs))
        else:
            sums = [lax.psum(partial_sum, "dom")]
        return call(
            lambda *refs: mix_kernel(len(sums), *refs),
            "mix",
            shape(state.shape),
            sums + pieces,
            None,
            [pltpu.VMEM((members * local_members, 8, 128), F32)],
        )

    return on_device


def solution(mesh):
    return jax.shard_map(
        make_on_device(mesh.shape["dom"], mesh.shape["ens"]),
        mesh=mesh,
        in_specs=(
            P("ens", ("groups", "dom"), None),
            P(None, ("groups", "dom")),
            P(("groups", "dom")),
            P(("groups", "dom"), None),
            P(("groups", "dom")),
            P(("groups", "dom")),
        ),
        out_specs=P("ens", ("groups", "dom"), None),
        check_vma=False,
    )
```

```python
import jax
import jax.numpy as jnp
from jax import lax
from jax.experimental import pallas as pl
from jax.experimental.pallas import tpu as pltpu
from jax.sharding import PartitionSpec as P

CAP = 64
NS_ITERS = 8


GLL_POINTS = (
    -1.0,
    -0.8717401485096066,
    -0.5917001814331423,
    -0.2092992179024789,
    0.2092992179024789,
    0.5917001814331423,
    0.8717401485096066,
    1.0,
)
INFLATION = 1.1
ORDER = len(GLL_POINTS)
F32 = jnp.float32
BF16 = jnp.bfloat16
DIRECT_DOM = 8
VMEM_LIMIT = 8 * 1024 * 1024


def lagrange_scale(index):
    product = 1.0
    for other in range(ORDER):
        if other != index:
            product *= GLL_POINTS[index] - GLL_POINTS[other]
    return 1.0 / product


def lagrange_rows(position):
    shape = (ORDER, position.shape[1])
    node = lax.broadcasted_iota(jnp.int32, shape, 0)
    product = jnp.full(shape, lagrange_scale(0), F32)
    for index in range(1, ORDER):
        product = jnp.where(node == index, lagrange_scale(index), product)
    for other in range(ORDER):
        product = product * jnp.where(node == other, 1.0, position - GLL_POINTS[other])
    return product


def split(value):
    high = value.astype(BF16)
    low = (value - high.astype(F32)).astype(BF16)
    return high, low


def pack_kernel(direct, paired, counts, coords, owner, obs, weight, *rest):
    outs, block = rest[:-1], rest[-1]
    n_dom = counts.shape[1]
    slots = coords.shape[1]
    here = lax.axis_index("dom")
    block[...] = jnp.zeros(block.shape, F32)
    block[0:3, :] = coords[...]
    block[3:4, :] = owner[...].astype(F32)
    block[4:5, :] = obs[...]
    block[5:6, :] = weight[...]
    rows = block[...]
    column = lax.broadcasted_iota(jnp.int32, (8, 2 * CAP), 1)

    def tile(target, half):
        start = jnp.int32(0)
        for other in range(n_dom):
            start = start + jnp.where(other < target, counts[0, other], 0)
        count = counts[0, target]
        turned = pltpu.roll(rows, lax.rem(half - start + slots, slots), axis=1)[:, : 2 * CAP]
        return jnp.where((column >= half) & (column < half + count), turned, 0.0)

    if paired:
        near = jnp.where(lax.rem(lax.axis_index("ens"), 2) == 0, 1, 3)
        for out, shift, half in zip(outs, (0, near, 2), (0, CAP, 0)):
            out[...] = tile(lax.rem(here + shift, n_dom), half)
    elif direct:
        for shift in range(n_dom):
            outs[shift][...] = tile(lax.rem(here + shift, n_dom), (shift % 2) * CAP)
    else:
        half = lax.rem(here, 2) * CAP

        def step(target, carry):
            outs[0][target] = tile(target, half)
            return carry

        lax.fori_loop(0, n_dom, step, 0)


def pick(state_rows, members, elements, high, low, chosen):
    rows_high, rows_low = split(state_rows)
    partial = (
        jnp.dot(rows_high, high, preferred_element_type=F32)
        + jnp.dot(rows_low, high, preferred_element_type=F32)
        + jnp.dot(rows_high, low, preferred_element_type=F32)
    )
    partial = partial.reshape(members, elements, partial.shape[1])
    return jnp.sum(jnp.where(chosen[None], partial, 0.0), axis=1)


def chosen_mask(sensors, elements):
    ids = lax.broadcasted_iota(jnp.int32, (elements, sensors.shape[1]), 0).astype(F32)
    return ids == sensors[3:4, :]


def values_kernel(tile_count, *refs):
    tiles, state_refs = refs[:tile_count], refs[tile_count:-4]
    sensors_out, high_out, low_out, values_out = refs[-4:]
    pairs = []
    for first in range(0, tile_count, 2):
        pair = tiles[first][...]
        if first + 1 < tile_count:
            pair = pair + tiles[first + 1][...]
        pairs.append(pair)
    sensors = jnp.concatenate(pairs, axis=1) if len(pairs) > 1 else pairs[0]
    sensors_out[...] = sensors
    along_r = lagrange_rows(sensors[0:1, :])
    along_s = lagrange_rows(sensors[1:2, :])
    along_t = lagrange_rows(sensors[2:3, :])
    for t in range(ORDER):
        for s in range(0, ORDER, 2):
            rows = [along_r * (along_t[t : t + 1, :] * along_s[k : k + 1, :]) for k in (s, s + 1)]
            high, low = split(jnp.concatenate(rows, axis=0))
            base = ORDER * ORDER * t + ORDER * s
            high_out[base : base + 2 * ORDER, :] = high
            low_out[base : base + 2 * ORDER, :] = low
    high, low = high_out[...], low_out[...]
    for index, ref in enumerate(state_refs):
        members, elements, nodes = ref.shape
        chosen = chosen_mask(sensors, elements)
        rows = ref[...].reshape(members * elements, nodes)
        values_out[index * members : (index + 1) * members, :] = pick(
            rows, members, elements, high, low, chosen
        )


def is_odd(paired):
    return lax.rem(lax.axis_index("ens"), 2) if paired else 0


def cross_kernel(paired, sensors_ref, high_ref, low_ref, values_ref, *refs):
    state_refs, out = refs[:-1], refs[-1]
    high, low = high_ref[...], low_ref[...]
    sensors = sensors_ref[...]
    parts = [values_ref[...]]
    for ref in state_refs:
        members, elements, nodes = ref.shape
        chosen = chosen_mask(sensors, elements)
        rows = ref[...].reshape(members * elements, nodes)
        parts.append(pick(rows, members, elements, high, low, chosen))
    values = jnp.concatenate(parts, axis=0)
    total = values.shape[0]
    if paired:
        size = total // (len(parts) + 1)
        blocks = [values[first : first + size] for first in range(0, total, size)]
        turned = [blocks[index ^ 1] for index in range(len(blocks))]
        values = jnp.where(is_odd(paired) == 1, jnp.concatenate(turned, axis=0), values)
    mean_value = jnp.sum(values, axis=0, keepdims=True) * (1.0 / total)
    anomaly = values - mean_value
    weighted = anomaly * sensors[5:6, :]
    innovation = sensors[4:5, :] - mean_value
    pad = jnp.zeros((out.shape[1] - total - 1, values.shape[1]), F32)
    right = jnp.concatenate([anomaly, innovation, pad], axis=0)
    out[...] = lax.dot_general(
        weighted,
        right,
        (((1,), (1,)), ((), ())),
        precision=lax.Precision.HIGHEST,
        preferred_element_type=F32,
    )


def mix_kernel(paired, sum_count, *refs):
    sums, state_refs, out, splats = refs[:sum_count], refs[sum_count:-2], refs[-2], refs[-1]
    highest = lax.Precision.HIGHEST
    total_sum = sums[0][...]
    for ref in sums[1:]:
        total_sum = total_sum + ref[...]
    local_members, elements, nodes = out.shape
    members = local_members * len(state_refs)
    row = lax.broadcasted_iota(jnp.int32, (members, members), 0)
    col = lax.broadcasted_iota(jnp.int32, (members, members), 1)
    identity = (row == col).astype(F32)
    system = total_sum[:, :members] + (members - 1) / INFLATION * identity
    project = total_sum[:, members : members + 1]
    trace_value = jnp.sum(
        jnp.sum(jnp.where(row == col, system, 0.0), axis=1, keepdims=True), axis=0, keepdims=True
    )
    iterate = system / trace_value
    inverse_root = identity
    for sweep in range(NS_ITERS):
        if sweep:
            product = jnp.dot(inverse_root, iterate, precision=highest)
        else:
            product = iterate
        middle = 0.5 * (3.0 * identity - product)
        if sweep + 1 < NS_ITERS:
            iterate = jnp.dot(iterate, middle, precision=highest)
        inverse_root = jnp.dot(middle, inverse_root, precision=highest) if sweep else middle
    mean_weights = (
        jnp.dot(inverse_root, jnp.dot(inverse_root, project, precision=highest), precision=highest)
        / trace_value
    )
    transform = inverse_root * jnp.sqrt((members - 1) / trace_value) + mean_weights
    mixing = transform - jnp.mean(transform, axis=0, keepdims=True) + 1.0 / members
    odd = is_odd(paired)
    if paired:
        mixing = jnp.where(
            odd == 1, mixing[:, local_members : 2 * local_members], mixing[:, :local_members]
        )
    for j in range(members):
        for k in range(local_members):
            splats[j * local_members + k] = jnp.broadcast_to(mixing[j : j + 1, k : k + 1], (8, 128))
    for block in range(elements // 8):
        span = slice(8 * block, 8 * block + 8)
        for lane in range(nodes // 128):
            lanes = slice(128 * lane, 128 * lane + 128)
            totals = [None] * local_members
            for j in range(members):
                piece, member = divmod(j, local_members)
                value = state_refs[piece][member, span, lanes]
                place = piece + odd * (1 - 2 * (piece % 2))
                for k in range(local_members):
                    term = splats[(place * local_members + member) * local_members + k] * value
                    totals[k] = term if totals[k] is None else totals[k] + term
            for k in range(local_members):
                out[k, span, lanes] = totals[k]


def exchange(value, axis, pairs):
    return lax.ppermute(value, axis, pairs)


def shifted(value, n_dom, shift):
    return exchange(value, "dom", [(d, (d + shift) % n_dom) for d in range(n_dom)])


def swapped(value, n_ens):
    return exchange(value, "ens", [(e, e ^ 1) for e in range(n_ens)])


def is_paired(n_dom, n_ens):
    return n_dom == 4 and n_ens % 2 == 0


def spread(values, n_dom, n_ens):
    if not is_paired(n_dom, n_ens):
        return [values[0]] + [shifted(values[s], n_dom, s) for s in range(1, n_dom)]
    here, near, far = values
    pairs = []
    for d in range(n_dom):
        for e in range(n_ens):
            target = (d + (3 if e % 2 else 1)) % n_dom
            pairs.append((d * n_ens + e, target * n_ens + e))
    near = exchange(near, ("dom", "ens"), pairs)
    far = shifted(far, n_dom, 2)
    return [here, near, far, swapped(near, n_ens)]


def gather_early(state, n_ens):
    pieces = {0: state}
    if n_ens & (n_ens - 1) == 0:
        for bit in {1, n_ens >> 1} - {0}:
            pieces[bit] = exchange(state, "ens", [(e, e ^ bit) for e in range(n_ens)])
    else:
        for shift in range(1, n_ens):
            pairs = [(e, (e + shift) % n_ens) for e in range(n_ens)]
            pieces[shift] = exchange(state, "ens", pairs)
    return pieces


def gather_late(pieces, n_ens, after):
    bit = n_ens >> 2
    while bit and len(pieces) < n_ens:
        for key in list(pieces):
            if key ^ bit not in pieces:
                source = lax.optimization_barrier((pieces[key], after))[0]
                pieces[key ^ bit] = exchange(source, "ens", [(e, e ^ bit) for e in range(n_ens)])
        bit >>= 1
    return pieces


def make_on_device(n_dom, n_ens):
    vmem = pl.BlockSpec(memory_space=pltpu.VMEM)
    smem = pl.BlockSpec(memory_space=pltpu.SMEM)
    direct = n_dom <= DIRECT_DOM
    paired = is_paired(n_dom, n_ens)
    limit = VMEM_LIMIT if direct else None

    def call(kernel, name, out_shape, operands, specs=None, scratch=()):
        many = isinstance(out_shape, (list, tuple))
        return pl.pallas_call(
            kernel,
            name=name,
            out_shape=out_shape,
            in_specs=specs or [vmem] * len(operands),
            out_specs=[vmem] * len(out_shape) if many else vmem,
            scratch_shapes=list(scratch),
            compiler_params=pltpu.CompilerParams(vmem_limit_bytes=limit),
        )(*operands)

    def shape(dims, dtype=F32):
        return jax.ShapeDtypeStruct(dims, dtype)

    def on_device(state, coords, owner_local, counts, obs_value, obs_weight):
        local_members, elements, nodes = state.shape
        slots = coords.shape[1]
        members = local_members * n_ens
        tile_shape = (8, 2 * CAP)
        tiles = list(call(
            lambda *refs: pack_kernel(direct, paired, *refs),
            "pack",
            [shape(tile_shape)] * (3 if paired else n_dom)
            if direct
            else [shape((n_dom,) + tile_shape)],
            [counts, coords, owner_local[None], obs_value[None], obs_weight[None]],
            [smem] + [vmem] * 4,
            [pltpu.VMEM((8, slots), F32)],
        ))
        if direct:
            tiles = spread(tiles, n_dom, n_ens)
        else:
            moved = lax.all_to_all(tiles[0], "dom", split_axis=0, concat_axis=0, tiled=True)
            tiles = [moved[d] for d in range(n_dom)]
        pieces = gather_early(state, n_ens)
        sensor_count = CAP * (n_dom + n_dom % 2)
        early = min(2, n_ens)
        sensors, high, low, values = call(
            lambda *refs: values_kernel(n_dom, *refs),
            "values",
            [
                shape((8, sensor_count)),
                shape((nodes, sensor_count), BF16),
                shape((nodes, sensor_count), BF16),
                shape((early * local_members, sensor_count)),
            ],
            list(tiles) + [pieces[key] for key in range(early)],
        )
        pieces = gather_late(pieces, n_ens, sensors)
        pieces = [pieces[key] for key in range(n_ens)]
        partial_sum = call(
            lambda *refs: cross_kernel(paired, *refs),
            "cross",
            shape((members, members + 8)),
            [sensors, high, low, values] + pieces[early:],
        )
        if direct:
            sums = spread([partial_sum] * (3 if paired else n_dom), n_dom, n_ens)
        else:
            sums = [lax.psum(partial_sum, "dom")]
        return call(
            lambda *refs: mix_kernel(paired, len(sums), *refs),
            "mix",
            shape(state.shape),
            sums + pieces,
            None,
            [pltpu.VMEM((members * local_members, 8, 128), F32)],
        )

    return on_device


def solution(mesh):
    return jax.shard_map(
        make_on_device(mesh.shape["dom"], mesh.shape["ens"]),
        mesh=mesh,
        in_specs=(
            P("ens", ("groups", "dom"), None),
            P(None, ("groups", "dom")),
            P(("groups", "dom")),
            P(("groups", "dom"), None),
            P(("groups", "dom")),
            P(("groups", "dom")),
        ),
        out_specs=P("ens", ("groups", "dom"), None),
        check_vma=False,
    )
```

```python
import jax
import jax.numpy as jnp
from jax import lax
from jax.experimental import pallas as pl
from jax.experimental.pallas import tpu as pltpu
from jax.sharding import PartitionSpec as P


CAP = 64
NS_ITERS = 8


GLL_POINTS = (
    -1.0,
    -0.8717401485096066,
    -0.5917001814331423,
    -0.2092992179024789,
    0.2092992179024789,
    0.5917001814331423,
    0.8717401485096066,
    1.0,
)
INFLATION = 1.1
ORDER = len(GLL_POINTS)
F32 = jnp.float32
BF16 = jnp.bfloat16
DIRECT_DOM = 8
VMEM_LIMIT = 8 * 1024 * 1024


def lagrange_scale(index):
    product = 1.0
    for other in range(ORDER):
        if other != index:
            product *= GLL_POINTS[index] - GLL_POINTS[other]
    return 1.0 / product


def lagrange_rows(position):
    shape = (ORDER, position.shape[1])
    node = lax.broadcasted_iota(jnp.int32, shape, 0)
    product = jnp.full(shape, lagrange_scale(0), F32)
    for index in range(1, ORDER):
        product = jnp.where(node == index, lagrange_scale(index), product)
    for other in range(ORDER):
        product = product * jnp.where(node == other, 1.0, position - GLL_POINTS[other])
    return product


def split(value):
    high = value.astype(BF16)
    low = (value - high.astype(F32)).astype(BF16)
    return high, low


def is_odd(paired):
    return lax.rem(lax.axis_index("ens"), 2) if paired else 0


def pack_kernel(direct, paired, state, counts, coords, owner, obs, weight, *rest):
    own, outs = rest[0], rest[1:-8]
    count_box, coord_box, owner_box, obs_box, weight_box, block, state_sem, sems = rest[-8:]
    state_copy = pltpu.make_async_copy(state, own, state_sem)
    pairs = zip(
        (counts, coords, owner, obs, weight), (count_box, coord_box, owner_box, obs_box, weight_box)
    )
    copies = [
        pltpu.make_async_copy(source, target, sems.at[index])
        for index, (source, target) in enumerate(pairs)
    ]
    for copy in copies:
        copy.start()
    state_copy.start()
    n_dom = counts.shape[1]
    slots = coords.shape[1]
    here = lax.axis_index("dom")
    block[...] = jnp.zeros(block.shape, F32)
    column = lax.broadcasted_iota(jnp.int32, (8, 2 * CAP), 1)
    for copy in copies:
        copy.wait()
    block[0:3, :] = coord_box[...]
    block[3:4, :] = owner_box[...].astype(F32)
    block[4:5, :] = obs_box[...]
    block[5:6, :] = weight_box[...]
    rows = block[...]

    def tile(target, half):
        start = jnp.int32(0)
        for other in range(n_dom):
            start = start + jnp.where(other < target, count_box[0, other], 0)
        count = count_box[0, target]
        turned = pltpu.roll(rows, lax.rem(half - start + slots, slots), axis=1)[:, : 2 * CAP]
        return jnp.where((column >= half) & (column < half + count), turned, 0.0)

    if paired:
        near = jnp.where(is_odd(paired) == 0, 1, 3)
        for out, bits, half in zip(outs, (0, near, 2), (0, CAP, 0)):
            out[...] = tile(jnp.bitwise_xor(here, bits), half)
    elif direct:
        for shift in range(n_dom):
            outs[shift][...] = tile(lax.rem(here + shift, n_dom), (shift % 2) * CAP)
    else:
        half = lax.rem(here, 2) * CAP

        def step(target, carry):
            outs[0][target] = tile(target, half)
            return carry

        lax.fori_loop(0, n_dom, step, 0)
    state_copy.wait()


def pick(state_rows, members, elements, high, low, chosen):
    rows_high, rows_low = split(state_rows)
    partial = (
        jnp.dot(rows_high, high, preferred_element_type=F32)
        + jnp.dot(rows_low, high, preferred_element_type=F32)
        + jnp.dot(rows_high, low, preferred_element_type=F32)
    )
    partial = partial.reshape(members, elements, partial.shape[1])
    return jnp.sum(jnp.where(chosen[None], partial, 0.0), axis=1)


def chosen_mask(sensors, elements):
    ids = lax.broadcasted_iota(jnp.int32, (elements, sensors.shape[1]), 0).astype(F32)
    return ids == sensors[3:4, :]


def values_kernel(tile_count, *refs):
    tiles, state_refs = refs[:tile_count], refs[tile_count:-4]
    sensors_out, high_out, low_out, values_out = refs[-4:]
    pairs = []
    for first in range(0, tile_count, 2):
        pair = tiles[first][...]
        if first + 1 < tile_count:
            pair = pair + tiles[first + 1][...]
        pairs.append(pair)
    sensors = jnp.concatenate(pairs, axis=1) if len(pairs) > 1 else pairs[0]
    sensors_out[...] = sensors
    along_r = lagrange_rows(sensors[0:1, :])
    along_s = lagrange_rows(sensors[1:2, :])
    along_t = lagrange_rows(sensors[2:3, :])
    for t in range(ORDER):
        for s in range(0, ORDER, 2):
            rows = [along_r * (along_t[t : t + 1, :] * along_s[k : k + 1, :]) for k in (s, s + 1)]
            high, low = split(jnp.concatenate(rows, axis=0))
            base = ORDER * ORDER * t + ORDER * s
            high_out[base : base + 2 * ORDER, :] = high
            low_out[base : base + 2 * ORDER, :] = low
    high, low = high_out[...], low_out[...]
    for index, ref in enumerate(state_refs):
        members, elements, nodes = ref.shape
        chosen = chosen_mask(sensors, elements)
        rows = ref[...].reshape(members * elements, nodes)
        values_out[index * members : (index + 1) * members, :] = pick(
            rows, members, elements, high, low, chosen
        )


def cross_kernel(paired, sensors_ref, high_ref, low_ref, values_ref, *refs):
    state_refs, out = refs[:-1], refs[-1]
    high, low = high_ref[...], low_ref[...]
    sensors = sensors_ref[...]
    parts = [values_ref[...]]
    for ref in state_refs:
        members, elements, nodes = ref.shape
        chosen = chosen_mask(sensors, elements)
        rows = ref[...].reshape(members * elements, nodes)
        parts.append(pick(rows, members, elements, high, low, chosen))
    values = jnp.concatenate(parts, axis=0)
    total = values.shape[0]
    if paired:
        size = total // (len(parts) + 1)
        blocks = [values[first : first + size] for first in range(0, total, size)]
        turned = [blocks[index ^ 1] for index in range(len(blocks))]
        values = jnp.where(is_odd(paired) == 1, jnp.concatenate(turned, axis=0), values)
    mean_value = jnp.sum(values, axis=0, keepdims=True) * (1.0 / total)
    anomaly = values - mean_value
    weighted = anomaly * sensors[5:6, :]
    innovation = sensors[4:5, :] - mean_value
    pad = jnp.zeros((out.shape[1] - total - 1, values.shape[1]), F32)
    right = jnp.concatenate([anomaly, innovation, pad], axis=0)
    out[...] = lax.dot_general(
        weighted,
        right,
        (((1,), (1,)), ((), ())),
        precision=lax.Precision.HIGHEST,
        preferred_element_type=F32,
    )


def mix_kernel(paired, sum_count, *refs):
    sums, state_refs, out, splats = refs[:sum_count], refs[sum_count:-2], refs[-2], refs[-1]
    highest = lax.Precision.HIGHEST
    total_sum = sums[0][...]
    for ref in sums[1:]:
        total_sum = total_sum + ref[...]
    local_members, elements, nodes = out.shape
    members = local_members * len(state_refs)
    row = lax.broadcasted_iota(jnp.int32, (members, members), 0)
    col = lax.broadcasted_iota(jnp.int32, (members, members), 1)
    identity = (row == col).astype(F32)
    system = total_sum[:, :members] + (members - 1) / INFLATION * identity
    project = total_sum[:, members : members + 1]
    trace_value = jnp.sum(
        jnp.sum(jnp.where(row == col, system, 0.0), axis=1, keepdims=True), axis=0, keepdims=True
    )
    iterate = system / trace_value
    inverse_root = identity
    for sweep in range(NS_ITERS):
        if sweep:
            product = jnp.dot(inverse_root, iterate, precision=highest)
        else:
            product = iterate
        middle = 0.5 * (3.0 * identity - product)
        if sweep + 1 < NS_ITERS:
            iterate = jnp.dot(iterate, middle, precision=highest)
        inverse_root = jnp.dot(middle, inverse_root, precision=highest) if sweep else middle
    mean_weights = (
        jnp.dot(inverse_root, jnp.dot(inverse_root, project, precision=highest), precision=highest)
        / trace_value
    )
    transform = inverse_root * jnp.sqrt((members - 1) / trace_value) + mean_weights
    mixing = transform - jnp.mean(transform, axis=0, keepdims=True) + 1.0 / members
    odd = is_odd(paired)
    if paired:
        mixing = jnp.where(
            odd == 1, mixing[:, local_members : 2 * local_members], mixing[:, :local_members]
        )
    for j in range(members):
        for k in range(local_members):
            splats[j * local_members + k] = jnp.broadcast_to(mixing[j : j + 1, k : k + 1], (8, 128))
    for block in range(elements // 8):
        span = slice(8 * block, 8 * block + 8)
        for lane in range(nodes // 128):
            lanes = slice(128 * lane, 128 * lane + 128)
            totals = [None] * local_members
            for j in range(members):
                piece, member = divmod(j, local_members)
                value = state_refs[piece][member, span, lanes]
                place = piece + odd * (1 - 2 * (piece % 2))
                for k in range(local_members):
                    term = splats[(place * local_members + member) * local_members + k] * value
                    totals[k] = term if totals[k] is None else totals[k] + term
            for k in range(local_members):
                out[k, span, lanes] = totals[k]


def is_paired(n_dom, n_ens):
    return n_dom == 4 and n_ens % 2 == 0


def spread(values, n_dom, n_ens):
    if not is_paired(n_dom, n_ens):
        return [values[0]] + [
            lax.ppermute(values[s], "dom", [(d, (d + s) % n_dom) for d in range(n_dom)])
            for s in range(1, n_dom)
        ]
    here, near, far = values
    pairs = []
    for d in range(n_dom):
        for e in range(n_ens):
            pairs.append((d * n_ens + e, (d ^ (3 if e % 2 else 1)) * n_ens + e))
    near = lax.ppermute(near, ("dom", "ens"), pairs)
    far = lax.ppermute(far, "dom", [(d, d ^ 2) for d in range(n_dom)])
    other = lax.ppermute(near, "ens", [(e, e ^ 1) for e in range(n_ens)])
    return [here, near, far, other]


def gather_members(state, n_ens):
    pieces = {0: state}
    if n_ens & (n_ens - 1):
        for shift in range(1, n_ens):
            pairs = [(e, (e + shift) % n_ens) for e in range(n_ens)]
            pieces[shift] = lax.ppermute(state, "ens", pairs)
        return [pieces[key] for key in range(n_ens)]
    bit = n_ens >> 1
    while bit:
        for key in list(pieces):
            pairs = [(e, e ^ bit) for e in range(n_ens)]
            pieces[key ^ bit] = lax.ppermute(pieces[key], "ens", pairs)
        bit >>= 1
    return [pieces[key] for key in range(n_ens)]


def make_on_device(n_dom, n_ens):
    vmem = pl.BlockSpec(memory_space=pltpu.VMEM)
    smem = pl.BlockSpec(memory_space=pltpu.SMEM)
    direct = n_dom <= DIRECT_DOM
    paired = is_paired(n_dom, n_ens)
    limit = VMEM_LIMIT if direct else None

    def call(kernel, out_shape, operands, specs=None, scratch=()):
        many = isinstance(out_shape, (list, tuple))
        return pl.pallas_call(
            kernel,
            out_shape=out_shape,
            in_specs=specs or [vmem] * len(operands),
            out_specs=[vmem] * len(out_shape) if many else vmem,
            scratch_shapes=list(scratch),
            compiler_params=pltpu.CompilerParams(vmem_limit_bytes=limit),
        )(*operands)

    def shape(dims, dtype=F32):
        return jax.ShapeDtypeStruct(dims, dtype)

    def on_device(state, coords, owner_local, counts, obs_value, obs_weight):
        local_members, _, nodes = state.shape
        slots = coords.shape[1]
        members = local_members * n_ens
        tile_shape = (8, 2 * CAP)
        hbm = [
            pltpu.with_memory_space_constraint(value, pltpu.HBM)
            for value in (
                state,
                counts,
                coords,
                owner_local[None],
                obs_value[None],
                obs_weight[None],
            )
        ]
        own, *tiles = call(
            lambda *refs: pack_kernel(direct, paired, *refs),
            [shape(state.shape)]
            + (
                [shape(tile_shape)] * (3 if paired else n_dom)
                if direct
                else [shape((n_dom,) + tile_shape)]
            ),
            hbm,
            [pl.BlockSpec(memory_space=pltpu.HBM)] * len(hbm),
            [
                pltpu.SMEM(counts.shape, jnp.int32),
                pltpu.VMEM(coords.shape, F32),
                pltpu.VMEM((1, slots), jnp.int32),
                pltpu.VMEM((1, slots), F32),
                pltpu.VMEM((1, slots), F32),
                pltpu.VMEM((8, slots), F32),
                pltpu.SemaphoreType.DMA(()),
                pltpu.SemaphoreType.DMA((5,)),
            ],
        )
        if direct:
            tiles = spread(tiles, n_dom, n_ens)
        else:
            moved = lax.all_to_all(tiles[0], "dom", split_axis=0, concat_axis=0, tiled=True)
            tiles = [moved[d] for d in range(n_dom)]
        pieces = gather_members(state, n_ens)
        pieces[0] = own
        sensor_count = CAP * (n_dom + n_dom % 2)
        early = min(2, n_ens)
        sensors, high, low, values = call(
            lambda *refs: values_kernel(n_dom, *refs),
            [
                shape((8, sensor_count)),
                shape((nodes, sensor_count), BF16),
                shape((nodes, sensor_count), BF16),
                shape((early * local_members, sensor_count)),
            ],
            list(tiles) + [pieces[key] for key in range(early)],
        )
        partial_sum = call(
            lambda *refs: cross_kernel(paired, *refs),
            shape((members, members + 8)),
            [sensors, high, low, values] + pieces[early:],
        )
        if direct:
            sums = spread([partial_sum] * (3 if paired else n_dom), n_dom, n_ens)
        else:
            sums = [lax.psum(partial_sum, "dom")]
        return call(
            lambda *refs: mix_kernel(paired, len(sums), *refs),
            shape(state.shape),
            sums + pieces,
            None,
            [pltpu.VMEM((members * local_members, 8, 128), F32)],
        )

    return on_device


def solution(mesh):
    n_dom, n_ens = mesh.shape["dom"], mesh.shape["ens"]
    return jax.shard_map(
        make_on_device(n_dom, n_ens),
        mesh=mesh,
        in_specs=(
            P("ens", ("groups", "dom"), None),
            P(None, ("groups", "dom")),
            P(("groups", "dom")),
            P(("groups", "dom"), None),
            P(("groups", "dom")),
            P(("groups", "dom")),
        ),
        out_specs=P("ens", ("groups", "dom"), None),
        check_vma=False,
    )
```

```python
import jax
import jax.numpy as jnp
from jax import lax
from jax.experimental import pallas as pl
from jax.experimental.pallas import tpu as pltpu
from jax.sharding import PartitionSpec as P


CAP = 64
NS_ITERS = 8


GLL_POINTS = (
    -1.0,
    -0.8717401485096066,
    -0.5917001814331423,
    -0.2092992179024789,
    0.2092992179024789,
    0.5917001814331423,
    0.8717401485096066,
    1.0,
)
INFLATION = 1.1
ORDER = len(GLL_POINTS)
F32 = jnp.float32
BF16 = jnp.bfloat16
DIRECT_DOM = 8
VMEM_LIMIT = 8 * 1024 * 1024
LANES = 128


def lagrange_scale(index):
    product = 1.0
    for other in range(ORDER):
        if other != index:
            product *= GLL_POINTS[index] - GLL_POINTS[other]
    return 1.0 / product


def lagrange_rows(position):
    shape = (ORDER, position.shape[1])
    node = lax.broadcasted_iota(jnp.int32, shape, 0)
    product = jnp.full(shape, lagrange_scale(0), F32)
    for index in range(1, ORDER):
        product = jnp.where(node == index, lagrange_scale(index), product)
    for other in range(ORDER):
        product = product * jnp.where(node == other, 1.0, position - GLL_POINTS[other])
    return product


def split(value):
    high = value.astype(BF16)
    low = (value - high.astype(F32)).astype(BF16)
    return high, low


def is_odd(paired):
    return lax.rem(lax.axis_index("ens"), 2) if paired else 0


def pack_kernel(direct, paired, state, counts, coords, owner, obs, weight, *rest):
    own, outs = rest[0], rest[1:-8]
    count_box, coord_box, owner_box, obs_box, weight_box, block, state_sem, sems = rest[-8:]
    state_copy = pltpu.make_async_copy(state, own, state_sem)
    pairs = zip(
        (counts, coords, owner, obs, weight), (count_box, coord_box, owner_box, obs_box, weight_box)
    )
    copies = [
        pltpu.make_async_copy(source, target, sems.at[index])
        for index, (source, target) in enumerate(pairs)
    ]
    for copy in copies:
        copy.start()
    state_copy.start()
    n_dom = counts.shape[1]
    slots = coords.shape[1]
    here = lax.axis_index("dom")
    block[...] = jnp.zeros(block.shape, F32)
    column = lax.broadcasted_iota(jnp.int32, (8, 2 * CAP), 1)
    for copy in copies:
        copy.wait()
    block[0:3, :] = coord_box[...]
    block[3:4, :] = owner_box[...].astype(F32)
    block[4:5, :] = obs_box[...]
    block[5:6, :] = weight_box[...]
    rows = block[...]

    def tile(target, half):
        start = jnp.int32(0)
        for other in range(n_dom):
            start = start + jnp.where(other < target, count_box[0, other], 0)
        count = count_box[0, target]
        turned = pltpu.roll(rows, lax.rem(half - start + slots, slots), axis=1)[:, : 2 * CAP]
        return jnp.where((column >= half) & (column < half + count), turned, 0.0)

    if paired:
        near = jnp.where(is_odd(paired) == 0, 1, 3)
        for out, bits, half in zip(outs, (0, near, 2), (0, CAP, 0)):
            out[...] = tile(jnp.bitwise_xor(here, bits), half)
    elif direct:
        for shift in range(n_dom):
            outs[shift][...] = tile(lax.rem(here + shift, n_dom), (shift % 2) * CAP)
    else:
        half = lax.rem(here, 2) * CAP

        def step(target, carry):
            outs[0][target] = tile(target, half)
            return carry

        lax.fori_loop(0, n_dom, step, 0)
    state_copy.wait()


def pick(state_rows, members, elements, high, low, chosen):
    rows_high, rows_low = split(state_rows)
    partial = (
        jnp.dot(rows_high, high, preferred_element_type=F32)
        + jnp.dot(rows_low, high, preferred_element_type=F32)
        + jnp.dot(rows_high, low, preferred_element_type=F32)
    )
    partial = partial.reshape(members, elements, partial.shape[1])
    return jnp.sum(jnp.where(chosen[None], partial, 0.0), axis=1)


def chosen_mask(sensors, elements):
    ids = lax.broadcasted_iota(jnp.int32, (elements, sensors.shape[1]), 0).astype(F32)
    return ids == sensors[3:4, :]


def values_kernel(tile_count, *refs):
    tiles, state_refs = refs[:tile_count], refs[tile_count:-4]
    sensors_out, high_out, low_out, values_out = refs[-4:]
    pairs = []
    for first in range(0, tile_count, 2):
        pair = tiles[first][...]
        if first + 1 < tile_count:
            pair = pair + tiles[first + 1][...]
        pairs.append(pair)
    sensors = jnp.concatenate(pairs, axis=1) if len(pairs) > 1 else pairs[0]
    sensors_out[...] = sensors
    along_r = lagrange_rows(sensors[0:1, :])
    along_s = lagrange_rows(sensors[1:2, :])
    along_t = lagrange_rows(sensors[2:3, :])
    for t in range(ORDER):
        for s in range(0, ORDER, 2):
            rows = [along_r * (along_t[t : t + 1, :] * along_s[k : k + 1, :]) for k in (s, s + 1)]
            high, low = split(jnp.concatenate(rows, axis=0))
            base = ORDER * ORDER * t + ORDER * s
            high_out[base : base + 2 * ORDER, :] = high
            low_out[base : base + 2 * ORDER, :] = low
    high, low = high_out[...], low_out[...]
    for index, ref in enumerate(state_refs):
        members, elements, nodes = ref.shape
        chosen = chosen_mask(sensors, elements)
        rows = ref[...].reshape(members * elements, nodes)
        values_out[index * members : (index + 1) * members, :] = pick(
            rows, members, elements, high, low, chosen
        )


def cross_kernel(paired, sensors_ref, high_ref, low_ref, values_ref, *refs):
    state_refs, out = refs[:-1], refs[-1]
    high, low = high_ref[...], low_ref[...]
    sensors = sensors_ref[...]
    parts = [values_ref[...]]
    for ref in state_refs:
        members, elements, nodes = ref.shape
        chosen = chosen_mask(sensors, elements)
        rows = ref[...].reshape(members * elements, nodes)
        parts.append(pick(rows, members, elements, high, low, chosen))
    values = jnp.concatenate(parts, axis=0)
    total = values.shape[0]
    if paired:
        size = total // (len(parts) + 1)
        blocks = [values[first : first + size] for first in range(0, total, size)]
        turned = [blocks[index ^ 1] for index in range(len(blocks))]
        values = jnp.where(is_odd(paired) == 1, jnp.concatenate(turned, axis=0), values)
    mean_value = jnp.sum(values, axis=0, keepdims=True) * (1.0 / total)
    anomaly = values - mean_value
    weighted = anomaly * sensors[5:6, :]
    innovation = sensors[5:6, :] * (sensors[4:5, :] - mean_value)
    copies = LANES // total
    left = jnp.concatenate([weighted, jnp.broadcast_to(innovation, (8, innovation.shape[1]))], axis=0)
    products = lax.dot_general(
        left,
        jnp.concatenate([anomaly] * copies, axis=0),
        (((1,), (1,)), ((), ())),
        precision=lax.Precision.HIGHEST,
        preferred_element_type=F32,
    )
    own_row = lax.broadcasted_iota(jnp.int32, (copies, LANES), 0)
    group = lax.broadcasted_iota(jnp.int32, (copies, LANES), 1) // total
    for half in range(total // copies):
        rows = products[half * copies : (half + 1) * copies, :]
        out[half : half + 1, :] = jnp.sum(
            jnp.where(own_row == group, rows, 0.0), axis=0, keepdims=True
        )
    out[2:3, :] = products[total : total + 1, :]
    trace_part = jnp.sum(jnp.sum(weighted * anomaly, axis=0, keepdims=True), axis=1, keepdims=True)
    out[3:4, :] = jnp.broadcast_to(trace_part, (1, LANES))
    out[4:8, :] = jnp.zeros((4, LANES), F32)


def lane_gather(value, lanes):
    return jnp.take_along_axis(value, lanes, axis=1, mode="promise_in_bounds")


def sublane_total(value):
    for shift in (4, 2, 1):
        value = value + pltpu.roll(value, shift, axis=0)
    return value


def mix_kernel(paired, sum_count, *refs):
    sums, state_refs = refs[:sum_count], refs[sum_count:-4]
    out, staged, splats, sems = refs[-4:]
    local_members, elements, nodes = out.shape
    members = local_members * len(state_refs)
    tile = (8, LANES)
    sub = lax.broadcasted_iota(jnp.int32, tile, 0)
    lane = lax.broadcasted_iota(jnp.int32, tile, 1)
    left_lanes = [(lane // members) * members + (sub + 8 * g) for g in range(2)]
    right_lanes = sub * members + lane % members
    identity = [(lane // members + 8 * h == lane % members).astype(F32) for h in range(2)]

    def as_left(matrix):
        return [[lane_gather(matrix[h], left_lanes[g]) for g in range(2)] for h in range(2)]

    def as_right(matrix):
        return [lane_gather(matrix[g], right_lanes) for g in range(2)]

    def product(left, right):
        return [sublane_total(left[h][0] * right[0] + left[h][1] * right[1]) for h in range(2)]

    total_sum = sums[0][...]
    for ref in sums[1:]:
        total_sum = total_sum + ref[...]
    trace_value = total_sum[3:4, :] + members * ((members - 1) / INFLATION)
    scale = 1.0 / trace_value
    project_row = jnp.broadcast_to(total_sum[2:3, :], tile)
    project = [lane_gather(project_row, sub + 8 * g) for g in range(2)]
    iterate = [
        (total_sum[h : h + 1, :] + (members - 1) / INFLATION * identity[h]) * scale
        for h in range(2)
    ]
    inverse_left = inverse_right = None
    solved = None
    for sweep in range(NS_ITERS):
        last = sweep + 1 == NS_ITERS
        if sweep:
            step = product(inverse_left, as_right(iterate))
        else:
            step = iterate
        middle = [1.5 * identity[h] - 0.5 * step[h] for h in range(2)]
        if last:
            middle_left = as_left(middle)
            solved = product(middle_left, as_right(product(inverse_left, project)))
            inverse_root = product(middle_left, inverse_right)
            break
        iterate = product(as_left(iterate), as_right(middle))
        inverse_root = product(as_left(middle), inverse_right) if sweep else middle
        inverse_left, inverse_right = as_left(inverse_root), as_right(inverse_root)
    mean_weights = product(as_left(inverse_root), as_right(solved))
    root_scale = jnp.sqrt((members - 1) * scale)
    transform = [inverse_root[h] * root_scale + mean_weights[h] * scale for h in range(2)]
    transform_right = as_right(transform)
    column_mean = sublane_total(transform_right[0] + transform_right[1]) * (1.0 / members)
    mixing = [transform[h] - column_mean + 1.0 / members for h in range(2)]
    odd = is_odd(paired)
    for k in range(local_members):
        lanes = sub * members + (k + local_members * odd)
        for h in range(2):
            column = lane_gather(mixing[h], lanes)
            for i in range(8):
                splats[(8 * h + i) * local_members + k] = jnp.broadcast_to(column[i : i + 1, :], tile)
    copies = []
    for block in range(elements // 8):
        span = slice(8 * block, 8 * block + 8)
        for lane in range(nodes // 128):
            lanes = slice(128 * lane, 128 * lane + 128)
            totals = [None] * local_members
            for j in range(members):
                piece, member = divmod(j, local_members)
                value = state_refs[piece][member, span, lanes]
                place = piece + odd * (1 - 2 * (piece % 2))
                for k in range(local_members):
                    term = splats[(place * local_members + member) * local_members + k] * value
                    totals[k] = term if totals[k] is None else totals[k] + term
            for k in range(local_members):
                staged[k, span, lanes] = totals[k]
        place = pl.ds(8 * block, 8)
        copy = pltpu.make_async_copy(staged.at[:, place], out.at[:, place], sems.at[block])
        copy.start()
        copies.append(copy)
    for copy in copies:
        copy.wait()


def is_paired(n_dom, n_ens):
    return n_dom == 4 and n_ens % 2 == 0


def spread(values, n_dom, n_ens):
    if not is_paired(n_dom, n_ens):
        return [values[0]] + [
            lax.ppermute(values[s], "dom", [(d, (d + s) % n_dom) for d in range(n_dom)])
            for s in range(1, n_dom)
        ]
    here, near, far = values
    pairs = []
    for d in range(n_dom):
        for e in range(n_ens):
            pairs.append((d * n_ens + e, (d ^ (3 if e % 2 else 1)) * n_ens + e))
    near = lax.ppermute(near, ("dom", "ens"), pairs)
    far = lax.ppermute(far, "dom", [(d, d ^ 2) for d in range(n_dom)])
    other = lax.ppermute(near, "ens", [(e, e ^ 1) for e in range(n_ens)])
    return [here, near, far, other]


def gather_members(state, n_ens):
    pieces = {0: state}
    if n_ens & (n_ens - 1):
        for shift in range(1, n_ens):
            pairs = [(e, (e + shift) % n_ens) for e in range(n_ens)]
            pieces[shift] = lax.ppermute(state, "ens", pairs)
        return [pieces[key] for key in range(n_ens)]
    bit = n_ens >> 1
    while bit:
        for key in list(pieces):
            pairs = [(e, e ^ bit) for e in range(n_ens)]
            pieces[key ^ bit] = lax.ppermute(pieces[key], "ens", pairs)
        bit >>= 1
    return [pieces[key] for key in range(n_ens)]


def make_on_device(n_dom, n_ens):
    vmem = pl.BlockSpec(memory_space=pltpu.VMEM)
    smem = pl.BlockSpec(memory_space=pltpu.SMEM)
    direct = n_dom <= DIRECT_DOM
    paired = is_paired(n_dom, n_ens)
    limit = VMEM_LIMIT if direct else None

    def call(kernel, out_shape, operands, specs=None, scratch=(), out_spec=vmem):
        many = isinstance(out_shape, (list, tuple))
        return pl.pallas_call(
            kernel,
            out_shape=out_shape,
            in_specs=specs or [vmem] * len(operands),
            out_specs=[out_spec] * len(out_shape) if many else out_spec,
            scratch_shapes=list(scratch),
            compiler_params=pltpu.CompilerParams(vmem_limit_bytes=limit),
        )(*operands)

    def shape(dims, dtype=F32):
        return jax.ShapeDtypeStruct(dims, dtype)

    def on_device(state, coords, owner_local, counts, obs_value, obs_weight):
        local_members, elements, nodes = state.shape
        slots = coords.shape[1]
        members = local_members * n_ens
        tile_shape = (8, 2 * CAP)
        hbm = [
            pltpu.with_memory_space_constraint(value, pltpu.HBM)
            for value in (
                state,
                counts,
                coords,
                owner_local[None],
                obs_value[None],
                obs_weight[None],
            )
        ]
        own, *tiles = call(
            lambda *refs: pack_kernel(direct, paired, *refs),
            [shape(state.shape)]
            + (
                [shape(tile_shape)] * (3 if paired else n_dom)
                if direct
                else [shape((n_dom,) + tile_shape)]
            ),
            hbm,
            [pl.BlockSpec(memory_space=pltpu.HBM)] * len(hbm),
            [
                pltpu.SMEM(counts.shape, jnp.int32),
                pltpu.VMEM(coords.shape, F32),
                pltpu.VMEM((1, slots), jnp.int32),
                pltpu.VMEM((1, slots), F32),
                pltpu.VMEM((1, slots), F32),
                pltpu.VMEM((8, slots), F32),
                pltpu.SemaphoreType.DMA(()),
                pltpu.SemaphoreType.DMA((5,)),
            ],
        )
        if direct:
            tiles = spread(tiles, n_dom, n_ens)
        else:
            moved = lax.all_to_all(tiles[0], "dom", split_axis=0, concat_axis=0, tiled=True)
            tiles = [moved[d] for d in range(n_dom)]
        pieces = gather_members(state, n_ens)
        pieces[0] = own
        sensor_count = CAP * (n_dom + n_dom % 2)
        early = min(2, n_ens)
        sensors, high, low, values = call(
            lambda *refs: values_kernel(n_dom, *refs),
            [
                shape((8, sensor_count)),
                shape((nodes, sensor_count), BF16),
                shape((nodes, sensor_count), BF16),
                shape((early * local_members, sensor_count)),
            ],
            list(tiles) + [pieces[key] for key in range(early)],
        )
        partial_sum = call(
            lambda *refs: cross_kernel(paired, *refs),
            shape((8, LANES)),
            [sensors, high, low, values] + pieces[early:],
        )
        if direct:
            sums = spread([partial_sum] * (3 if paired else n_dom), n_dom, n_ens)
        else:
            sums = [lax.psum(partial_sum, "dom")]
        return call(
            lambda *refs: mix_kernel(paired, len(sums), *refs),
            shape(state.shape),
            sums + pieces,
            None,
            [
                pltpu.VMEM(state.shape, F32),
                pltpu.VMEM((members * local_members, 8, 128), F32),
                pltpu.SemaphoreType.DMA((elements // 8,)),
            ],
            pl.BlockSpec(memory_space=pltpu.HBM),
        )

    return on_device


def solution(mesh):
    n_dom, n_ens = mesh.shape["dom"], mesh.shape["ens"]
    return jax.shard_map(
        make_on_device(n_dom, n_ens),
        mesh=mesh,
        in_specs=(
            P("ens", ("groups", "dom"), None),
            P(None, ("groups", "dom")),
            P(("groups", "dom")),
            P(("groups", "dom"), None),
            P(("groups", "dom")),
            P(("groups", "dom")),
        ),
        out_specs=P("ens", ("groups", "dom"), None),
        check_vma=False,
    )
```

```python
import jax
import jax.numpy as jnp
from jax import lax
from jax.experimental import pallas as pl
from jax.experimental.pallas import tpu as pltpu
from jax.sharding import PartitionSpec as P


CAP = 64
NS_ITERS = 8


GLL_POINTS = (
    -1.0,
    -0.8717401485096066,
    -0.5917001814331423,
    -0.2092992179024789,
    0.2092992179024789,
    0.5917001814331423,
    0.8717401485096066,
    1.0,
)
INFLATION = 1.1
ORDER = len(GLL_POINTS)
F32 = jnp.float32
BF16 = jnp.bfloat16
DIRECT_DOM = 8
VMEM_LIMIT = 8 * 1024 * 1024
LANES = 128
PROJECT_LANES = 8
TRACE_LANE = 64


def lagrange_scale(index):
    product = 1.0
    for other in range(ORDER):
        if other != index:
            product *= GLL_POINTS[index] - GLL_POINTS[other]
    return 1.0 / product


def lagrange_rows(position):
    shape = (ORDER, position.shape[1])
    node = lax.broadcasted_iota(jnp.int32, shape, 0)
    product = jnp.full(shape, lagrange_scale(0), F32)
    for index in range(1, ORDER):
        product = jnp.where(node == index, lagrange_scale(index), product)
    for other in range(ORDER):
        product = product * jnp.where(node == other, 1.0, position - GLL_POINTS[other])
    return product


def split(value):
    high = value.astype(BF16)
    low = (value - high.astype(F32)).astype(BF16)
    return high, low


def is_odd(paired):
    return lax.rem(lax.axis_index("ens"), 2) if paired else 0


def pack_kernel(direct, paired, counts, coords, owner, obs, weight, *rest):
    outs = rest[:-7]
    count_box, coord_box, owner_box, obs_box, weight_box, block, sems = rest[-7:]
    pairs = zip(
        (counts, coords, owner, obs, weight), (count_box, coord_box, owner_box, obs_box, weight_box)
    )
    copies = [
        pltpu.make_async_copy(source, target, sems.at[index])
        for index, (source, target) in enumerate(pairs)
    ]
    for copy in copies:
        copy.start()
    n_dom = counts.shape[1]
    slots = coords.shape[1]
    here = lax.axis_index("dom")
    block[...] = jnp.zeros(block.shape, F32)
    column = lax.broadcasted_iota(jnp.int32, (8, 2 * CAP), 1)
    for copy in copies:
        copy.wait()
    block[0:3, :] = coord_box[...]
    block[3:4, :] = owner_box[...].astype(F32)
    block[4:5, :] = obs_box[...]
    block[5:6, :] = weight_box[...]
    rows = block[...]

    def tile(target, half):
        start = jnp.int32(0)
        for other in range(n_dom):
            start = start + jnp.where(other < target, count_box[0, other], 0)
        count = count_box[0, target]
        turned = pltpu.roll(rows, lax.rem(half - start + slots, slots), axis=1)[:, : 2 * CAP]
        return jnp.where((column >= half) & (column < half + count), turned, 0.0)

    if paired:
        near = jnp.where(is_odd(paired) == 0, 1, 3)
        for out, bits, half in zip(outs, (0, near, 2), (0, CAP, 0)):
            out[...] = tile(jnp.bitwise_xor(here, bits), half)
    elif direct:
        for shift in range(n_dom):
            outs[shift][...] = tile(lax.rem(here + shift, n_dom), (shift % 2) * CAP)
    else:
        half = lax.rem(here, 2) * CAP

        def step(target, carry):
            outs[0][target] = tile(target, half)
            return carry

        lax.fori_loop(0, n_dom, step, 0)


def pick(refs, sensors, high, low):
    members, elements, nodes = refs[0].shape
    rows = jnp.concatenate([ref[...].reshape(members * elements, nodes) for ref in refs], axis=0)
    rows_high, rows_low = split(rows)
    both = jnp.dot(
        jnp.concatenate([rows_high, rows_low], axis=0), high, preferred_element_type=F32
    )
    partial = (
        both[: rows.shape[0]]
        + both[rows.shape[0] :]
        + jnp.dot(rows_high, low, preferred_element_type=F32)
    )
    ids = lax.broadcasted_iota(jnp.int32, (elements, sensors.shape[1]), 0).astype(F32)
    partial = partial.reshape(len(refs) * members, elements, partial.shape[1])
    return jnp.sum(jnp.where((ids == sensors[3:4, :])[None], partial, 0.0), axis=1)


def values_kernel(tile_count, *refs):
    tiles, state, state_refs = refs[:tile_count], refs[tile_count], refs[tile_count + 1 : -6]
    sensors_out, high_out, low_out, values_out, own, sem = refs[-6:]
    copy = pltpu.make_async_copy(state, own, sem)
    copy.start()
    pairs = []
    for first in range(0, tile_count, 2):
        pair = tiles[first][...]
        if first + 1 < tile_count:
            pair = pair + tiles[first + 1][...]
        pairs.append(pair)
    sensors = jnp.concatenate(pairs, axis=1) if len(pairs) > 1 else pairs[0]
    sensors_out[...] = sensors
    along_r = lagrange_rows(sensors[0:1, :])
    along_s = lagrange_rows(sensors[1:2, :])
    along_t = lagrange_rows(sensors[2:3, :])
    for t in range(ORDER):
        for s in range(0, ORDER, 2):
            rows = [along_r * (along_t[t : t + 1, :] * along_s[k : k + 1, :]) for k in (s, s + 1)]
            high, low = split(jnp.concatenate(rows, axis=0))
            base = ORDER * ORDER * t + ORDER * s
            high_out[base : base + 2 * ORDER, :] = high
            low_out[base : base + 2 * ORDER, :] = low
    members = own.shape[0]
    if state_refs:
        values_out[members:, :] = pick(state_refs, sensors, high_out[...], low_out[...])
    copy.wait()
    values_out[:members, :] = pick([own], sensors, high_out[...], low_out[...])


def cross_kernel(paired, sensors_ref, high_ref, low_ref, values_ref, *refs):
    state_refs, out = refs[:-1], refs[-1]
    sensors = sensors_ref[...]
    values = jnp.concatenate(
        [values_ref[...], pick(state_refs, sensors, high_ref[...], low_ref[...])], axis=0
    )
    total = values.shape[0]
    if paired:
        size = state_refs[0].shape[0]
        blocks = [values[first : first + size] for first in range(0, total, size)]
        turned = [blocks[index ^ 1] for index in range(len(blocks))]
        values = jnp.where(is_odd(paired) == 1, jnp.concatenate(turned, axis=0), values)
    mean_value = jnp.sum(values, axis=0, keepdims=True) * (1.0 / total)
    anomaly = values - mean_value
    weighted = anomaly * sensors[5:6, :]
    innovation = sensors[4:5, :] - mean_value
    pad = jnp.zeros((PROJECT_LANES - 1, values.shape[1]), F32)
    right = jnp.concatenate([anomaly, innovation, pad], axis=0)
    left_high, left_low = split(weighted)
    right_high, right_low = split(right)
    across = (((1,), (1,)), ((), ()))
    both = lax.dot_general(
        jnp.concatenate([left_high, left_low], axis=0),
        right_high,
        across,
        preferred_element_type=F32,
    )
    out[:, : total + PROJECT_LANES] = (
        both[:total]
        + both[total:]
        + lax.dot_general(left_high, right_low, across, preferred_element_type=F32)
    )
    trace_part = jnp.sum(jnp.sum(weighted * anomaly, axis=0, keepdims=True), axis=1, keepdims=True)
    out[:, TRACE_LANE:] = jnp.broadcast_to(trace_part, (total, LANES - TRACE_LANE))


def lane_gather(value, lanes):
    return jnp.take_along_axis(value, lanes, axis=1, mode="promise_in_bounds")


def sublane_total(value):
    for shift in (4, 2, 1):
        value = value + pltpu.roll(value, shift, axis=0)
    return value


def mix_kernel(paired, sum_count, *refs):
    sums, state_refs = refs[:sum_count], refs[sum_count:-4]
    out, staged, splats, sems = refs[-4:]
    local_members, elements, nodes = out.shape
    members = local_members * len(state_refs)
    tile = (8, LANES)
    sub = lax.broadcasted_iota(jnp.int32, tile, 0)
    lane = lax.broadcasted_iota(jnp.int32, tile, 1)
    left_lanes = [(lane // members) * members + (sub + 8 * g) for g in range(2)]
    right_lanes = sub * members + lane % members
    identity = [(lane // members + 8 * h == lane % members).astype(F32) for h in range(2)]

    def as_left(matrix):
        return [[lane_gather(matrix[h], left_lanes[g]) for g in range(2)] for h in range(2)]

    def as_right(matrix):
        return [lane_gather(matrix[g], right_lanes) for g in range(2)]

    def product(left, right):
        return [sublane_total(left[h][0] * right[0] + left[h][1] * right[1]) for h in range(2)]

    total_sum = sums[0][...]
    for ref in sums[1:]:
        total_sum = total_sum + ref[...]
    rows = [total_sum[8 * g : 8 * g + 8, :] for g in range(2)]
    project = [lane_gather(rows[g], jnp.full(tile, members, jnp.int32)) for g in range(2)]
    trace_value = lane_gather(rows[0], jnp.full(tile, TRACE_LANE, jnp.int32))
    scale = 1.0 / (trace_value + members * ((members - 1) / INFLATION))
    diagonal = (members - 1) / INFLATION
    unit_left = [[(lane // members + 8 * h == sub + 8 * g).astype(F32) for g in range(2)] for h in range(2)]
    unit_right = [(lane % members == sub + 8 * g).astype(F32) for g in range(2)]
    system_left = [
        [
            (lane_gather(rows[g], lane // members + 8 * h) + diagonal * unit_left[h][g]) * scale
            for g in range(2)
        ]
        for h in range(2)
    ]
    system_right = [
        (lane_gather(rows[g], lane % members) + diagonal * unit_right[g]) * scale for g in range(2)
    ]
    inverse_left = [
        [1.5 * unit_left[h][g] - 0.5 * system_left[h][g] for g in range(2)] for h in range(2)
    ]
    inverse_right = [1.5 * unit_right[g] - 0.5 * system_right[g] for g in range(2)]
    iterate = product(system_left, inverse_right)
    for sweep in range(1, NS_ITERS):
        step = product(inverse_left, as_right(iterate))
        middle = [1.5 * identity[h] - 0.5 * step[h] for h in range(2)]
        middle_left = as_left(middle)
        inverse_root = product(middle_left, inverse_right)
        if sweep + 1 < NS_ITERS:
            iterate = product(as_left(iterate), as_right(middle))
            inverse_left, inverse_right = as_left(inverse_root), as_right(inverse_root)
        else:
            solved = product(middle_left, as_right(product(inverse_left, project)))
    mean_weights = product(as_left(inverse_root), as_right(solved))
    root_scale = jnp.sqrt((members - 1) * scale)
    transform = [inverse_root[h] * root_scale + mean_weights[h] * scale for h in range(2)]
    transform_right = as_right(transform)
    column_mean = sublane_total(transform_right[0] + transform_right[1]) * (1.0 / members)
    mixing = [transform[h] - column_mean + 1.0 / members for h in range(2)]
    odd = is_odd(paired)
    for k in range(local_members):
        lanes = sub * members + (k + local_members * odd)
        for h in range(2):
            column = lane_gather(mixing[h], lanes)
            for i in range(8):
                splats[(8 * h + i) * local_members + k] = jnp.broadcast_to(column[i : i + 1, :], tile)
    copies = []
    for block in range(elements // 8):
        span = slice(8 * block, 8 * block + 8)
        for lane in range(nodes // 128):
            lanes = slice(128 * lane, 128 * lane + 128)
            totals = [None] * local_members
            for j in range(members):
                piece, member = divmod(j, local_members)
                value = state_refs[piece][member, span, lanes]
                place = piece + odd * (1 - 2 * (piece % 2))
                for k in range(local_members):
                    term = splats[(place * local_members + member) * local_members + k] * value
                    totals[k] = term if totals[k] is None else totals[k] + term
            for k in range(local_members):
                staged[k, span, lanes] = totals[k]
        place = pl.ds(8 * block, 8)
        copy = pltpu.make_async_copy(staged.at[:, place], out.at[:, place], sems.at[block])
        copy.start()
        copies.append(copy)
    for copy in copies:
        copy.wait()


def is_paired(n_dom, n_ens):
    return n_dom == 4 and n_ens % 2 == 0


def spread(values, n_dom, n_ens):
    if not is_paired(n_dom, n_ens):
        return [values[0]] + [
            lax.ppermute(values[s], "dom", [(d, (d + s) % n_dom) for d in range(n_dom)])
            for s in range(1, n_dom)
        ]
    here, near, far = values
    pairs = []
    for d in range(n_dom):
        for e in range(n_ens):
            pairs.append((d * n_ens + e, (d ^ (3 if e % 2 else 1)) * n_ens + e))
    near = lax.ppermute(near, ("dom", "ens"), pairs)
    far = lax.ppermute(far, "dom", [(d, d ^ 2) for d in range(n_dom)])
    other = lax.ppermute(near, "ens", [(e, e ^ 1) for e in range(n_ens)])
    return [here, near, far, other]


def gather_members(state, n_ens):
    pieces = {0: state}
    if n_ens & (n_ens - 1):
        for shift in range(1, n_ens):
            pairs = [(e, (e + shift) % n_ens) for e in range(n_ens)]
            pieces[shift] = lax.ppermute(state, "ens", pairs)
        return [pieces[key] for key in range(n_ens)]
    bit = n_ens >> 1
    while bit:
        for key in list(pieces):
            pairs = [(e, e ^ bit) for e in range(n_ens)]
            pieces[key ^ bit] = lax.ppermute(pieces[key], "ens", pairs)
        bit >>= 1
    return [pieces[key] for key in range(n_ens)]


def make_on_device(n_dom, n_ens):
    vmem = pl.BlockSpec(memory_space=pltpu.VMEM)
    hbm = pl.BlockSpec(memory_space=pltpu.HBM)
    direct = n_dom <= DIRECT_DOM
    paired = is_paired(n_dom, n_ens)
    limit = VMEM_LIMIT if direct else None

    def call(kernel, out_shape, operands, specs=None, scratch=(), out_spec=vmem):
        many = isinstance(out_shape, (list, tuple))
        return pl.pallas_call(
            kernel,
            out_shape=out_shape,
            in_specs=specs or [vmem] * len(operands),
            out_specs=[out_spec] * len(out_shape) if many else out_spec,
            scratch_shapes=list(scratch),
            compiler_params=pltpu.CompilerParams(vmem_limit_bytes=limit),
        )(*operands)

    def in_hbm(value):
        return pltpu.with_memory_space_constraint(value, pltpu.HBM)

    def shape(dims, dtype=F32):
        return jax.ShapeDtypeStruct(dims, dtype)

    def on_device(state, coords, owner_local, counts, obs_value, obs_weight):
        local_members, elements, nodes = state.shape
        slots = coords.shape[1]
        members = local_members * n_ens
        tile_shape = (8, 2 * CAP)
        inputs = [counts, coords, owner_local[None], obs_value[None], obs_weight[None]]
        tiles = call(
            lambda *refs: pack_kernel(direct, paired, *refs),
            [shape(tile_shape)] * (3 if paired else n_dom)
            if direct
            else [shape((n_dom,) + tile_shape)],
            [in_hbm(value) for value in inputs],
            [hbm] * len(inputs),
            [
                pltpu.SMEM(counts.shape, jnp.int32),
                pltpu.VMEM(coords.shape, F32),
                pltpu.VMEM((1, slots), jnp.int32),
                pltpu.VMEM((1, slots), F32),
                pltpu.VMEM((1, slots), F32),
                pltpu.VMEM((8, slots), F32),
                pltpu.SemaphoreType.DMA((5,)),
            ],
        )
        if direct:
            tiles = spread(tiles, n_dom, n_ens)
        else:
            moved = lax.all_to_all(tiles[0], "dom", split_axis=0, concat_axis=0, tiled=True)
            tiles = [moved[d] for d in range(n_dom)]
        pieces = gather_members(state, n_ens)
        sensor_count = CAP * (n_dom + n_dom % 2)
        early = n_ens - 1
        sensors, high, low, values, pieces[0] = call(
            lambda *refs: values_kernel(n_dom, *refs),
            [
                shape((8, sensor_count)),
                shape((nodes, sensor_count), BF16),
                shape((nodes, sensor_count), BF16),
                shape((early * local_members, sensor_count)),
                shape(state.shape),
            ],
            list(tiles) + [in_hbm(state)] + pieces[1:early],
            [vmem] * n_dom + [hbm] + [vmem] * (early - 1),
            [pltpu.SemaphoreType.DMA(())],
        )
        partial_sum = call(
            lambda *refs: cross_kernel(paired, *refs),
            shape((members, LANES)),
            [sensors, high, low, values] + pieces[early:],
        )
        if direct:
            sums = spread([partial_sum] * (3 if paired else n_dom), n_dom, n_ens)
        else:
            sums = [lax.psum(partial_sum, "dom")]
        return call(
            lambda *refs: mix_kernel(paired, len(sums), *refs),
            shape(state.shape),
            sums + pieces,
            None,
            [
                pltpu.VMEM(state.shape, F32),
                pltpu.VMEM((members * local_members, 8, 128), F32),
                pltpu.SemaphoreType.DMA((elements // 8,)),
            ],
            hbm,
        )

    return on_device


def solution(mesh):
    n_dom, n_ens = mesh.shape["dom"], mesh.shape["ens"]
    return jax.shard_map(
        make_on_device(n_dom, n_ens),
        mesh=mesh,
        in_specs=(
            P("ens", ("groups", "dom"), None),
            P(None, ("groups", "dom")),
            P(("groups", "dom")),
            P(("groups", "dom"), None),
            P(("groups", "dom")),
            P(("groups", "dom")),
        ),
        out_specs=P("ens", ("groups", "dom"), None),
        check_vma=False,
    )
```

```python
import jax
import jax.numpy as jnp
from jax import lax
from jax.experimental import pallas as pl
from jax.experimental.pallas import tpu as pltpu
from jax.sharding import PartitionSpec as P


CAP = 64
NS_ITERS = 8


GLL_POINTS = (
    -1.0,
    -0.8717401485096066,
    -0.5917001814331423,
    -0.2092992179024789,
    0.2092992179024789,
    0.5917001814331423,
    0.8717401485096066,
    1.0,
)
INFLATION = 1.1
ORDER = len(GLL_POINTS)
F32 = jnp.float32
BF16 = jnp.bfloat16
DIRECT_DOM = 8
VMEM_LIMIT = 8 * 1024 * 1024
LANES = 128
PROJECT_LANES = 8
TRACE_LANE = 64


def lagrange_scale(index):
    product = 1.0
    for other in range(ORDER):
        if other != index:
            product *= GLL_POINTS[index] - GLL_POINTS[other]
    return 1.0 / product


def lagrange_rows(position):
    shape = (ORDER, position.shape[1])
    node = lax.broadcasted_iota(jnp.int32, shape, 0)
    product = jnp.full(shape, lagrange_scale(0), F32)
    for index in range(1, ORDER):
        product = jnp.where(node == index, lagrange_scale(index), product)
    for other in range(ORDER):
        product = product * jnp.where(node == other, 1.0, position - GLL_POINTS[other])
    return product


def split(value):
    high = value.astype(BF16)
    low = (value - high.astype(F32)).astype(BF16)
    return high, low


def is_odd(paired):
    return lax.rem(lax.axis_index("ens"), 2) if paired else 0


def pack_kernel(direct, paired, state, counts, coords, owner, obs, weight, *rest):
    own, outs = rest[0], rest[1:-8]
    count_box, coord_box, owner_box, obs_box, weight_box, block, state_sem, sems = rest[-8:]
    state_copy = pltpu.make_async_copy(state, own, state_sem)
    pairs = zip(
        (counts, coords, owner, obs, weight), (count_box, coord_box, owner_box, obs_box, weight_box)
    )
    copies = [
        pltpu.make_async_copy(source, target, sems.at[index])
        for index, (source, target) in enumerate(pairs)
    ]
    for copy in copies:
        copy.start()
    state_copy.start()
    n_dom = counts.shape[1]
    slots = coords.shape[1]
    here = lax.axis_index("dom")
    block[...] = jnp.zeros(block.shape, F32)
    column = lax.broadcasted_iota(jnp.int32, (8, 2 * CAP), 1)
    for copy in copies:
        copy.wait()
    block[0:3, :] = coord_box[...]
    block[3:4, :] = owner_box[...].astype(F32)
    block[4:5, :] = obs_box[...]
    block[5:6, :] = weight_box[...]
    rows = block[...]

    def tile(target, half):
        start = jnp.int32(0)
        for other in range(n_dom):
            start = start + jnp.where(other < target, count_box[0, other], 0)
        count = count_box[0, target]
        turned = pltpu.roll(rows, lax.rem(half - start + slots, slots), axis=1)[:, : 2 * CAP]
        return jnp.where((column >= half) & (column < half + count), turned, 0.0)

    if paired:
        near = jnp.where(is_odd(paired) == 0, 1, 3)
        for out, bits, half in zip(outs, (0, near, 2), (0, CAP, 0)):
            out[...] = tile(jnp.bitwise_xor(here, bits), half)
    elif direct:
        for shift in range(n_dom):
            outs[shift][...] = tile(lax.rem(here + shift, n_dom), (shift % 2) * CAP)
    else:
        half = lax.rem(here, 2) * CAP

        def step(target, carry):
            outs[0][target] = tile(target, half)
            return carry

        lax.fori_loop(0, n_dom, step, 0)
    state_copy.wait()


def pick(refs, sensors, high, low):
    members, elements, nodes = refs[0].shape
    rows = jnp.concatenate([ref[...].reshape(members * elements, nodes) for ref in refs], axis=0)
    rows_high, rows_low = split(rows)
    both = jnp.dot(
        jnp.concatenate([rows_high, rows_low], axis=0), high, preferred_element_type=F32
    )
    partial = (
        both[: rows.shape[0]]
        + both[rows.shape[0] :]
        + jnp.dot(rows_high, low, preferred_element_type=F32)
    )
    ids = lax.broadcasted_iota(jnp.int32, (elements, sensors.shape[1]), 0).astype(F32)
    partial = partial.reshape(len(refs) * members, elements, partial.shape[1])
    return jnp.sum(jnp.where((ids == sensors[3:4, :])[None], partial, 0.0), axis=1)


def values_kernel(tile_count, *refs):
    tiles, state_refs = refs[:tile_count], refs[tile_count:-4]
    sensors_out, high_out, low_out, values_out = refs[-4:]
    pairs = []
    for first in range(0, tile_count, 2):
        pair = tiles[first][...]
        if first + 1 < tile_count:
            pair = pair + tiles[first + 1][...]
        pairs.append(pair)
    sensors = jnp.concatenate(pairs, axis=1) if len(pairs) > 1 else pairs[0]
    sensors_out[...] = sensors
    along_r = lagrange_rows(sensors[0:1, :])
    along_s = lagrange_rows(sensors[1:2, :])
    along_t = lagrange_rows(sensors[2:3, :])
    for t in range(ORDER):
        for s in range(0, ORDER, 2):
            rows = [along_r * (along_t[t : t + 1, :] * along_s[k : k + 1, :]) for k in (s, s + 1)]
            high, low = split(jnp.concatenate(rows, axis=0))
            base = ORDER * ORDER * t + ORDER * s
            high_out[base : base + 2 * ORDER, :] = high
            low_out[base : base + 2 * ORDER, :] = low
    values_out[...] = pick(state_refs, sensors, high_out[...], low_out[...])


def cross_kernel(paired, sensors_ref, high_ref, low_ref, values_ref, *refs):
    state_refs, out = refs[:-1], refs[-1]
    sensors = sensors_ref[...]
    values = jnp.concatenate(
        [values_ref[...], pick(state_refs, sensors, high_ref[...], low_ref[...])], axis=0
    )
    total = values.shape[0]
    if paired:
        size = state_refs[0].shape[0]
        blocks = [values[first : first + size] for first in range(0, total, size)]
        turned = [blocks[index ^ 1] for index in range(len(blocks))]
        values = jnp.where(is_odd(paired) == 1, jnp.concatenate(turned, axis=0), values)
    mean_value = jnp.sum(values, axis=0, keepdims=True) * (1.0 / total)
    anomaly = values - mean_value
    weighted = anomaly * sensors[5:6, :]
    innovation = sensors[4:5, :] - mean_value
    pad = jnp.zeros((PROJECT_LANES - 1, values.shape[1]), F32)
    right = jnp.concatenate([anomaly, innovation, pad], axis=0)
    left_high, left_low = split(weighted)
    right_high, right_low = split(right)
    across = (((1,), (1,)), ((), ()))
    both = lax.dot_general(
        jnp.concatenate([left_high, left_low], axis=0),
        right_high,
        across,
        preferred_element_type=F32,
    )
    out[:, : total + PROJECT_LANES] = (
        both[:total]
        + both[total:]
        + lax.dot_general(left_high, right_low, across, preferred_element_type=F32)
    )
    trace_part = jnp.sum(jnp.sum(weighted * anomaly, axis=0, keepdims=True), axis=1, keepdims=True)
    out[:, TRACE_LANE:] = jnp.broadcast_to(trace_part, (total, LANES - TRACE_LANE))


def lane_gather(value, lanes):
    return jnp.take_along_axis(value, lanes, axis=1, mode="promise_in_bounds")


def sublane_total(value):
    for shift in (4, 2, 1):
        value = value + pltpu.roll(value, shift, axis=0)
    return value


def mix_kernel(paired, sum_count, *refs):
    sums, state_refs = refs[:sum_count], refs[sum_count:-4]
    out, staged, splats, sems = refs[-4:]
    local_members, elements, nodes = out.shape
    members = local_members * len(state_refs)
    tile = (8, LANES)
    sub = lax.broadcasted_iota(jnp.int32, tile, 0)
    lane = lax.broadcasted_iota(jnp.int32, tile, 1)
    left_lanes = [(lane // members) * members + (sub + 8 * g) for g in range(2)]
    right_lanes = sub * members + lane % members
    identity = [(lane // members + 8 * h == lane % members).astype(F32) for h in range(2)]

    def as_left(matrix):
        return [[lane_gather(matrix[h], left_lanes[g]) for g in range(2)] for h in range(2)]

    def as_right(matrix):
        return [lane_gather(matrix[g], right_lanes) for g in range(2)]

    def product(left, right):
        return [sublane_total(left[h][0] * right[0] + left[h][1] * right[1]) for h in range(2)]

    total_sum = sums[0][...]
    for ref in sums[1:]:
        total_sum = total_sum + ref[...]
    rows = [total_sum[8 * g : 8 * g + 8, :] for g in range(2)]
    project = [lane_gather(rows[g], jnp.full(tile, members, jnp.int32)) for g in range(2)]
    trace_value = lane_gather(rows[0], jnp.full(tile, TRACE_LANE, jnp.int32))
    scale = 1.0 / (trace_value + members * ((members - 1) / INFLATION))
    diagonal = (members - 1) / INFLATION
    unit_left = [[(lane // members + 8 * h == sub + 8 * g).astype(F32) for g in range(2)] for h in range(2)]
    unit_right = [(lane % members == sub + 8 * g).astype(F32) for g in range(2)]
    system_left = [
        [
            (lane_gather(rows[g], lane // members + 8 * h) + diagonal * unit_left[h][g]) * scale
            for g in range(2)
        ]
        for h in range(2)
    ]
    system_right = [
        (lane_gather(rows[g], lane % members) + diagonal * unit_right[g]) * scale for g in range(2)
    ]
    inverse_left = [
        [1.5 * unit_left[h][g] - 0.5 * system_left[h][g] for g in range(2)] for h in range(2)
    ]
    inverse_right = [1.5 * unit_right[g] - 0.5 * system_right[g] for g in range(2)]
    iterate = product(system_left, inverse_right)
    for sweep in range(1, NS_ITERS):
        step = product(inverse_left, as_right(iterate))
        middle = [1.5 * identity[h] - 0.5 * step[h] for h in range(2)]
        middle_left = as_left(middle)
        inverse_root = product(middle_left, inverse_right)
        if sweep + 1 < NS_ITERS:
            iterate = product(as_left(iterate), as_right(middle))
            inverse_left, inverse_right = as_left(inverse_root), as_right(inverse_root)
        else:
            solved = product(middle_left, as_right(product(inverse_left, project)))
    mean_weights = product(as_left(inverse_root), as_right(solved))
    root_scale = jnp.sqrt((members - 1) * scale)
    transform = [inverse_root[h] * root_scale + mean_weights[h] * scale for h in range(2)]
    transform_right = as_right(transform)
    column_mean = sublane_total(transform_right[0] + transform_right[1]) * (1.0 / members)
    mixing = [transform[h] - column_mean + 1.0 / members for h in range(2)]
    odd = is_odd(paired)
    for k in range(local_members):
        lanes = sub * members + (k + local_members * odd)
        for h in range(2):
            column = lane_gather(mixing[h], lanes)
            for i in range(8):
                splats[(8 * h + i) * local_members + k] = jnp.broadcast_to(column[i : i + 1, :], tile)
    copies = []
    for block in range(elements // 8):
        span = slice(8 * block, 8 * block + 8)
        for lane in range(nodes // 128):
            lanes = slice(128 * lane, 128 * lane + 128)
            totals = [None] * local_members
            for j in range(members):
                piece, member = divmod(j, local_members)
                value = state_refs[piece][member, span, lanes]
                place = piece + odd * (1 - 2 * (piece % 2))
                for k in range(local_members):
                    term = splats[(place * local_members + member) * local_members + k] * value
                    totals[k] = term if totals[k] is None else totals[k] + term
            for k in range(local_members):
                staged[k, span, lanes] = totals[k]
        place = pl.ds(8 * block, 8)
        copy = pltpu.make_async_copy(staged.at[:, place], out.at[:, place], sems.at[block])
        copy.start()
        copies.append(copy)
    for copy in copies:
        copy.wait()


def is_paired(n_dom, n_ens):
    return n_dom == 4 and n_ens % 2 == 0


def spread(values, n_dom, n_ens):
    if not is_paired(n_dom, n_ens):
        return [values[0]] + [
            lax.ppermute(values[s], "dom", [(d, (d + s) % n_dom) for d in range(n_dom)])
            for s in range(1, n_dom)
        ]
    here, near, far = values
    pairs = []
    for d in range(n_dom):
        for e in range(n_ens):
            pairs.append((d * n_ens + e, (d ^ (3 if e % 2 else 1)) * n_ens + e))
    near = lax.ppermute(near, ("dom", "ens"), pairs)
    far = lax.ppermute(far, "dom", [(d, d ^ 2) for d in range(n_dom)])
    other = lax.ppermute(near, "ens", [(e, e ^ 1) for e in range(n_ens)])
    return [here, near, far, other]


def gather_members(state, n_ens):
    pieces = {0: state}
    if n_ens & (n_ens - 1):
        for shift in range(1, n_ens):
            pairs = [(e, (e + shift) % n_ens) for e in range(n_ens)]
            pieces[shift] = lax.ppermute(state, "ens", pairs)
        return [pieces[key] for key in range(n_ens)]
    bit = n_ens >> 1
    while bit:
        for key in list(pieces):
            pairs = [(e, e ^ bit) for e in range(n_ens)]
            pieces[key ^ bit] = lax.ppermute(pieces[key], "ens", pairs)
        bit >>= 1
    return [pieces[key] for key in range(n_ens)]


def make_on_device(n_dom, n_ens):
    vmem = pl.BlockSpec(memory_space=pltpu.VMEM)
    hbm = pl.BlockSpec(memory_space=pltpu.HBM)
    direct = n_dom <= DIRECT_DOM
    paired = is_paired(n_dom, n_ens)
    limit = VMEM_LIMIT if direct else None

    def call(kernel, out_shape, operands, specs=None, scratch=(), out_spec=vmem):
        many = isinstance(out_shape, (list, tuple))
        return pl.pallas_call(
            kernel,
            out_shape=out_shape,
            in_specs=specs or [vmem] * len(operands),
            out_specs=[out_spec] * len(out_shape) if many else out_spec,
            scratch_shapes=list(scratch),
            compiler_params=pltpu.CompilerParams(vmem_limit_bytes=limit),
        )(*operands)

    def in_hbm(value):
        return pltpu.with_memory_space_constraint(value, pltpu.HBM)

    def shape(dims, dtype=F32):
        return jax.ShapeDtypeStruct(dims, dtype)

    def on_device(state, coords, owner_local, counts, obs_value, obs_weight):
        local_members, elements, nodes = state.shape
        slots = coords.shape[1]
        members = local_members * n_ens
        tile_shape = (8, 2 * CAP)
        inputs = [state, counts, coords, owner_local[None], obs_value[None], obs_weight[None]]
        own, *tiles = call(
            lambda *refs: pack_kernel(direct, paired, *refs),
            [shape(state.shape)]
            + (
                [shape(tile_shape)] * (3 if paired else n_dom)
                if direct
                else [shape((n_dom,) + tile_shape)]
            ),
            [in_hbm(value) for value in inputs],
            [hbm] * len(inputs),
            [
                pltpu.SMEM(counts.shape, jnp.int32),
                pltpu.VMEM(coords.shape, F32),
                pltpu.VMEM((1, slots), jnp.int32),
                pltpu.VMEM((1, slots), F32),
                pltpu.VMEM((1, slots), F32),
                pltpu.VMEM((8, slots), F32),
                pltpu.SemaphoreType.DMA(()),
                pltpu.SemaphoreType.DMA((5,)),
            ],
        )
        if direct:
            tiles = spread(tiles, n_dom, n_ens)
        else:
            moved = lax.all_to_all(tiles[0], "dom", split_axis=0, concat_axis=0, tiled=True)
            tiles = [moved[d] for d in range(n_dom)]
        pieces = gather_members(state, n_ens)
        pieces[0] = own
        sensor_count = CAP * (n_dom + n_dom % 2)
        early = n_ens - 1
        sensors, high, low, values = call(
            lambda *refs: values_kernel(n_dom, *refs),
            [
                shape((8, sensor_count)),
                shape((nodes, sensor_count), BF16),
                shape((nodes, sensor_count), BF16),
                shape((early * local_members, sensor_count)),
            ],
            list(tiles) + pieces[:early],
        )
        partial_sum = call(
            lambda *refs: cross_kernel(paired, *refs),
            shape((members, LANES)),
            [sensors, high, low, values] + pieces[early:],
        )
        if direct:
            sums = spread([partial_sum] * (3 if paired else n_dom), n_dom, n_ens)
        else:
            sums = [lax.psum(partial_sum, "dom")]
        return call(
            lambda *refs: mix_kernel(paired, len(sums), *refs),
            shape(state.shape),
            sums + pieces,
            None,
            [
                pltpu.VMEM(state.shape, F32),
                pltpu.VMEM((members * local_members, 8, 128), F32),
                pltpu.SemaphoreType.DMA((elements // 8,)),
            ],
            hbm,
        )

    return on_device


def solution(mesh):
    n_dom, n_ens = mesh.shape["dom"], mesh.shape["ens"]
    return jax.shard_map(
        make_on_device(n_dom, n_ens),
        mesh=mesh,
        in_specs=(
            P("ens", ("groups", "dom"), None),
            P(None, ("groups", "dom")),
            P(("groups", "dom")),
            P(("groups", "dom"), None),
            P(("groups", "dom")),
            P(("groups", "dom")),
        ),
        out_specs=P("ens", ("groups", "dom"), None),
        check_vma=False,
    )
```

```python
import jax
import jax.numpy as jnp
from jax import lax
from jax.experimental import pallas as pl
from jax.experimental.pallas import tpu as pltpu
from jax.sharding import PartitionSpec as P


CAP = 64
NS_ITERS = 8


GLL_POINTS = (
    -1.0,
    -0.8717401485096066,
    -0.5917001814331423,
    -0.2092992179024789,
    0.2092992179024789,
    0.5917001814331423,
    0.8717401485096066,
    1.0,
)
INFLATION = 1.1
ORDER = len(GLL_POINTS)
F32 = jnp.float32
BF16 = jnp.bfloat16
DIRECT_DOM = 8
VMEM_LIMIT = 8 * 1024 * 1024
LANES = 128
PROJECT_LANES = 8
TRACE_LANE = 64


def lagrange_scale(index):
    product = 1.0
    for other in range(ORDER):
        if other != index:
            product *= GLL_POINTS[index] - GLL_POINTS[other]
    return 1.0 / product


def lagrange_rows(position):
    shape = (ORDER, position.shape[1])
    node = lax.broadcasted_iota(jnp.int32, shape, 0)
    product = jnp.full(shape, lagrange_scale(0), F32)
    for index in range(1, ORDER):
        product = jnp.where(node == index, lagrange_scale(index), product)
    for other in range(ORDER):
        product = product * jnp.where(node == other, 1.0, position - GLL_POINTS[other])
    return product


def split(value):
    high = value.astype(BF16)
    low = (value - high.astype(F32)).astype(BF16)
    return high, low


def is_odd(halves):
    return lax.rem(lax.axis_index("ens"), 2) if halves else 0


def pack_kernel(direct, paired, state, counts, coords, owner, obs, weight, *rest):
    own, outs = rest[0], rest[1:-8]
    count_box, coord_box, owner_box, obs_box, weight_box, block, state_sem, sems = rest[-8:]
    state_copy = pltpu.make_async_copy(state, own, state_sem)
    pairs = zip(
        (counts, coords, owner, obs, weight), (count_box, coord_box, owner_box, obs_box, weight_box)
    )
    copies = [
        pltpu.make_async_copy(source, target, sems.at[index])
        for index, (source, target) in enumerate(pairs)
    ]
    for copy in copies:
        copy.start()
    state_copy.start()
    n_dom = counts.shape[1]
    slots = coords.shape[1]
    here = lax.axis_index("dom")
    block[...] = jnp.zeros(block.shape, F32)
    column = lax.broadcasted_iota(jnp.int32, (8, 2 * CAP), 1)
    for copy in copies:
        copy.wait()
    block[0:3, :] = coord_box[...]
    block[3:4, :] = owner_box[...].astype(F32)
    block[4:5, :] = obs_box[...]
    block[5:6, :] = weight_box[...]
    rows = block[...]

    def tile(target, half):
        start = jnp.int32(0)
        for other in range(n_dom):
            start = start + jnp.where(other < target, count_box[0, other], 0)
        count = count_box[0, target]
        turned = pltpu.roll(rows, lax.rem(half - start + slots, slots), axis=1)[:, : 2 * CAP]
        return jnp.where((column >= half) & (column < half + count), turned, 0.0)

    if paired:
        near = jnp.where(is_odd(paired) == 0, 1, 3)
        for out, bits, half in zip(outs, (0, near, 2), (0, CAP, 0)):
            out[...] = tile(jnp.bitwise_xor(here, bits), half)
    elif direct:
        for shift in range(n_dom):
            outs[shift][...] = tile(lax.rem(here + shift, n_dom), (shift % 2) * CAP)
    else:
        half = lax.rem(here, 2) * CAP

        def step(target, carry):
            outs[0][target] = tile(target, half)
            return carry

        lax.fori_loop(0, n_dom, step, 0)
    state_copy.wait()


def pick(refs, sensors, high, low):
    members, elements, nodes = refs[0].shape
    rows = jnp.concatenate([ref[...].reshape(members * elements, nodes) for ref in refs], axis=0)
    rows_high, rows_low = split(rows)
    both = jnp.dot(
        jnp.concatenate([rows_high, rows_low], axis=0), high, preferred_element_type=F32
    )
    partial = (
        both[: rows.shape[0]]
        + both[rows.shape[0] :]
        + jnp.dot(rows_high, low, preferred_element_type=F32)
    )
    ids = lax.broadcasted_iota(jnp.int32, (elements, sensors.shape[1]), 0).astype(F32)
    partial = partial.reshape(len(refs) * members, elements, partial.shape[1])
    return jnp.sum(jnp.where((ids == sensors[3:4, :])[None], partial, 0.0), axis=1)


def values_kernel(paired, tile_count, *refs):
    tiles, state_refs = refs[:tile_count], refs[tile_count:-4]
    sensors_out, high_out, low_out, values_out = refs[-4:]
    blocks = [ref[...] for ref in tiles]
    if paired:
        here, near, far, other = blocks
        odd = is_odd(paired) == 1
        blocks = [here, jnp.where(odd, other, near), far, jnp.where(odd, near, other)]
    pairs = []
    for first in range(0, tile_count, 2):
        pair = blocks[first]
        if first + 1 < tile_count:
            pair = pair + blocks[first + 1]
        pairs.append(pair)
    sensors = jnp.concatenate(pairs, axis=1) if len(pairs) > 1 else pairs[0]
    sensors_out[...] = sensors
    along_r = lagrange_rows(sensors[0:1, :])
    along_s = lagrange_rows(sensors[1:2, :])
    along_t = lagrange_rows(sensors[2:3, :])
    for t in range(ORDER):
        for s in range(0, ORDER, 2):
            rows = [along_r * (along_t[t : t + 1, :] * along_s[k : k + 1, :]) for k in (s, s + 1)]
            high, low = split(jnp.concatenate(rows, axis=0))
            base = ORDER * ORDER * t + ORDER * s
            high_out[base : base + 2 * ORDER, :] = high
            low_out[base : base + 2 * ORDER, :] = low
    values_out[...] = pick(state_refs, sensors, high_out[...], low_out[...])


def reach_kernel(sensors_ref, high_ref, low_ref, values_ref, *refs):
    state_refs, out = refs[:-1], refs[-1]
    first = values_ref.shape[0]
    out[:first, :] = values_ref[...]
    out[first:, :] = pick(state_refs, sensors_ref[...], high_ref[...], low_ref[...])


def cross_kernel(halves, sensors_ref, *refs):
    value_refs, out = refs[:-1], refs[-1]
    sensors = sensors_ref[...]
    values = jnp.concatenate([ref[...] for ref in value_refs], axis=0)
    total = values.shape[0]
    if halves:
        turned = jnp.concatenate([ref[...] for ref in value_refs[::-1]], axis=0)
        values = jnp.where(is_odd(halves) == 1, turned, values)
    mean_value = jnp.sum(values, axis=0, keepdims=True) * (1.0 / total)
    anomaly = values - mean_value
    weighted = anomaly * sensors[5:6, :]
    innovation = sensors[4:5, :] - mean_value
    pad = jnp.zeros((PROJECT_LANES - 1, values.shape[1]), F32)
    right = jnp.concatenate([anomaly, innovation, pad], axis=0)
    left_high, left_low = split(weighted)
    right_high, right_low = split(right)
    across = (((1,), (1,)), ((), ()))
    both = lax.dot_general(
        jnp.concatenate([left_high, left_low], axis=0),
        right_high,
        across,
        preferred_element_type=F32,
    )
    out[:, : total + PROJECT_LANES] = (
        both[:total]
        + both[total:]
        + lax.dot_general(left_high, right_low, across, preferred_element_type=F32)
    )
    trace_part = jnp.sum(jnp.sum(weighted * anomaly, axis=0, keepdims=True), axis=1, keepdims=True)
    out[:, TRACE_LANE:] = jnp.broadcast_to(trace_part, (total, LANES - TRACE_LANE))


def lane_gather(value, lanes):
    return jnp.take_along_axis(value, lanes, axis=1, mode="promise_in_bounds")


def sublane_total(value):
    for shift in (4, 2, 1):
        value = value + pltpu.roll(value, shift, axis=0)
    return value


def mix_kernel(halves, sum_count, *refs):
    sums, state_refs = refs[:sum_count], refs[sum_count:-4]
    out, staged, splats, sems = refs[-4:]
    local_members, elements, nodes = out.shape
    members = local_members * len(state_refs)
    tile = (8, LANES)
    sub = lax.broadcasted_iota(jnp.int32, tile, 0)
    lane = lax.broadcasted_iota(jnp.int32, tile, 1)
    left_lanes = [(lane // members) * members + (sub + 8 * g) for g in range(2)]
    right_lanes = sub * members + lane % members
    identity = [(lane // members + 8 * h == lane % members).astype(F32) for h in range(2)]

    def as_left(matrix):
        return [[lane_gather(matrix[h], left_lanes[g]) for g in range(2)] for h in range(2)]

    def as_right(matrix):
        return [lane_gather(matrix[g], right_lanes) for g in range(2)]

    def product(left, right):
        return [sublane_total(left[h][0] * right[0] + left[h][1] * right[1]) for h in range(2)]

    total_sum = sums[0][...]
    for ref in sums[1:]:
        total_sum = total_sum + ref[...]
    rows = [total_sum[8 * g : 8 * g + 8, :] for g in range(2)]
    project = [lane_gather(rows[g], jnp.full(tile, members, jnp.int32)) for g in range(2)]
    trace_value = lane_gather(rows[0], jnp.full(tile, TRACE_LANE, jnp.int32))
    scale = 1.0 / (trace_value + members * ((members - 1) / INFLATION))
    diagonal = (members - 1) / INFLATION
    unit_left = [[(lane // members + 8 * h == sub + 8 * g).astype(F32) for g in range(2)] for h in range(2)]
    unit_right = [(lane % members == sub + 8 * g).astype(F32) for g in range(2)]
    system_left = [
        [
            (lane_gather(rows[g], lane // members + 8 * h) + diagonal * unit_left[h][g]) * scale
            for g in range(2)
        ]
        for h in range(2)
    ]
    system_right = [
        (lane_gather(rows[g], lane % members) + diagonal * unit_right[g]) * scale for g in range(2)
    ]
    inverse_left = [
        [1.5 * unit_left[h][g] - 0.5 * system_left[h][g] for g in range(2)] for h in range(2)
    ]
    inverse_right = [1.5 * unit_right[g] - 0.5 * system_right[g] for g in range(2)]
    iterate = product(system_left, inverse_right)
    for sweep in range(1, NS_ITERS):
        step = product(inverse_left, as_right(iterate))
        middle = [1.5 * identity[h] - 0.5 * step[h] for h in range(2)]
        middle_left = as_left(middle)
        inverse_root = product(middle_left, inverse_right)
        if sweep + 1 < NS_ITERS:
            iterate = product(as_left(iterate), as_right(middle))
            inverse_left, inverse_right = as_left(inverse_root), as_right(inverse_root)
        else:
            solved = product(middle_left, as_right(product(inverse_left, project)))
    mean_weights = product(as_left(inverse_root), as_right(solved))
    root_scale = jnp.sqrt((members - 1) * scale)
    transform = [inverse_root[h] * root_scale + mean_weights[h] * scale for h in range(2)]
    transform_right = as_right(transform)
    column_mean = sublane_total(transform_right[0] + transform_right[1]) * (1.0 / members)
    mixing = [transform[h] - column_mean + 1.0 / members for h in range(2)]
    odd = is_odd(halves)
    order = key_order(len(state_refs))
    own_place = odd * order.index(1) if halves else 0
    for k in range(local_members):
        lanes = sub * members + (k + local_members * own_place)
        for h in range(2):
            column = lane_gather(mixing[h], lanes)
            for i in range(8):
                splats[(8 * h + i) * local_members + k] = jnp.broadcast_to(column[i : i + 1, :], tile)
    places = []
    for piece in range(len(state_refs)):
        place = order.index(piece)
        places.append(place + odd * (order.index(piece ^ 1) - place) if halves else place)
    copies = []
    for block in range(elements // 8):
        span = slice(8 * block, 8 * block + 8)
        for first in range(0, nodes, 2 * LANES):
            spans = [slice(first + LANES * u, first + LANES * (u + 1)) for u in range(2)]
            totals = [[None, None] for _ in range(local_members)]
            for j in range(members):
                piece, member = divmod(j, local_members)
                values = [state_refs[piece][member, span, lanes] for lanes in spans]
                for k in range(local_members):
                    factor = splats[(places[piece] * local_members + member) * local_members + k]
                    for u in range(2):
                        term = factor * values[u]
                        totals[k][u] = term if j == 0 else totals[k][u] + term
            for k in range(local_members):
                for u in range(2):
                    staged[k, span, spans[u]] = totals[k][u]
        place = pl.ds(8 * block, 8)
        copy = pltpu.make_async_copy(staged.at[:, place], out.at[:, place], sems.at[block])
        copy.start()
        copies.append(copy)
    for copy in copies:
        copy.wait()


def has_halves(n_ens):
    return n_ens > 1 and n_ens & (n_ens - 1) == 0


def is_paired(n_dom, n_ens):
    return n_dom == 4 and has_halves(n_ens)


def key_order(n_ens):
    if not has_halves(n_ens):
        return list(range(n_ens))
    return list(range(0, n_ens, 2)) + list(range(1, n_ens, 2))


def spread(values, n_dom, n_ens):
    if not is_paired(n_dom, n_ens):
        return [values[0]] + [
            lax.ppermute(values[s], "dom", [(d, (d + s) % n_dom) for d in range(n_dom)])
            for s in range(1, n_dom)
        ]
    here, near, far = values
    pairs = []
    for d in range(n_dom):
        for e in range(n_ens):
            pairs.append((d * n_ens + e, (d ^ (3 if e % 2 else 1)) * n_ens + e))
    near = lax.ppermute(near, ("dom", "ens"), pairs)
    far = lax.ppermute(far, "dom", [(d, d ^ 2) for d in range(n_dom)])
    other = lax.ppermute(near, "ens", [(e, e ^ 1) for e in range(n_ens)])
    return [here, near, far, other]


def gather_members(state, own, n_ens):
    pieces = {0: state}
    if not has_halves(n_ens):
        for shift in range(1, n_ens):
            pairs = [(e, (e + shift) % n_ens) for e in range(n_ens)]
            pieces[shift] = lax.ppermute(state, "ens", pairs)
        pieces[0] = own
        return pieces
    bit = n_ens >> 1
    while bit:
        pairs = [(e, e ^ bit) for e in range(n_ens)]
        for key in list(pieces):
            pieces[key ^ bit] = lax.ppermute(pieces[key], "ens", pairs)
        bit >>= 1
        if bit == 1:
            pieces[0] = own
    pieces[0] = own
    return pieces


def make_on_device(n_dom, n_ens):
    vmem = pl.BlockSpec(memory_space=pltpu.VMEM)
    hbm = pl.BlockSpec(memory_space=pltpu.HBM)
    direct = n_dom <= DIRECT_DOM
    paired = is_paired(n_dom, n_ens)
    halves = has_halves(n_ens)
    limit = VMEM_LIMIT if direct else None

    def call(kernel, out_shape, operands, specs=None, scratch=(), out_spec=vmem):
        many = isinstance(out_shape, (list, tuple))
        return pl.pallas_call(
            kernel,
            out_shape=out_shape,
            in_specs=specs or [vmem] * len(operands),
            out_specs=[out_spec] * len(out_shape) if many else out_spec,
            scratch_shapes=list(scratch),
            compiler_params=pltpu.CompilerParams(vmem_limit_bytes=limit),
        )(*operands)

    def in_hbm(value):
        return pltpu.with_memory_space_constraint(value, pltpu.HBM)

    def shape(dims, dtype=F32):
        return jax.ShapeDtypeStruct(dims, dtype)

    def on_device(state, coords, owner_local, counts, obs_value, obs_weight):
        local_members, elements, nodes = state.shape
        slots = coords.shape[1]
        members = local_members * n_ens
        tile_shape = (8, 2 * CAP)
        inputs = [state, counts, coords, owner_local[None], obs_value[None], obs_weight[None]]
        own, *tiles = call(
            lambda *refs: pack_kernel(direct, paired, *refs),
            [shape(state.shape)]
            + (
                [shape(tile_shape)] * (3 if paired else n_dom)
                if direct
                else [shape((n_dom,) + tile_shape)]
            ),
            [in_hbm(value) for value in inputs],
            [hbm] * len(inputs),
            [
                pltpu.SMEM(counts.shape, jnp.int32),
                pltpu.VMEM(coords.shape, F32),
                pltpu.VMEM((1, slots), jnp.int32),
                pltpu.VMEM((1, slots), F32),
                pltpu.VMEM((1, slots), F32),
                pltpu.VMEM((8, slots), F32),
                pltpu.SemaphoreType.DMA(()),
                pltpu.SemaphoreType.DMA((5,)),
            ],
        )
        if direct:
            tiles = spread(tiles, n_dom, n_ens)
        else:
            moved = lax.all_to_all(tiles[0], "dom", split_axis=0, concat_axis=0, tiled=True)
            tiles = [moved[d] for d in range(n_dom)]
        pieces = gather_members(state, own, n_ens)
        sensor_count = CAP * (n_dom + n_dom % 2)
        order = key_order(n_ens)
        local = order[: n_ens // 2] if halves else order
        sensors, high, low, values = call(
            lambda *refs: values_kernel(paired, n_dom, *refs),
            [
                shape((8, sensor_count)),
                shape((nodes, sensor_count), BF16),
                shape((nodes, sensor_count), BF16),
                shape((local_members, sensor_count)),
            ],
            list(tiles) + [pieces[0]],
        )
        if len(local) > 1:
            values = call(
                reach_kernel,
                shape((len(local) * local_members, sensor_count)),
                [sensors, high, low, values] + [pieces[key] for key in local[1:]],
            )
        values = [values]
        if halves:
            pairs = [(e, e ^ 1) for e in range(n_ens)]
            values.append(lax.ppermute(values[0], "ens", pairs))
        partial_sum = call(
            lambda *refs: cross_kernel(halves, *refs), shape((members, LANES)), [sensors] + values
        )
        if direct:
            sums = spread([partial_sum] * (3 if paired else n_dom), n_dom, n_ens)
        else:
            sums = [lax.psum(partial_sum, "dom")]
        return call(
            lambda *refs: mix_kernel(halves, len(sums), *refs),
            shape(state.shape),
            sums + [pieces[key] for key in range(n_ens)],
            None,
            [
                pltpu.VMEM(state.shape, F32),
                pltpu.VMEM((members * local_members, 8, 128), F32),
                pltpu.SemaphoreType.DMA((elements // 8,)),
            ],
            hbm,
        )

    return on_device


def solution(mesh):
    n_dom, n_ens = mesh.shape["dom"], mesh.shape["ens"]
    return jax.shard_map(
        make_on_device(n_dom, n_ens),
        mesh=mesh,
        in_specs=(
            P("ens", ("groups", "dom"), None),
            P(None, ("groups", "dom")),
            P(("groups", "dom")),
            P(("groups", "dom"), None),
            P(("groups", "dom")),
            P(("groups", "dom")),
        ),
        out_specs=P("ens", ("groups", "dom"), None),
        check_vma=False,
    )
```

```python
import jax
import jax.numpy as jnp
from jax import lax
from jax.experimental import pallas as pl
from jax.experimental.pallas import tpu as pltpu
from jax.sharding import PartitionSpec as P


CAP = 64
NS_ITERS = 8


GLL_POINTS = (
    -1.0,
    -0.8717401485096066,
    -0.5917001814331423,
    -0.2092992179024789,
    0.2092992179024789,
    0.5917001814331423,
    0.8717401485096066,
    1.0,
)
INFLATION = 1.1
ORDER = len(GLL_POINTS)
F32 = jnp.float32
BF16 = jnp.bfloat16
DIRECT_DOM = 8
VMEM_LIMIT = 8 * 1024 * 1024
LANES = 128
PROJECT_LANES = 8
TRACE_LANE = 64


def lagrange_scale(index):
    product = 1.0
    for other in range(ORDER):
        if other != index:
            product *= GLL_POINTS[index] - GLL_POINTS[other]
    return 1.0 / product


def lagrange_rows(position):
    shape = (ORDER, position.shape[1])
    node = lax.broadcasted_iota(jnp.int32, shape, 0)
    product = jnp.full(shape, lagrange_scale(0), F32)
    for index in range(1, ORDER):
        product = jnp.where(node == index, lagrange_scale(index), product)
    for other in range(ORDER):
        product = product * jnp.where(node == other, 1.0, position - GLL_POINTS[other])
    return product


def split(value):
    high = value.astype(BF16)
    low = (value - high.astype(F32)).astype(BF16)
    return high, low


def is_odd(halves):
    return lax.rem(lax.axis_index("ens"), 2) if halves else 0


def fetch_kernel(state, own, sem):
    copy = pltpu.make_async_copy(state, own, sem)
    copy.start()
    copy.wait()


def pack_kernel(direct, paired, counts, coords, owner, obs, weight, *rest):
    outs = rest[:-7]
    count_box, coord_box, owner_box, obs_box, weight_box, block, sems = rest[-7:]
    pairs = zip(
        (counts, coords, owner, obs, weight), (count_box, coord_box, owner_box, obs_box, weight_box)
    )
    copies = [
        pltpu.make_async_copy(source, target, sems.at[index])
        for index, (source, target) in enumerate(pairs)
    ]
    for copy in copies:
        copy.start()
    n_dom = counts.shape[1]
    slots = coords.shape[1]
    here = lax.axis_index("dom")
    block[...] = jnp.zeros(block.shape, F32)
    column = lax.broadcasted_iota(jnp.int32, (8, 2 * CAP), 1)
    for copy in copies:
        copy.wait()
    block[0:3, :] = coord_box[...]
    block[3:4, :] = owner_box[...].astype(F32)
    block[4:5, :] = obs_box[...]
    block[5:6, :] = weight_box[...]
    rows = block[...]

    def tile(target, half):
        start = jnp.int32(0)
        for other in range(n_dom):
            start = start + jnp.where(other < target, count_box[0, other], 0)
        count = count_box[0, target]
        turned = pltpu.roll(rows, lax.rem(half - start + slots, slots), axis=1)[:, : 2 * CAP]
        return jnp.where((column >= half) & (column < half + count), turned, 0.0)

    if paired:
        near = jnp.where(is_odd(paired) == 0, 1, 3)
        for out, bits, half in zip(outs, (0, near, 2), (0, CAP, 0)):
            out[...] = tile(jnp.bitwise_xor(here, bits), half)
    elif direct:
        for shift in range(n_dom):
            outs[shift][...] = tile(lax.rem(here + shift, n_dom), (shift % 2) * CAP)
    else:
        half = lax.rem(here, 2) * CAP

        def step(target, carry):
            outs[0][target] = tile(target, half)
            return carry

        lax.fori_loop(0, n_dom, step, 0)


def pick(refs, sensors, high, low):
    members, elements, nodes = refs[0].shape
    rows = jnp.concatenate([ref[...].reshape(members * elements, nodes) for ref in refs], axis=0)
    rows_high, rows_low = split(rows)
    both = jnp.dot(
        jnp.concatenate([rows_high, rows_low], axis=0), high, preferred_element_type=F32
    )
    partial = (
        both[: rows.shape[0]]
        + both[rows.shape[0] :]
        + jnp.dot(rows_high, low, preferred_element_type=F32)
    )
    ids = lax.broadcasted_iota(jnp.int32, (elements, sensors.shape[1]), 0).astype(F32)
    partial = partial.reshape(len(refs) * members, elements, partial.shape[1])
    return jnp.sum(jnp.where((ids == sensors[3:4, :])[None], partial, 0.0), axis=1)


def values_kernel(paired, tile_count, *refs):
    tiles, state_refs = refs[:tile_count], refs[tile_count:-4]
    sensors_out, high_out, low_out, values_out = refs[-4:]
    blocks = [ref[...] for ref in tiles]
    if paired:
        here, near, far, other = blocks
        odd = is_odd(paired) == 1
        blocks = [here, jnp.where(odd, other, near), far, jnp.where(odd, near, other)]
    pairs = []
    for first in range(0, tile_count, 2):
        pair = blocks[first]
        if first + 1 < tile_count:
            pair = pair + blocks[first + 1]
        pairs.append(pair)
    sensors = jnp.concatenate(pairs, axis=1) if len(pairs) > 1 else pairs[0]
    sensors_out[...] = sensors
    along_r = lagrange_rows(sensors[0:1, :])
    along_s = lagrange_rows(sensors[1:2, :])
    along_t = lagrange_rows(sensors[2:3, :])
    for t in range(ORDER):
        for s in range(0, ORDER, 2):
            rows = [along_r * (along_t[t : t + 1, :] * along_s[k : k + 1, :]) for k in (s, s + 1)]
            high, low = split(jnp.concatenate(rows, axis=0))
            base = ORDER * ORDER * t + ORDER * s
            high_out[base : base + 2 * ORDER, :] = high
            low_out[base : base + 2 * ORDER, :] = low
    values_out[...] = pick(state_refs, sensors, high_out[...], low_out[...])


def reach_kernel(sensors_ref, high_ref, low_ref, values_ref, *refs):
    state_refs, out = refs[:-1], refs[-1]
    first = values_ref.shape[0]
    out[:first, :] = values_ref[...]
    out[first:, :] = pick(state_refs, sensors_ref[...], high_ref[...], low_ref[...])


def cross_kernel(halves, sensors_ref, *refs):
    value_refs, out = refs[:-1], refs[-1]
    sensors = sensors_ref[...]
    values = jnp.concatenate([ref[...] for ref in value_refs], axis=0)
    total = values.shape[0]
    if halves:
        turned = jnp.concatenate([ref[...] for ref in value_refs[::-1]], axis=0)
        values = jnp.where(is_odd(halves) == 1, turned, values)
    mean_value = jnp.sum(values, axis=0, keepdims=True) * (1.0 / total)
    anomaly = values - mean_value
    weighted = anomaly * sensors[5:6, :]
    innovation = sensors[4:5, :] - mean_value
    pad = jnp.zeros((PROJECT_LANES - 1, values.shape[1]), F32)
    right = jnp.concatenate([anomaly, innovation, pad], axis=0)
    left_high, left_low = split(weighted)
    right_high, right_low = split(right)
    across = (((1,), (1,)), ((), ()))
    both = lax.dot_general(
        jnp.concatenate([left_high, left_low], axis=0),
        right_high,
        across,
        preferred_element_type=F32,
    )
    out[:, : total + PROJECT_LANES] = (
        both[:total]
        + both[total:]
        + lax.dot_general(left_high, right_low, across, preferred_element_type=F32)
    )
    trace_part = jnp.sum(jnp.sum(weighted * anomaly, axis=0, keepdims=True), axis=1, keepdims=True)
    out[:, TRACE_LANE:] = jnp.broadcast_to(trace_part, (total, LANES - TRACE_LANE))


def lane_gather(value, lanes):
    return jnp.take_along_axis(value, lanes, axis=1, mode="promise_in_bounds")


def sublane_total(value):
    for shift in (4, 2, 1):
        value = value + pltpu.roll(value, shift, axis=0)
    return value


def mix_kernel(halves, sum_count, *refs):
    sums, state_refs = refs[:sum_count], refs[sum_count:-4]
    out, staged, splats, sems = refs[-4:]
    local_members, elements, nodes = out.shape
    members = local_members * len(state_refs)
    tile = (8, LANES)
    sub = lax.broadcasted_iota(jnp.int32, tile, 0)
    lane = lax.broadcasted_iota(jnp.int32, tile, 1)
    left_lanes = [(lane // members) * members + (sub + 8 * g) for g in range(2)]
    right_lanes = sub * members + lane % members
    identity = [(lane // members + 8 * h == lane % members).astype(F32) for h in range(2)]

    def as_left(matrix):
        return [[lane_gather(matrix[h], left_lanes[g]) for g in range(2)] for h in range(2)]

    def as_right(matrix):
        return [lane_gather(matrix[g], right_lanes) for g in range(2)]

    def product(left, right):
        return [sublane_total(left[h][0] * right[0] + left[h][1] * right[1]) for h in range(2)]

    total_sum = sums[0][...]
    for ref in sums[1:]:
        total_sum = total_sum + ref[...]
    rows = [total_sum[8 * g : 8 * g + 8, :] for g in range(2)]
    project = [lane_gather(rows[g], jnp.full(tile, members, jnp.int32)) for g in range(2)]
    trace_value = lane_gather(rows[0], jnp.full(tile, TRACE_LANE, jnp.int32))
    scale = 1.0 / (trace_value + members * ((members - 1) / INFLATION))
    diagonal = (members - 1) / INFLATION
    unit_left = [[(lane // members + 8 * h == sub + 8 * g).astype(F32) for g in range(2)] for h in range(2)]
    unit_right = [(lane % members == sub + 8 * g).astype(F32) for g in range(2)]
    system_left = [
        [
            (lane_gather(rows[g], lane // members + 8 * h) + diagonal * unit_left[h][g]) * scale
            for g in range(2)
        ]
        for h in range(2)
    ]
    system_right = [
        (lane_gather(rows[g], lane % members) + diagonal * unit_right[g]) * scale for g in range(2)
    ]
    inverse_left = [
        [1.5 * unit_left[h][g] - 0.5 * system_left[h][g] for g in range(2)] for h in range(2)
    ]
    inverse_right = [1.5 * unit_right[g] - 0.5 * system_right[g] for g in range(2)]
    iterate = product(system_left, inverse_right)
    for sweep in range(1, NS_ITERS):
        step = product(inverse_left, as_right(iterate))
        middle = [1.5 * identity[h] - 0.5 * step[h] for h in range(2)]
        middle_left = as_left(middle)
        inverse_root = product(middle_left, inverse_right)
        if sweep + 1 < NS_ITERS:
            iterate = product(as_left(iterate), as_right(middle))
            inverse_left, inverse_right = as_left(inverse_root), as_right(inverse_root)
        else:
            solved = product(middle_left, as_right(product(inverse_left, project)))
    mean_weights = product(as_left(inverse_root), as_right(solved))
    root_scale = jnp.sqrt((members - 1) * scale)
    transform = [inverse_root[h] * root_scale + mean_weights[h] * scale for h in range(2)]
    transform_right = as_right(transform)
    column_mean = sublane_total(transform_right[0] + transform_right[1]) * (1.0 / members)
    mixing = [transform[h] - column_mean + 1.0 / members for h in range(2)]
    odd = is_odd(halves)
    order = key_order(len(state_refs))
    own_place = odd * order.index(1) if halves else 0
    for k in range(local_members):
        lanes = sub * members + (k + local_members * own_place)
        for h in range(2):
            column = lane_gather(mixing[h], lanes)
            for i in range(8):
                splats[(8 * h + i) * local_members + k] = jnp.broadcast_to(column[i : i + 1, :], tile)
    places = []
    for piece in range(len(state_refs)):
        place = order.index(piece)
        places.append(place + odd * (order.index(piece ^ 1) - place) if halves else place)
    copies = []
    for block in range(elements // 8):
        span = slice(8 * block, 8 * block + 8)
        for first in range(0, nodes, 2 * LANES):
            spans = [slice(first + LANES * u, first + LANES * (u + 1)) for u in range(2)]
            totals = [[None, None] for _ in range(local_members)]
            for j in range(members):
                piece, member = divmod(j, local_members)
                values = [state_refs[piece][member, span, lanes] for lanes in spans]
                for k in range(local_members):
                    factor = splats[(places[piece] * local_members + member) * local_members + k]
                    for u in range(2):
                        term = factor * values[u]
                        totals[k][u] = term if j == 0 else totals[k][u] + term
            for k in range(local_members):
                for u in range(2):
                    staged[k, span, spans[u]] = totals[k][u]
        place = pl.ds(8 * block, 8)
        copy = pltpu.make_async_copy(staged.at[:, place], out.at[:, place], sems.at[block])
        copy.start()
        copies.append(copy)
    for copy in copies:
        copy.wait()


def has_halves(n_ens):
    return n_ens > 1 and n_ens & (n_ens - 1) == 0


def is_paired(n_dom, n_ens):
    return n_dom == 4 and has_halves(n_ens)


def key_order(n_ens):
    if not has_halves(n_ens):
        return list(range(n_ens))
    return list(range(0, n_ens, 2)) + list(range(1, n_ens, 2))


def spread(values, n_dom, n_ens):
    if not is_paired(n_dom, n_ens):
        return [values[0]] + [
            lax.ppermute(values[s], "dom", [(d, (d + s) % n_dom) for d in range(n_dom)])
            for s in range(1, n_dom)
        ]
    here, near, far = values
    pairs, cross = [], []
    for d in range(n_dom):
        for e in range(n_ens):
            pairs.append((d * n_ens + e, (d ^ (3 if e % 2 else 1)) * n_ens + e))
            cross.append((d * n_ens + e, (d ^ 2) * n_ens + (e ^ 1)))
    near = lax.ppermute(near, ("dom", "ens"), pairs)
    far = lax.ppermute(far, ("dom", "ens"), cross)
    other = lax.ppermute(near, "ens", [(e, e ^ 1) for e in range(n_ens)])
    return [here, near, far, other]


def gather_members(state, own, n_ens):
    pieces = {0: state}
    if not has_halves(n_ens):
        for shift in range(1, n_ens):
            pairs = [(e, (e + shift) % n_ens) for e in range(n_ens)]
            pieces[shift] = lax.ppermute(state, "ens", pairs)
        pieces[0] = own
        return pieces
    bit = n_ens >> 1
    while bit:
        pairs = [(e, e ^ bit) for e in range(n_ens)]
        for key in list(pieces):
            pieces[key ^ bit] = lax.ppermute(pieces[key], "ens", pairs)
        bit >>= 1
        if bit == 1:
            pieces[0] = own
    pieces[0] = own
    return pieces


def make_on_device(n_dom, n_ens):
    vmem = pl.BlockSpec(memory_space=pltpu.VMEM)
    hbm = pl.BlockSpec(memory_space=pltpu.HBM)
    direct = n_dom <= DIRECT_DOM
    paired = is_paired(n_dom, n_ens)
    halves = has_halves(n_ens)
    limit = VMEM_LIMIT if direct else None

    def call(kernel, out_shape, operands, specs=None, scratch=(), out_spec=vmem):
        many = isinstance(out_shape, (list, tuple))
        return pl.pallas_call(
            kernel,
            out_shape=out_shape,
            in_specs=specs or [vmem] * len(operands),
            out_specs=[out_spec] * len(out_shape) if many else out_spec,
            scratch_shapes=list(scratch),
            compiler_params=pltpu.CompilerParams(vmem_limit_bytes=limit),
        )(*operands)

    def in_hbm(value):
        return pltpu.with_memory_space_constraint(value, pltpu.HBM)

    def shape(dims, dtype=F32):
        return jax.ShapeDtypeStruct(dims, dtype)

    def on_device(state, coords, owner_local, counts, obs_value, obs_weight):
        local_members, elements, nodes = state.shape
        slots = coords.shape[1]
        members = local_members * n_ens
        tile_shape = (8, 2 * CAP)
        inputs = [counts, coords, owner_local[None], obs_value[None], obs_weight[None]]
        tiles = call(
            lambda *refs: pack_kernel(direct, paired, *refs),
            [shape(tile_shape)] * (3 if paired else n_dom)
            if direct
            else [shape((n_dom,) + tile_shape)],
            [in_hbm(value) for value in inputs],
            [hbm] * len(inputs),
            [
                pltpu.SMEM(counts.shape, jnp.int32),
                pltpu.VMEM(coords.shape, F32),
                pltpu.VMEM((1, slots), jnp.int32),
                pltpu.VMEM((1, slots), F32),
                pltpu.VMEM((1, slots), F32),
                pltpu.VMEM((8, slots), F32),
                pltpu.SemaphoreType.DMA((5,)),
            ],
        )
        if direct:
            tiles = spread(tiles, n_dom, n_ens)
        else:
            moved = lax.all_to_all(tiles[0], "dom", split_axis=0, concat_axis=0, tiled=True)
            tiles = [moved[d] for d in range(n_dom)]
        own = call(
            fetch_kernel, shape(state.shape), [in_hbm(state)], [hbm], [pltpu.SemaphoreType.DMA(())]
        )
        pieces = gather_members(state, own, n_ens)
        sensor_count = CAP * (n_dom + n_dom % 2)
        order = key_order(n_ens)
        local = order[: n_ens // 2] if halves else order
        sensors, high, low, values = call(
            lambda *refs: values_kernel(paired, n_dom, *refs),
            [
                shape((8, sensor_count)),
                shape((nodes, sensor_count), BF16),
                shape((nodes, sensor_count), BF16),
                shape((local_members, sensor_count)),
            ],
            list(tiles) + [pieces[0]],
        )
        if len(local) > 1:
            values = call(
                reach_kernel,
                shape((len(local) * local_members, sensor_count)),
                [sensors, high, low, values] + [pieces[key] for key in local[1:]],
            )
        values = [values]
        if halves:
            pairs = [(e, e ^ 1) for e in range(n_ens)]
            values.append(lax.ppermute(values[0], "ens", pairs))
        partial_sum = call(
            lambda *refs: cross_kernel(halves, *refs), shape((members, LANES)), [sensors] + values
        )
        if direct:
            sums = spread([partial_sum] * (3 if paired else n_dom), n_dom, n_ens)
        else:
            sums = [lax.psum(partial_sum, "dom")]
        return call(
            lambda *refs: mix_kernel(halves, len(sums), *refs),
            shape(state.shape),
            sums + [pieces[key] for key in range(n_ens)],
            None,
            [
                pltpu.VMEM(state.shape, F32),
                pltpu.VMEM((members * local_members, 8, 128), F32),
                pltpu.SemaphoreType.DMA((elements // 8,)),
            ],
            hbm,
        )

    return on_device


def solution(mesh):
    n_dom, n_ens = mesh.shape["dom"], mesh.shape["ens"]
    return jax.shard_map(
        make_on_device(n_dom, n_ens),
        mesh=mesh,
        in_specs=(
            P("ens", ("groups", "dom"), None),
            P(None, ("groups", "dom")),
            P(("groups", "dom")),
            P(("groups", "dom"), None),
            P(("groups", "dom")),
            P(("groups", "dom")),
        ),
        out_specs=P("ens", ("groups", "dom"), None),
        check_vma=False,
    )
```

```python
import jax
import jax.numpy as jnp
from jax import lax
from jax.experimental import pallas as pl
from jax.experimental.pallas import tpu as pltpu
from jax.sharding import PartitionSpec as P


CAP = 64
NS_ITERS = 8


GLL_POINTS = (
    -1.0,
    -0.8717401485096066,
    -0.5917001814331423,
    -0.2092992179024789,
    0.2092992179024789,
    0.5917001814331423,
    0.8717401485096066,
    1.0,
)
INFLATION = 1.1
ORDER = len(GLL_POINTS)
F32 = jnp.float32
BF16 = jnp.bfloat16
DIRECT_DOM = 8
VMEM_LIMIT = 8 * 1024 * 1024
LANES = 128
PROJECT_LANES = 8
TRACE_LANE = 64


def lagrange_scale(index):
    product = 1.0
    for other in range(ORDER):
        if other != index:
            product *= GLL_POINTS[index] - GLL_POINTS[other]
    return 1.0 / product


def lagrange_rows(position):
    shape = (ORDER, position.shape[1])
    node = lax.broadcasted_iota(jnp.int32, shape, 0)
    product = jnp.full(shape, lagrange_scale(0), F32)
    for index in range(1, ORDER):
        product = jnp.where(node == index, lagrange_scale(index), product)
    for other in range(ORDER):
        product = product * jnp.where(node == other, 1.0, position - GLL_POINTS[other])
    return product


def split(value):
    high = value.astype(BF16)
    low = (value - high.astype(F32)).astype(BF16)
    return high, low


def is_odd(halves):
    return lax.rem(lax.axis_index("ens"), 2) if halves else 0


def fetch_kernel(state, own, sem):
    copy = pltpu.make_async_copy(state, own, sem)
    copy.start()
    copy.wait()


def pack_kernel(direct, paired, counts, coords, owner, obs, weight, *rest):
    outs = rest[:-7]
    count_box, coord_box, owner_box, obs_box, weight_box, block, sems = rest[-7:]
    pairs = zip(
        (counts, coords, owner, obs, weight), (count_box, coord_box, owner_box, obs_box, weight_box)
    )
    copies = [
        pltpu.make_async_copy(source, target, sems.at[index])
        for index, (source, target) in enumerate(pairs)
    ]
    for copy in copies:
        copy.start()
    n_dom = counts.shape[1]
    slots = coords.shape[1]
    here = lax.axis_index("dom")
    block[...] = jnp.zeros(block.shape, F32)
    column = lax.broadcasted_iota(jnp.int32, (8, 2 * CAP), 1)
    for copy in copies:
        copy.wait()
    block[0:3, :] = coord_box[...]
    block[3:4, :] = owner_box[...].astype(F32)
    block[4:5, :] = obs_box[...]
    block[5:6, :] = weight_box[...]
    rows = block[...]

    def tile(target, half):
        start = jnp.int32(0)
        for other in range(n_dom):
            start = start + jnp.where(other < target, count_box[0, other], 0)
        count = count_box[0, target]
        turned = pltpu.roll(rows, lax.rem(half - start + slots, slots), axis=1)[:, : 2 * CAP]
        return jnp.where((column >= half) & (column < half + count), turned, 0.0)

    if paired:
        near = jnp.where(is_odd(paired) == 0, 1, 3)
        for out, bits, half in zip(outs, (0, near, 2), (0, CAP, 0)):
            out[...] = tile(jnp.bitwise_xor(here, bits), half)
    elif direct:
        for shift in range(n_dom):
            outs[shift][...] = tile(lax.rem(here + shift, n_dom), (shift % 2) * CAP)
    else:
        half = lax.rem(here, 2) * CAP

        def step(target, carry):
            outs[0][target] = tile(target, half)
            return carry

        lax.fori_loop(0, n_dom, step, 0)


def pick(refs, sensors, high, low):
    members, elements, nodes = refs[0].shape
    rows = jnp.concatenate([ref[...].reshape(members * elements, nodes) for ref in refs], axis=0)
    rows_high, rows_low = split(rows)
    both = jnp.dot(
        jnp.concatenate([rows_high, rows_low], axis=0), high, preferred_element_type=F32
    )
    partial = (
        both[: rows.shape[0]]
        + both[rows.shape[0] :]
        + jnp.dot(rows_high, low, preferred_element_type=F32)
    )
    ids = lax.broadcasted_iota(jnp.int32, (elements, sensors.shape[1]), 0).astype(F32)
    partial = partial.reshape(len(refs) * members, elements, partial.shape[1])
    return jnp.sum(jnp.where((ids == sensors[3:4, :])[None], partial, 0.0), axis=1)


def values_kernel(paired, tile_count, *refs):
    tiles, state_refs = refs[:tile_count], refs[tile_count:-4]
    sensors_out, high_out, low_out, values_out = refs[-4:]
    blocks = [ref[...] for ref in tiles]
    if paired:
        here, near, far, other = blocks
        odd = is_odd(paired) == 1
        blocks = [here, jnp.where(odd, other, near), far, jnp.where(odd, near, other)]
    pairs = []
    for first in range(0, tile_count, 2):
        pair = blocks[first]
        if first + 1 < tile_count:
            pair = pair + blocks[first + 1]
        pairs.append(pair)
    sensors = jnp.concatenate(pairs, axis=1) if len(pairs) > 1 else pairs[0]
    sensors_out[...] = sensors
    along_r = lagrange_rows(sensors[0:1, :])
    along_s = lagrange_rows(sensors[1:2, :])
    along_t = lagrange_rows(sensors[2:3, :])
    for t in range(ORDER):
        for s in range(0, ORDER, 2):
            rows = [along_r * (along_t[t : t + 1, :] * along_s[k : k + 1, :]) for k in (s, s + 1)]
            high, low = split(jnp.concatenate(rows, axis=0))
            base = ORDER * ORDER * t + ORDER * s
            high_out[base : base + 2 * ORDER, :] = high
            low_out[base : base + 2 * ORDER, :] = low
    values_out[...] = pick(state_refs, sensors, high_out[...], low_out[...])


def reach_kernel(sensors_ref, high_ref, low_ref, values_ref, *refs):
    state_refs, out = refs[:-1], refs[-1]
    first = values_ref.shape[0]
    out[:first, :] = values_ref[...]
    out[first:, :] = pick(state_refs, sensors_ref[...], high_ref[...], low_ref[...])


def cross_kernel(halves, sensors_ref, *refs):
    value_refs, out = refs[:-1], refs[-1]
    sensors = sensors_ref[...]
    values = jnp.concatenate([ref[...] for ref in value_refs], axis=0)
    total = values.shape[0]
    if halves:
        turned = jnp.concatenate([ref[...] for ref in value_refs[::-1]], axis=0)
        values = jnp.where(is_odd(halves) == 1, turned, values)
    mean_value = jnp.sum(values, axis=0, keepdims=True) * (1.0 / total)
    anomaly = values - mean_value
    weighted = anomaly * sensors[5:6, :]
    innovation = sensors[4:5, :] - mean_value
    pad = jnp.zeros((PROJECT_LANES - 1, values.shape[1]), F32)
    right = jnp.concatenate([anomaly, innovation, pad], axis=0)
    left_high, left_low = split(weighted)
    right_high, right_low = split(right)
    across = (((1,), (1,)), ((), ()))
    both = lax.dot_general(
        jnp.concatenate([left_high, left_low], axis=0),
        right_high,
        across,
        preferred_element_type=F32,
    )
    out[:, : total + PROJECT_LANES] = (
        both[:total]
        + both[total:]
        + lax.dot_general(left_high, right_low, across, preferred_element_type=F32)
    )
    trace_part = jnp.sum(jnp.sum(weighted * anomaly, axis=0, keepdims=True), axis=1, keepdims=True)
    out[:, TRACE_LANE:] = jnp.broadcast_to(trace_part, (total, LANES - TRACE_LANE))


def lane_gather(value, lanes):
    return jnp.take_along_axis(value, lanes, axis=1, mode="promise_in_bounds")


def sublane_total(value):
    for shift in (4, 2, 1):
        value = value + pltpu.roll(value, shift, axis=0)
    return value


def mix_kernel(halves, sum_count, *refs):
    sums, state_refs = refs[:sum_count], refs[sum_count:-4]
    out, staged, splats, sems = refs[-4:]
    local_members, elements, nodes = out.shape
    members = local_members * len(state_refs)
    tile = (8, LANES)
    sub = lax.broadcasted_iota(jnp.int32, tile, 0)
    lane = lax.broadcasted_iota(jnp.int32, tile, 1)
    left_lanes = [(lane // members) * members + (sub + 8 * g) for g in range(2)]
    right_lanes = sub * members + lane % members
    identity = [(lane // members + 8 * h == lane % members).astype(F32) for h in range(2)]

    def as_left(matrix):
        return [[lane_gather(matrix[h], left_lanes[g]) for g in range(2)] for h in range(2)]

    def as_right(matrix):
        return [lane_gather(matrix[g], right_lanes) for g in range(2)]

    def product(left, right):
        return [sublane_total(left[h][0] * right[0] + left[h][1] * right[1]) for h in range(2)]

    total_sum = sums[0][...]
    for ref in sums[1:]:
        total_sum = total_sum + ref[...]
    rows = [total_sum[8 * g : 8 * g + 8, :] for g in range(2)]
    project = [lane_gather(rows[g], jnp.full(tile, members, jnp.int32)) for g in range(2)]
    trace_value = lane_gather(rows[0], jnp.full(tile, TRACE_LANE, jnp.int32))
    scale = 1.0 / (trace_value + members * ((members - 1) / INFLATION))
    diagonal = (members - 1) / INFLATION
    unit_left = [[(lane // members + 8 * h == sub + 8 * g).astype(F32) for g in range(2)] for h in range(2)]
    unit_right = [(lane % members == sub + 8 * g).astype(F32) for g in range(2)]
    system_left = [
        [
            (lane_gather(rows[g], lane // members + 8 * h) + diagonal * unit_left[h][g]) * scale
            for g in range(2)
        ]
        for h in range(2)
    ]
    system_right = [
        (lane_gather(rows[g], lane % members) + diagonal * unit_right[g]) * scale for g in range(2)
    ]
    inverse_left = [
        [1.5 * unit_left[h][g] - 0.5 * system_left[h][g] for g in range(2)] for h in range(2)
    ]
    inverse_right = [1.5 * unit_right[g] - 0.5 * system_right[g] for g in range(2)]
    iterate = product(system_left, inverse_right)
    for sweep in range(1, NS_ITERS):
        step = product(inverse_left, as_right(iterate))
        middle = [1.5 * identity[h] - 0.5 * step[h] for h in range(2)]
        middle_left = as_left(middle)
        inverse_root = product(middle_left, inverse_right)
        if sweep + 1 < NS_ITERS:
            iterate = product(as_left(iterate), as_right(middle))
            inverse_left, inverse_right = as_left(inverse_root), as_right(inverse_root)
        else:
            solved = product(middle_left, as_right(product(inverse_left, project)))
    mean_weights = product(as_left(inverse_root), as_right(solved))
    root_scale = jnp.sqrt((members - 1) * scale)
    transform = [inverse_root[h] * root_scale + mean_weights[h] * scale for h in range(2)]
    transform_right = as_right(transform)
    column_mean = sublane_total(transform_right[0] + transform_right[1]) * (1.0 / members)
    mixing = [transform[h] - column_mean + 1.0 / members for h in range(2)]
    odd = is_odd(halves)
    order = key_order(len(state_refs))
    own_place = odd * order.index(1) if halves else 0
    for k in range(local_members):
        lanes = sub * members + (k + local_members * own_place)
        for h in range(2):
            column = lane_gather(mixing[h], lanes)
            for i in range(8):
                splats[(8 * h + i) * local_members + k] = jnp.broadcast_to(column[i : i + 1, :], tile)
    places = []
    for piece in range(len(state_refs)):
        place = order.index(piece)
        places.append(place + odd * (order.index(piece ^ 1) - place) if halves else place)
    copies = []
    for block in range(elements // 8):
        span = slice(8 * block, 8 * block + 8)
        for first in range(0, nodes, 2 * LANES):
            spans = [slice(first + LANES * u, first + LANES * (u + 1)) for u in range(2)]
            totals = [[None, None] for _ in range(local_members)]
            for j in range(members):
                piece, member = divmod(j, local_members)
                values = [state_refs[piece][member, span, lanes] for lanes in spans]
                for k in range(local_members):
                    factor = splats[(places[piece] * local_members + member) * local_members + k]
                    for u in range(2):
                        term = factor * values[u]
                        totals[k][u] = term if j == 0 else totals[k][u] + term
            for k in range(local_members):
                for u in range(2):
                    staged[k, span, spans[u]] = totals[k][u]
        place = pl.ds(8 * block, 8)
        copy = pltpu.make_async_copy(staged.at[:, place], out.at[:, place], sems.at[block])
        copy.start()
        copies.append(copy)
    for copy in copies:
        copy.wait()


def has_halves(n_ens):
    return n_ens > 1 and n_ens & (n_ens - 1) == 0


def is_paired(n_dom, n_ens):
    return n_dom == 4 and has_halves(n_ens)


def key_order(n_ens):
    if not has_halves(n_ens):
        return list(range(n_ens))
    return list(range(0, n_ens, 2)) + list(range(1, n_ens, 2))


def spread(values, n_dom, n_ens):
    if not is_paired(n_dom, n_ens):
        return [values[0]] + [
            lax.ppermute(values[s], "dom", [(d, (d + s) % n_dom) for d in range(n_dom)])
            for s in range(1, n_dom)
        ]
    here, near, far = values
    pairs = []
    for d in range(n_dom):
        for e in range(n_ens):
            pairs.append((d * n_ens + e, (d ^ (3 if e % 2 else 1)) * n_ens + e))
    near = lax.ppermute(near, ("dom", "ens"), pairs)
    far = lax.ppermute(far, "dom", [(d, d ^ 2) for d in range(n_dom)])
    other = lax.ppermute(near, "ens", [(e, e ^ 1) for e in range(n_ens)])
    return [here, near, far, other]


def gather_members(state, own, n_ens):
    pieces = {0: state}
    if not has_halves(n_ens):
        for shift in range(1, n_ens):
            pairs = [(e, (e + shift) % n_ens) for e in range(n_ens)]
            pieces[shift] = lax.ppermute(state, "ens", pairs)
        pieces[0] = own
        return pieces
    bit = n_ens >> 1
    while bit:
        pairs = [(e, e ^ bit) for e in range(n_ens)]
        for key in list(pieces):
            pieces[key ^ bit] = lax.ppermute(pieces[key], "ens", pairs)
        bit >>= 1
        if bit == 1:
            pieces[0] = own
    pieces[0] = own
    return pieces


def make_on_device(n_dom, n_ens):
    vmem = pl.BlockSpec(memory_space=pltpu.VMEM)
    hbm = pl.BlockSpec(memory_space=pltpu.HBM)
    direct = n_dom <= DIRECT_DOM
    paired = is_paired(n_dom, n_ens)
    halves = has_halves(n_ens)
    limit = VMEM_LIMIT if direct else None

    def call(kernel, out_shape, operands, specs=None, scratch=(), out_spec=vmem):
        many = isinstance(out_shape, (list, tuple))
        return pl.pallas_call(
            kernel,
            out_shape=out_shape,
            in_specs=specs or [vmem] * len(operands),
            out_specs=[out_spec] * len(out_shape) if many else out_spec,
            scratch_shapes=list(scratch),
            compiler_params=pltpu.CompilerParams(vmem_limit_bytes=limit),
        )(*operands)

    def in_hbm(value):
        return pltpu.with_memory_space_constraint(value, pltpu.HBM)

    def shape(dims, dtype=F32):
        return jax.ShapeDtypeStruct(dims, dtype)

    def on_device(state, coords, owner_local, counts, obs_value, obs_weight):
        local_members, elements, nodes = state.shape
        slots = coords.shape[1]
        members = local_members * n_ens
        tile_shape = (8, 2 * CAP)
        inputs = [counts, coords, owner_local[None], obs_value[None], obs_weight[None]]
        tiles = call(
            lambda *refs: pack_kernel(direct, paired, *refs),
            [shape(tile_shape)] * (3 if paired else n_dom)
            if direct
            else [shape((n_dom,) + tile_shape)],
            [in_hbm(value) for value in inputs],
            [hbm] * len(inputs),
            [
                pltpu.SMEM(counts.shape, jnp.int32),
                pltpu.VMEM(coords.shape, F32),
                pltpu.VMEM((1, slots), jnp.int32),
                pltpu.VMEM((1, slots), F32),
                pltpu.VMEM((1, slots), F32),
                pltpu.VMEM((8, slots), F32),
                pltpu.SemaphoreType.DMA((5,)),
            ],
        )
        if direct:
            tiles = spread(tiles, n_dom, n_ens)
        else:
            moved = lax.all_to_all(tiles[0], "dom", split_axis=0, concat_axis=0, tiled=True)
            tiles = [moved[d] for d in range(n_dom)]
        own = call(
            fetch_kernel, shape(state.shape), [in_hbm(state)], [hbm], [pltpu.SemaphoreType.DMA(())]
        )
        pieces = gather_members(state, own, n_ens)
        sensor_count = CAP * (n_dom + n_dom % 2)
        order = key_order(n_ens)
        local = order[: n_ens // 2] if halves else order
        sensors, high, low, values = call(
            lambda *refs: values_kernel(paired, n_dom, *refs),
            [
                shape((8, sensor_count)),
                shape((nodes, sensor_count), BF16),
                shape((nodes, sensor_count), BF16),
                shape((local_members, sensor_count)),
            ],
            list(tiles) + [pieces[0]],
        )
        if len(local) > 1:
            values = call(
                reach_kernel,
                shape((len(local) * local_members, sensor_count)),
                [sensors, high, low, values] + [pieces[key] for key in local[1:]],
            )
        values = [values]
        if halves:
            pairs = [(e, e ^ 1) for e in range(n_ens)]
            values.append(lax.ppermute(values[0], "ens", pairs))
        partial_sum = call(
            lambda *refs: cross_kernel(halves, *refs), shape((members, LANES)), [sensors] + values
        )
        if direct:
            sums = spread([partial_sum] * (3 if paired else n_dom), n_dom, n_ens)
        else:
            sums = [lax.psum(partial_sum, "dom")]
        return call(
            lambda *refs: mix_kernel(halves, len(sums), *refs),
            shape(state.shape),
            sums + [pieces[key] for key in range(n_ens)],
            None,
            [
                pltpu.VMEM(state.shape, F32),
                pltpu.VMEM((members * local_members, 8, 128), F32),
                pltpu.SemaphoreType.DMA((elements // 8,)),
            ],
            hbm,
        )

    return on_device


def solution(mesh):
    n_dom, n_ens = mesh.shape["dom"], mesh.shape["ens"]
    return jax.shard_map(
        make_on_device(n_dom, n_ens),
        mesh=mesh,
        in_specs=(
            P("ens", ("groups", "dom"), None),
            P(None, ("groups", "dom")),
            P(("groups", "dom")),
            P(("groups", "dom"), None),
            P(("groups", "dom")),
            P(("groups", "dom")),
        ),
        out_specs=P("ens", ("groups", "dom"), None),
        check_vma=False,
    )
```

```python
import jax
import jax.numpy as jnp
from jax import lax
from jax.experimental import pallas as pl
from jax.experimental.pallas import tpu as pltpu
from jax.sharding import PartitionSpec as P


CAP = 64
NS_ITERS = 8


GLL_POINTS = (
    -1.0,
    -0.8717401485096066,
    -0.5917001814331423,
    -0.2092992179024789,
    0.2092992179024789,
    0.5917001814331423,
    0.8717401485096066,
    1.0,
)
INFLATION = 1.1
ORDER = len(GLL_POINTS)
F32 = jnp.float32
BF16 = jnp.bfloat16
DIRECT_DOM = 8
VMEM_LIMIT = 8 * 1024 * 1024
LANES = 128
PROJECT_LANES = 8
TRACE_LANE = 64


def lagrange_scale(index):
    product = 1.0
    for other in range(ORDER):
        if other != index:
            product *= GLL_POINTS[index] - GLL_POINTS[other]
    return 1.0 / product


def lagrange_rows(position):
    shape = (ORDER, position.shape[1])
    node = lax.broadcasted_iota(jnp.int32, shape, 0)
    product = jnp.full(shape, lagrange_scale(0), F32)
    for index in range(1, ORDER):
        product = jnp.where(node == index, lagrange_scale(index), product)
    for other in range(ORDER):
        product = product * jnp.where(node == other, 1.0, position - GLL_POINTS[other])
    return product


def split(value):
    high = value.astype(BF16)
    low = (value - high.astype(F32)).astype(BF16)
    return high, low


def is_odd(halves):
    return lax.rem(lax.axis_index("ens"), 2) if halves else 0


def fetch_kernel(state, own, sem):
    copy = pltpu.make_async_copy(state, own, sem)
    copy.start()
    copy.wait()


def pack_kernel(direct, paired, counts, coords, owner, obs, weight, *rest):
    outs = rest[:-7]
    count_box, coord_box, owner_box, obs_box, weight_box, block, sems = rest[-7:]
    pairs = zip(
        (counts, coords, owner, obs, weight), (count_box, coord_box, owner_box, obs_box, weight_box)
    )
    copies = [
        pltpu.make_async_copy(source, target, sems.at[index])
        for index, (source, target) in enumerate(pairs)
    ]
    for copy in copies:
        copy.start()
    n_dom = counts.shape[1]
    slots = coords.shape[1]
    here = lax.axis_index("dom")
    block[...] = jnp.zeros(block.shape, F32)
    column = lax.broadcasted_iota(jnp.int32, (8, 2 * CAP), 1)
    for copy in copies:
        copy.wait()
    block[0:3, :] = coord_box[...]
    block[3:4, :] = owner_box[...].astype(F32)
    block[4:5, :] = obs_box[...]
    block[5:6, :] = weight_box[...]
    rows = block[...]

    def tile(target, half):
        start = jnp.int32(0)
        for other in range(n_dom):
            start = start + jnp.where(other < target, count_box[0, other], 0)
        count = count_box[0, target]
        turned = pltpu.roll(rows, lax.rem(half - start + slots, slots), axis=1)[:, : 2 * CAP]
        return jnp.where((column >= half) & (column < half + count), turned, 0.0)

    if paired:
        near = jnp.where(is_odd(paired) == 0, 1, 2)
        for out, bits, half in zip(outs, (0, near, 3), (0, CAP, 0)):
            out[...] = tile(jnp.bitwise_xor(here, bits), half)
    elif direct:
        for shift in range(n_dom):
            outs[shift][...] = tile(lax.rem(here + shift, n_dom), (shift % 2) * CAP)
    else:
        half = lax.rem(here, 2) * CAP

        def step(target, carry):
            outs[0][target] = tile(target, half)
            return carry

        lax.fori_loop(0, n_dom, step, 0)


def pick(refs, sensors, high, low):
    members, elements, nodes = refs[0].shape
    rows = jnp.concatenate([ref[...].reshape(members * elements, nodes) for ref in refs], axis=0)
    rows_high, rows_low = split(rows)
    both = jnp.dot(
        jnp.concatenate([rows_high, rows_low], axis=0), high, preferred_element_type=F32
    )
    partial = (
        both[: rows.shape[0]]
        + both[rows.shape[0] :]
        + jnp.dot(rows_high, low, preferred_element_type=F32)
    )
    ids = lax.broadcasted_iota(jnp.int32, (elements, sensors.shape[1]), 0).astype(F32)
    partial = partial.reshape(len(refs) * members, elements, partial.shape[1])
    return jnp.sum(jnp.where((ids == sensors[3:4, :])[None], partial, 0.0), axis=1)


def values_kernel(paired, tile_count, *refs):
    tiles, state_refs = refs[:tile_count], refs[tile_count:-4]
    sensors_out, high_out, low_out, values_out = refs[-4:]
    blocks = [ref[...] for ref in tiles]
    if paired:
        here, near, far, other = blocks
        odd = is_odd(paired) == 1
        blocks = [here, jnp.where(odd, other, near), far, jnp.where(odd, near, other)]
    pairs = []
    for first in range(0, tile_count, 2):
        pair = blocks[first]
        if first + 1 < tile_count:
            pair = pair + blocks[first + 1]
        pairs.append(pair)
    sensors = jnp.concatenate(pairs, axis=1) if len(pairs) > 1 else pairs[0]
    sensors_out[...] = sensors
    along_r = lagrange_rows(sensors[0:1, :])
    along_s = lagrange_rows(sensors[1:2, :])
    along_t = lagrange_rows(sensors[2:3, :])
    for t in range(ORDER):
        for s in range(0, ORDER, 2):
            rows = [along_r * (along_t[t : t + 1, :] * along_s[k : k + 1, :]) for k in (s, s + 1)]
            high, low = split(jnp.concatenate(rows, axis=0))
            base = ORDER * ORDER * t + ORDER * s
            high_out[base : base + 2 * ORDER, :] = high
            low_out[base : base + 2 * ORDER, :] = low
    values_out[...] = pick(state_refs, sensors, high_out[...], low_out[...])


def reach_kernel(sensors_ref, high_ref, low_ref, values_ref, *refs):
    state_refs, out = refs[:-1], refs[-1]
    first = values_ref.shape[0]
    out[:first, :] = values_ref[...]
    out[first:, :] = pick(state_refs, sensors_ref[...], high_ref[...], low_ref[...])


def cross_kernel(halves, sensors_ref, *refs):
    value_refs, out = refs[:-1], refs[-1]
    sensors = sensors_ref[...]
    values = jnp.concatenate([ref[...] for ref in value_refs], axis=0)
    total = values.shape[0]
    if halves:
        turned = jnp.concatenate([ref[...] for ref in value_refs[::-1]], axis=0)
        values = jnp.where(is_odd(halves) == 1, turned, values)
    mean_value = jnp.sum(values, axis=0, keepdims=True) * (1.0 / total)
    anomaly = values - mean_value
    weighted = anomaly * sensors[5:6, :]
    innovation = sensors[4:5, :] - mean_value
    pad = jnp.zeros((PROJECT_LANES - 1, values.shape[1]), F32)
    right = jnp.concatenate([anomaly, innovation, pad], axis=0)
    left_high, left_low = split(weighted)
    right_high, right_low = split(right)
    across = (((1,), (1,)), ((), ()))
    both = lax.dot_general(
        jnp.concatenate([left_high, left_low], axis=0),
        right_high,
        across,
        preferred_element_type=F32,
    )
    out[:, : total + PROJECT_LANES] = (
        both[:total]
        + both[total:]
        + lax.dot_general(left_high, right_low, across, preferred_element_type=F32)
    )
    trace_part = jnp.sum(jnp.sum(weighted * anomaly, axis=0, keepdims=True), axis=1, keepdims=True)
    out[:, TRACE_LANE:] = jnp.broadcast_to(trace_part, (total, LANES - TRACE_LANE))


def lane_gather(value, lanes):
    return jnp.take_along_axis(value, lanes, axis=1, mode="promise_in_bounds")


def sublane_total(value):
    for shift in (4, 2, 1):
        value = value + pltpu.roll(value, shift, axis=0)
    return value


def mix_kernel(halves, sum_count, *refs):
    sums, state_refs = refs[:sum_count], refs[sum_count:-4]
    out, staged, splats, sems = refs[-4:]
    local_members, elements, nodes = out.shape
    members = local_members * len(state_refs)
    tile = (8, LANES)
    sub = lax.broadcasted_iota(jnp.int32, tile, 0)
    lane = lax.broadcasted_iota(jnp.int32, tile, 1)
    left_lanes = [(lane // members) * members + (sub + 8 * g) for g in range(2)]
    right_lanes = sub * members + lane % members
    identity = [(lane // members + 8 * h == lane % members).astype(F32) for h in range(2)]

    def as_left(matrix):
        return [[lane_gather(matrix[h], left_lanes[g]) for g in range(2)] for h in range(2)]

    def as_right(matrix):
        return [lane_gather(matrix[g], right_lanes) for g in range(2)]

    def product(left, right):
        return [sublane_total(left[h][0] * right[0] + left[h][1] * right[1]) for h in range(2)]

    total_sum = sums[0][...]
    for ref in sums[1:]:
        total_sum = total_sum + ref[...]
    rows = [total_sum[8 * g : 8 * g + 8, :] for g in range(2)]
    project = [lane_gather(rows[g], jnp.full(tile, members, jnp.int32)) for g in range(2)]
    trace_value = lane_gather(rows[0], jnp.full(tile, TRACE_LANE, jnp.int32))
    scale = 1.0 / (trace_value + members * ((members - 1) / INFLATION))
    diagonal = (members - 1) / INFLATION
    unit_left = [[(lane // members + 8 * h == sub + 8 * g).astype(F32) for g in range(2)] for h in range(2)]
    unit_right = [(lane % members == sub + 8 * g).astype(F32) for g in range(2)]
    system_left = [
        [
            (lane_gather(rows[g], lane // members + 8 * h) + diagonal * unit_left[h][g]) * scale
            for g in range(2)
        ]
        for h in range(2)
    ]
    system_right = [
        (lane_gather(rows[g], lane % members) + diagonal * unit_right[g]) * scale for g in range(2)
    ]
    inverse_left = [
        [1.5 * unit_left[h][g] - 0.5 * system_left[h][g] for g in range(2)] for h in range(2)
    ]
    inverse_right = [1.5 * unit_right[g] - 0.5 * system_right[g] for g in range(2)]
    iterate = product(system_left, inverse_right)
    for sweep in range(1, NS_ITERS):
        step = product(inverse_left, as_right(iterate))
        middle = [1.5 * identity[h] - 0.5 * step[h] for h in range(2)]
        middle_left = as_left(middle)
        inverse_root = product(middle_left, inverse_right)
        if sweep + 1 < NS_ITERS:
            iterate = product(as_left(iterate), as_right(middle))
            inverse_left, inverse_right = as_left(inverse_root), as_right(inverse_root)
        else:
            solved = product(middle_left, as_right(product(inverse_left, project)))
    mean_weights = product(as_left(inverse_root), as_right(solved))
    root_scale = jnp.sqrt((members - 1) * scale)
    transform = [inverse_root[h] * root_scale + mean_weights[h] * scale for h in range(2)]
    transform_right = as_right(transform)
    column_mean = sublane_total(transform_right[0] + transform_right[1]) * (1.0 / members)
    mixing = [transform[h] - column_mean + 1.0 / members for h in range(2)]
    odd = is_odd(halves)
    order = key_order(len(state_refs))
    own_place = odd * order.index(1) if halves else 0
    for k in range(local_members):
        lanes = sub * members + (k + local_members * own_place)
        for h in range(2):
            column = lane_gather(mixing[h], lanes)
            for i in range(8):
                splats[(8 * h + i) * local_members + k] = jnp.broadcast_to(column[i : i + 1, :], tile)
    places = []
    for piece in range(len(state_refs)):
        place = order.index(piece)
        places.append(place + odd * (order.index(piece ^ 1) - place) if halves else place)
    copies = []
    for block in range(elements // 8):
        span = slice(8 * block, 8 * block + 8)
        for first in range(0, nodes, 2 * LANES):
            spans = [slice(first + LANES * u, first + LANES * (u + 1)) for u in range(2)]
            totals = [[None, None] for _ in range(local_members)]
            for j in range(members):
                piece, member = divmod(j, local_members)
                values = [state_refs[piece][member, span, lanes] for lanes in spans]
                for k in range(local_members):
                    factor = splats[(places[piece] * local_members + member) * local_members + k]
                    for u in range(2):
                        term = factor * values[u]
                        totals[k][u] = term if j == 0 else totals[k][u] + term
            for k in range(local_members):
                for u in range(2):
                    staged[k, span, spans[u]] = totals[k][u]
        place = pl.ds(8 * block, 8)
        copy = pltpu.make_async_copy(staged.at[:, place], out.at[:, place], sems.at[block])
        copy.start()
        copies.append(copy)
    for copy in copies:
        copy.wait()


def has_halves(n_ens):
    return n_ens > 1 and n_ens & (n_ens - 1) == 0


def is_paired(n_dom, n_ens):
    return n_dom == 4 and has_halves(n_ens)


def key_order(n_ens):
    if not has_halves(n_ens):
        return list(range(n_ens))
    return list(range(0, n_ens, 2)) + list(range(1, n_ens, 2))


def spread(values, n_dom, n_ens):
    if not is_paired(n_dom, n_ens):
        return [values[0]] + [
            lax.ppermute(values[s], "dom", [(d, (d + s) % n_dom) for d in range(n_dom)])
            for s in range(1, n_dom)
        ]
    here, near, far = values
    pairs, cross = [], []
    for d in range(n_dom):
        for e in range(n_ens):
            pairs.append((d * n_ens + e, (d ^ (2 if e % 2 else 1)) * n_ens + e))
            cross.append((d * n_ens + e, (d ^ 3) * n_ens + (e ^ 1)))
    near = lax.ppermute(near, ("dom", "ens"), pairs)
    far = lax.ppermute(far, ("dom", "ens"), cross)
    other = lax.ppermute(near, "ens", [(e, e ^ 1) for e in range(n_ens)])
    return [here, near, far, other]


def gather_members(state, own, n_ens):
    pieces = {0: state}
    if not has_halves(n_ens):
        for shift in range(1, n_ens):
            pairs = [(e, (e + shift) % n_ens) for e in range(n_ens)]
            pieces[shift] = lax.ppermute(state, "ens", pairs)
        pieces[0] = own
        return pieces
    bit = n_ens >> 1
    while bit:
        pairs = [(e, e ^ bit) for e in range(n_ens)]
        for key in list(pieces):
            pieces[key ^ bit] = lax.ppermute(pieces[key], "ens", pairs)
        bit >>= 1
        if bit == 1:
            pieces[0] = own
    pieces[0] = own
    return pieces


def make_on_device(n_dom, n_ens):
    vmem = pl.BlockSpec(memory_space=pltpu.VMEM)
    hbm = pl.BlockSpec(memory_space=pltpu.HBM)
    direct = n_dom <= DIRECT_DOM
    paired = is_paired(n_dom, n_ens)
    halves = has_halves(n_ens)
    limit = VMEM_LIMIT if direct else None

    def call(kernel, out_shape, operands, specs=None, scratch=(), out_spec=vmem):
        many = isinstance(out_shape, (list, tuple))
        return pl.pallas_call(
            kernel,
            out_shape=out_shape,
            in_specs=specs or [vmem] * len(operands),
            out_specs=[out_spec] * len(out_shape) if many else out_spec,
            scratch_shapes=list(scratch),
            compiler_params=pltpu.CompilerParams(vmem_limit_bytes=limit),
        )(*operands)

    def in_hbm(value):
        return pltpu.with_memory_space_constraint(value, pltpu.HBM)

    def shape(dims, dtype=F32):
        return jax.ShapeDtypeStruct(dims, dtype)

    def on_device(state, coords, owner_local, counts, obs_value, obs_weight):
        local_members, elements, nodes = state.shape
        slots = coords.shape[1]
        members = local_members * n_ens
        tile_shape = (8, 2 * CAP)
        inputs = [counts, coords, owner_local[None], obs_value[None], obs_weight[None]]
        tiles = call(
            lambda *refs: pack_kernel(direct, paired, *refs),
            [shape(tile_shape)] * (3 if paired else n_dom)
            if direct
            else [shape((n_dom,) + tile_shape)],
            [in_hbm(value) for value in inputs],
            [hbm] * len(inputs),
            [
                pltpu.SMEM(counts.shape, jnp.int32),
                pltpu.VMEM(coords.shape, F32),
                pltpu.VMEM((1, slots), jnp.int32),
                pltpu.VMEM((1, slots), F32),
                pltpu.VMEM((1, slots), F32),
                pltpu.VMEM((8, slots), F32),
                pltpu.SemaphoreType.DMA((5,)),
            ],
        )
        if direct:
            tiles = spread(tiles, n_dom, n_ens)
        else:
            moved = lax.all_to_all(tiles[0], "dom", split_axis=0, concat_axis=0, tiled=True)
            tiles = [moved[d] for d in range(n_dom)]
        own = call(
            fetch_kernel, shape(state.shape), [in_hbm(state)], [hbm], [pltpu.SemaphoreType.DMA(())]
        )
        pieces = gather_members(state, own, n_ens)
        sensor_count = CAP * (n_dom + n_dom % 2)
        order = key_order(n_ens)
        local = order[: n_ens // 2] if halves else order
        sensors, high, low, values = call(
            lambda *refs: values_kernel(paired, n_dom, *refs),
            [
                shape((8, sensor_count)),
                shape((nodes, sensor_count), BF16),
                shape((nodes, sensor_count), BF16),
                shape((local_members, sensor_count)),
            ],
            list(tiles) + [pieces[0]],
        )
        if len(local) > 1:
            values = call(
                reach_kernel,
                shape((len(local) * local_members, sensor_count)),
                [sensors, high, low, values] + [pieces[key] for key in local[1:]],
            )
        values = [values]
        if halves:
            pairs = [(e, e ^ 1) for e in range(n_ens)]
            values.append(lax.ppermute(values[0], "ens", pairs))
        partial_sum = call(
            lambda *refs: cross_kernel(halves, *refs), shape((members, LANES)), [sensors] + values
        )
        if direct:
            sums = spread([partial_sum] * (3 if paired else n_dom), n_dom, n_ens)
        else:
            sums = [lax.psum(partial_sum, "dom")]
        return call(
            lambda *refs: mix_kernel(halves, len(sums), *refs),
            shape(state.shape),
            sums + [pieces[key] for key in range(n_ens)],
            None,
            [
                pltpu.VMEM(state.shape, F32),
                pltpu.VMEM((members * local_members, 8, 128), F32),
                pltpu.SemaphoreType.DMA((elements // 8,)),
            ],
            hbm,
        )

    return on_device


def solution(mesh):
    n_dom, n_ens = mesh.shape["dom"], mesh.shape["ens"]
    return jax.shard_map(
        make_on_device(n_dom, n_ens),
        mesh=mesh,
        in_specs=(
            P("ens", ("groups", "dom"), None),
            P(None, ("groups", "dom")),
            P(("groups", "dom")),
            P(("groups", "dom"), None),
            P(("groups", "dom")),
            P(("groups", "dom")),
        ),
        out_specs=P("ens", ("groups", "dom"), None),
        check_vma=False,
    )
```

```python
import jax
import jax.numpy as jnp
from jax import lax
from jax.experimental import pallas as pl
from jax.experimental.pallas import tpu as pltpu
from jax.sharding import PartitionSpec as P


CAP = 64
NS_ITERS = 8


GLL_POINTS = (
    -1.0,
    -0.8717401485096066,
    -0.5917001814331423,
    -0.2092992179024789,
    0.2092992179024789,
    0.5917001814331423,
    0.8717401485096066,
    1.0,
)
INFLATION = 1.1
ORDER = len(GLL_POINTS)
F32 = jnp.float32
BF16 = jnp.bfloat16
DIRECT_DOM = 8
VMEM_LIMIT = 8 * 1024 * 1024
LANES = 128
PROJECT_LANES = 8
TRACE_LANE = 64


def lagrange_scale(index):
    product = 1.0
    for other in range(ORDER):
        if other != index:
            product *= GLL_POINTS[index] - GLL_POINTS[other]
    return 1.0 / product


def lagrange_rows(position):
    shape = (ORDER, position.shape[1])
    node = lax.broadcasted_iota(jnp.int32, shape, 0)
    product = jnp.full(shape, lagrange_scale(0), F32)
    for index in range(1, ORDER):
        product = jnp.where(node == index, lagrange_scale(index), product)
    for other in range(ORDER):
        product = product * jnp.where(node == other, 1.0, position - GLL_POINTS[other])
    return product


def split(value):
    high = value.astype(BF16)
    low = (value - high.astype(F32)).astype(BF16)
    return high, low


def is_odd(halves):
    return lax.rem(lax.axis_index("ens"), 2) if halves else 0


def fetch_kernel(state, own, sem):
    copy = pltpu.make_async_copy(state, own, sem)
    copy.start()
    copy.wait()


def early_kernel(*refs):
    @pl.when(is_odd(True) == 1)
    def _():
        pack_kernel(True, True, *refs)


def later_kernel(early_count, *refs):
    early, refs = refs[:early_count], refs[early_count:]
    odd = is_odd(True)

    @pl.when(odd == 1)
    def _():
        for source, out in zip(early, refs[5 : 5 + early_count]):
            out[...] = source[...]

    @pl.when(odd == 0)
    def _():
        pack_kernel(True, True, *refs)


def pack_kernel(direct, paired, counts, coords, owner, obs, weight, *rest):
    outs = rest[:-7]
    count_box, coord_box, owner_box, obs_box, weight_box, block, sems = rest[-7:]
    pairs = zip(
        (counts, coords, owner, obs, weight), (count_box, coord_box, owner_box, obs_box, weight_box)
    )
    copies = [
        pltpu.make_async_copy(source, target, sems.at[index])
        for index, (source, target) in enumerate(pairs)
    ]
    for copy in copies:
        copy.start()
    n_dom = counts.shape[1]
    slots = coords.shape[1]
    here = lax.axis_index("dom")
    block[...] = jnp.zeros(block.shape, F32)
    column = lax.broadcasted_iota(jnp.int32, (8, 2 * CAP), 1)
    for copy in copies:
        copy.wait()
    block[0:3, :] = coord_box[...]
    block[3:4, :] = owner_box[...].astype(F32)
    block[4:5, :] = obs_box[...]
    block[5:6, :] = weight_box[...]
    rows = block[...]

    def tile(target, half):
        start = jnp.int32(0)
        for other in range(n_dom):
            start = start + jnp.where(other < target, count_box[0, other], 0)
        count = count_box[0, target]
        turned = pltpu.roll(rows, lax.rem(half - start + slots, slots), axis=1)[:, : 2 * CAP]
        return jnp.where((column >= half) & (column < half + count), turned, 0.0)

    if paired:
        near = jnp.where(is_odd(paired) == 0, 1, 3)
        for out, bits, half in zip(outs, (0, near, 2), (0, CAP, 0)):
            out[...] = tile(jnp.bitwise_xor(here, bits), half)
    elif direct:
        for shift in range(n_dom):
            outs[shift][...] = tile(lax.rem(here + shift, n_dom), (shift % 2) * CAP)
    else:
        half = lax.rem(here, 2) * CAP

        def step(target, carry):
            outs[0][target] = tile(target, half)
            return carry

        lax.fori_loop(0, n_dom, step, 0)


def pick(refs, sensors, high, low):
    members, elements, nodes = refs[0].shape
    rows = jnp.concatenate([ref[...].reshape(members * elements, nodes) for ref in refs], axis=0)
    rows_high, rows_low = split(rows)
    both = jnp.dot(
        jnp.concatenate([rows_high, rows_low], axis=0), high, preferred_element_type=F32
    )
    partial = (
        both[: rows.shape[0]]
        + both[rows.shape[0] :]
        + jnp.dot(rows_high, low, preferred_element_type=F32)
    )
    ids = lax.broadcasted_iota(jnp.int32, (elements, sensors.shape[1]), 0).astype(F32)
    partial = partial.reshape(len(refs) * members, elements, partial.shape[1])
    return jnp.sum(jnp.where((ids == sensors[3:4, :])[None], partial, 0.0), axis=1)


def values_kernel(paired, tile_count, *refs):
    tiles, state_refs = refs[:tile_count], refs[tile_count:-4]
    sensors_out, high_out, low_out, values_out = refs[-4:]
    blocks = [ref[...] for ref in tiles]
    if paired:
        here, near, far, other = blocks
        odd = is_odd(paired) == 1
        blocks = [here, jnp.where(odd, other, near), far, jnp.where(odd, near, other)]
    pairs = []
    for first in range(0, tile_count, 2):
        pair = blocks[first]
        if first + 1 < tile_count:
            pair = pair + blocks[first + 1]
        pairs.append(pair)
    sensors = jnp.concatenate(pairs, axis=1) if len(pairs) > 1 else pairs[0]
    sensors_out[...] = sensors
    along_r = lagrange_rows(sensors[0:1, :])
    along_s = lagrange_rows(sensors[1:2, :])
    along_t = lagrange_rows(sensors[2:3, :])
    for t in range(ORDER):
        for s in range(0, ORDER, 2):
            rows = [along_r * (along_t[t : t + 1, :] * along_s[k : k + 1, :]) for k in (s, s + 1)]
            high, low = split(jnp.concatenate(rows, axis=0))
            base = ORDER * ORDER * t + ORDER * s
            high_out[base : base + 2 * ORDER, :] = high
            low_out[base : base + 2 * ORDER, :] = low
    values_out[...] = pick(state_refs, sensors, high_out[...], low_out[...])


def reach_kernel(sensors_ref, high_ref, low_ref, values_ref, *refs):
    state_refs, out = refs[:-1], refs[-1]
    first = values_ref.shape[0]
    out[:first, :] = values_ref[...]
    out[first:, :] = pick(state_refs, sensors_ref[...], high_ref[...], low_ref[...])


def cross_kernel(halves, sensors_ref, *refs):
    value_refs, out = refs[:-1], refs[-1]
    sensors = sensors_ref[...]
    values = jnp.concatenate([ref[...] for ref in value_refs], axis=0)
    total = values.shape[0]
    if halves:
        turned = jnp.concatenate([ref[...] for ref in value_refs[::-1]], axis=0)
        values = jnp.where(is_odd(halves) == 1, turned, values)
    mean_value = jnp.sum(values, axis=0, keepdims=True) * (1.0 / total)
    anomaly = values - mean_value
    weighted = anomaly * sensors[5:6, :]
    innovation = sensors[4:5, :] - mean_value
    pad = jnp.zeros((PROJECT_LANES - 1, values.shape[1]), F32)
    right = jnp.concatenate([anomaly, innovation, pad], axis=0)
    left_high, left_low = split(weighted)
    right_high, right_low = split(right)
    across = (((1,), (1,)), ((), ()))
    both = lax.dot_general(
        jnp.concatenate([left_high, left_low], axis=0),
        right_high,
        across,
        preferred_element_type=F32,
    )
    out[:, : total + PROJECT_LANES] = (
        both[:total]
        + both[total:]
        + lax.dot_general(left_high, right_low, across, preferred_element_type=F32)
    )
    trace_part = jnp.sum(jnp.sum(weighted * anomaly, axis=0, keepdims=True), axis=1, keepdims=True)
    out[:, TRACE_LANE:] = jnp.broadcast_to(trace_part, (total, LANES - TRACE_LANE))


def lane_gather(value, lanes):
    return jnp.take_along_axis(value, lanes, axis=1, mode="promise_in_bounds")


def sublane_total(value):
    for shift in (4, 2, 1):
        value = value + pltpu.roll(value, shift, axis=0)
    return value


def mix_kernel(halves, sum_count, *refs):
    sums, state_refs = refs[:sum_count], refs[sum_count:-4]
    out, staged, splats, sems = refs[-4:]
    local_members, elements, nodes = out.shape
    members = local_members * len(state_refs)
    tile = (8, LANES)
    sub = lax.broadcasted_iota(jnp.int32, tile, 0)
    lane = lax.broadcasted_iota(jnp.int32, tile, 1)
    left_lanes = [(lane // members) * members + (sub + 8 * g) for g in range(2)]
    right_lanes = sub * members + lane % members
    identity = [(lane // members + 8 * h == lane % members).astype(F32) for h in range(2)]

    def as_left(matrix):
        return [[lane_gather(matrix[h], left_lanes[g]) for g in range(2)] for h in range(2)]

    def as_right(matrix):
        return [lane_gather(matrix[g], right_lanes) for g in range(2)]

    def product(left, right):
        return [sublane_total(left[h][0] * right[0] + left[h][1] * right[1]) for h in range(2)]

    total_sum = sums[0][...]
    for ref in sums[1:]:
        total_sum = total_sum + ref[...]
    rows = [total_sum[8 * g : 8 * g + 8, :] for g in range(2)]
    project = [lane_gather(rows[g], jnp.full(tile, members, jnp.int32)) for g in range(2)]
    trace_value = lane_gather(rows[0], jnp.full(tile, TRACE_LANE, jnp.int32))
    scale = 1.0 / (trace_value + members * ((members - 1) / INFLATION))
    diagonal = (members - 1) / INFLATION
    unit_left = [[(lane // members + 8 * h == sub + 8 * g).astype(F32) for g in range(2)] for h in range(2)]
    unit_right = [(lane % members == sub + 8 * g).astype(F32) for g in range(2)]
    system_left = [
        [
            (lane_gather(rows[g], lane // members + 8 * h) + diagonal * unit_left[h][g]) * scale
            for g in range(2)
        ]
        for h in range(2)
    ]
    system_right = [
        (lane_gather(rows[g], lane % members) + diagonal * unit_right[g]) * scale for g in range(2)
    ]
    inverse_left = [
        [1.5 * unit_left[h][g] - 0.5 * system_left[h][g] for g in range(2)] for h in range(2)
    ]
    inverse_right = [1.5 * unit_right[g] - 0.5 * system_right[g] for g in range(2)]
    iterate = product(system_left, inverse_right)
    for sweep in range(1, NS_ITERS):
        step = product(inverse_left, as_right(iterate))
        middle = [1.5 * identity[h] - 0.5 * step[h] for h in range(2)]
        middle_left = as_left(middle)
        inverse_root = product(middle_left, inverse_right)
        if sweep + 1 < NS_ITERS:
            iterate = product(as_left(iterate), as_right(middle))
            inverse_left, inverse_right = as_left(inverse_root), as_right(inverse_root)
        else:
            solved = product(middle_left, as_right(product(inverse_left, project)))
    mean_weights = product(as_left(inverse_root), as_right(solved))
    root_scale = jnp.sqrt((members - 1) * scale)
    transform = [inverse_root[h] * root_scale + mean_weights[h] * scale for h in range(2)]
    transform_right = as_right(transform)
    column_mean = sublane_total(transform_right[0] + transform_right[1]) * (1.0 / members)
    mixing = [transform[h] - column_mean + 1.0 / members for h in range(2)]
    odd = is_odd(halves)
    order = key_order(len(state_refs))
    own_place = odd * order.index(1) if halves else 0
    for k in range(local_members):
        lanes = sub * members + (k + local_members * own_place)
        for h in range(2):
            column = lane_gather(mixing[h], lanes)
            for i in range(8):
                splats[(8 * h + i) * local_members + k] = jnp.broadcast_to(column[i : i + 1, :], tile)
    places = []
    for piece in range(len(state_refs)):
        place = order.index(piece)
        places.append(place + odd * (order.index(piece ^ 1) - place) if halves else place)
    copies = []
    for block in range(elements // 8):
        span = slice(8 * block, 8 * block + 8)
        for first in range(0, nodes, 2 * LANES):
            spans = [slice(first + LANES * u, first + LANES * (u + 1)) for u in range(2)]
            totals = [[None, None] for _ in range(local_members)]
            for j in range(members):
                piece, member = divmod(j, local_members)
                values = [state_refs[piece][member, span, lanes] for lanes in spans]
                for k in range(local_members):
                    factor = splats[(places[piece] * local_members + member) * local_members + k]
                    for u in range(2):
                        term = factor * values[u]
                        totals[k][u] = term if j == 0 else totals[k][u] + term
            for k in range(local_members):
                for u in range(2):
                    staged[k, span, spans[u]] = totals[k][u]
        place = pl.ds(8 * block, 8)
        copy = pltpu.make_async_copy(staged.at[:, place], out.at[:, place], sems.at[block])
        copy.start()
        copies.append(copy)
    for copy in copies:
        copy.wait()


def has_halves(n_ens):
    return n_ens > 1 and n_ens & (n_ens - 1) == 0


def is_paired(n_dom, n_ens):
    return n_dom == 4 and has_halves(n_ens)


def key_order(n_ens):
    if not has_halves(n_ens):
        return list(range(n_ens))
    return list(range(0, n_ens, 2)) + list(range(1, n_ens, 2))


def spread(values, n_dom, n_ens):
    if not is_paired(n_dom, n_ens):
        return [values[0]] + [
            lax.ppermute(values[s], "dom", [(d, (d + s) % n_dom) for d in range(n_dom)])
            for s in range(1, n_dom)
        ]
    here, near, far = values
    pairs = []
    for d in range(n_dom):
        for e in range(n_ens):
            pairs.append((d * n_ens + e, (d ^ (3 if e % 2 else 1)) * n_ens + e))
    near = lax.ppermute(near, ("dom", "ens"), pairs)
    far = lax.ppermute(far, "dom", [(d, d ^ 2) for d in range(n_dom)])
    other = lax.ppermute(near, "ens", [(e, e ^ 1) for e in range(n_ens)])
    return [here, near, far, other]


def gather_members(state, own, n_ens):
    pieces = {0: state}
    if not has_halves(n_ens):
        for shift in range(1, n_ens):
            pairs = [(e, (e + shift) % n_ens) for e in range(n_ens)]
            pieces[shift] = lax.ppermute(state, "ens", pairs)
        pieces[0] = own
        return pieces
    bit = n_ens >> 1
    while bit:
        pairs = [(e, e ^ bit) for e in range(n_ens)]
        for key in list(pieces):
            pieces[key ^ bit] = lax.ppermute(pieces[key], "ens", pairs)
        bit >>= 1
        if bit == 1:
            pieces[0] = own
    pieces[0] = own
    return pieces


def make_on_device(n_dom, n_ens):
    vmem = pl.BlockSpec(memory_space=pltpu.VMEM)
    hbm = pl.BlockSpec(memory_space=pltpu.HBM)
    direct = n_dom <= DIRECT_DOM
    paired = is_paired(n_dom, n_ens)
    halves = has_halves(n_ens)
    limit = VMEM_LIMIT if direct else None

    def call(kernel, out_shape, operands, specs=None, scratch=(), out_spec=vmem):
        many = isinstance(out_shape, (list, tuple))
        return pl.pallas_call(
            kernel,
            out_shape=out_shape,
            in_specs=specs or [vmem] * len(operands),
            out_specs=[out_spec] * len(out_shape) if many else out_spec,
            scratch_shapes=list(scratch),
            compiler_params=pltpu.CompilerParams(vmem_limit_bytes=limit),
        )(*operands)

    def in_hbm(value):
        return pltpu.with_memory_space_constraint(value, pltpu.HBM)

    def shape(dims, dtype=F32):
        return jax.ShapeDtypeStruct(dims, dtype)

    def on_device(state, coords, owner_local, counts, obs_value, obs_weight):
        local_members, elements, nodes = state.shape
        slots = coords.shape[1]
        members = local_members * n_ens
        tile_shape = (8, 2 * CAP)
        inputs = [counts, coords, owner_local[None], obs_value[None], obs_weight[None]]
        pack_scratch = [
            pltpu.SMEM(counts.shape, jnp.int32),
            pltpu.VMEM(coords.shape, F32),
            pltpu.VMEM((1, slots), jnp.int32),
            pltpu.VMEM((1, slots), F32),
            pltpu.VMEM((1, slots), F32),
            pltpu.VMEM((8, slots), F32),
            pltpu.SemaphoreType.DMA((5,)),
        ]
        inputs = [in_hbm(value) for value in inputs]
        if paired:
            made = [shape(tile_shape)] * 3
            tiles = call(early_kernel, made, inputs, [hbm] * len(inputs), pack_scratch)
            tiles = call(
                lambda *refs: later_kernel(len(made), *refs),
                made,
                list(tiles) + inputs,
                [vmem] * len(made) + [hbm] * len(inputs),
                pack_scratch,
            )
        else:
            tiles = call(
                lambda *refs: pack_kernel(direct, paired, *refs),
                [shape(tile_shape)] * n_dom if direct else [shape((n_dom,) + tile_shape)],
                inputs,
                [hbm] * len(inputs),
                pack_scratch,
            )
        if direct:
            tiles = spread(tiles, n_dom, n_ens)
        else:
            moved = lax.all_to_all(tiles[0], "dom", split_axis=0, concat_axis=0, tiled=True)
            tiles = [moved[d] for d in range(n_dom)]
        own = call(
            fetch_kernel, shape(state.shape), [in_hbm(state)], [hbm], [pltpu.SemaphoreType.DMA(())]
        )
        pieces = gather_members(state, own, n_ens)
        sensor_count = CAP * (n_dom + n_dom % 2)
        order = key_order(n_ens)
        local = order[: n_ens // 2] if halves else order
        sensors, high, low, values = call(
            lambda *refs: values_kernel(paired, n_dom, *refs),
            [
                shape((8, sensor_count)),
                shape((nodes, sensor_count), BF16),
                shape((nodes, sensor_count), BF16),
                shape((local_members, sensor_count)),
            ],
            list(tiles) + [pieces[0]],
        )
        if len(local) > 1:
            values = call(
                reach_kernel,
                shape((len(local) * local_members, sensor_count)),
                [sensors, high, low, values] + [pieces[key] for key in local[1:]],
            )
        values = [values]
        if halves:
            pairs = [(e, e ^ 1) for e in range(n_ens)]
            values.append(lax.ppermute(values[0], "ens", pairs))
        partial_sum = call(
            lambda *refs: cross_kernel(halves, *refs), shape((members, LANES)), [sensors] + values
        )
        if direct:
            sums = spread([partial_sum] * (3 if paired else n_dom), n_dom, n_ens)
        else:
            sums = [lax.psum(partial_sum, "dom")]
        return call(
            lambda *refs: mix_kernel(halves, len(sums), *refs),
            shape(state.shape),
            sums + [pieces[key] for key in range(n_ens)],
            None,
            [
                pltpu.VMEM(state.shape, F32),
                pltpu.VMEM((members * local_members, 8, 128), F32),
                pltpu.SemaphoreType.DMA((elements // 8,)),
            ],
            hbm,
        )

    return on_device


def solution(mesh):
    n_dom, n_ens = mesh.shape["dom"], mesh.shape["ens"]
    return jax.shard_map(
        make_on_device(n_dom, n_ens),
        mesh=mesh,
        in_specs=(
            P("ens", ("groups", "dom"), None),
            P(None, ("groups", "dom")),
            P(("groups", "dom")),
            P(("groups", "dom"), None),
            P(("groups", "dom")),
            P(("groups", "dom")),
        ),
        out_specs=P("ens", ("groups", "dom"), None),
        check_vma=False,
    )
```

```python
import jax
import jax.numpy as jnp
from jax import lax
from jax.experimental import pallas as pl
from jax.experimental.pallas import tpu as pltpu
from jax.sharding import PartitionSpec as P


CAP = 64
NS_ITERS = 8


GLL_POINTS = (
    -1.0,
    -0.8717401485096066,
    -0.5917001814331423,
    -0.2092992179024789,
    0.2092992179024789,
    0.5917001814331423,
    0.8717401485096066,
    1.0,
)
INFLATION = 1.1
ORDER = len(GLL_POINTS)
F32 = jnp.float32
BF16 = jnp.bfloat16
DIRECT_DOM = 8
VMEM_LIMIT = 8 * 1024 * 1024
LANES = 128
PROJECT_LANES = 8
TRACE_LANE = 64


def lagrange_scale(index):
    product = 1.0
    for other in range(ORDER):
        if other != index:
            product *= GLL_POINTS[index] - GLL_POINTS[other]
    return 1.0 / product


def lagrange_rows(position):
    shape = (ORDER, position.shape[1])
    node = lax.broadcasted_iota(jnp.int32, shape, 0)
    product = jnp.full(shape, lagrange_scale(0), F32)
    for index in range(1, ORDER):
        product = jnp.where(node == index, lagrange_scale(index), product)
    for other in range(ORDER):
        product = product * jnp.where(node == other, 1.0, position - GLL_POINTS[other])
    return product


def split(value):
    high = value.astype(BF16)
    low = (value - high.astype(F32)).astype(BF16)
    return high, low


def is_odd(halves):
    return lax.rem(lax.axis_index("ens"), 2) if halves else 0


def fetch_kernel(state, own, sem):
    copy = pltpu.make_async_copy(state, own, sem)
    copy.start()
    copy.wait()


def pack_kernel(direct, paired, counts, coords, owner, obs, weight, *rest):
    outs = rest[:-7]
    count_box, coord_box, owner_box, obs_box, weight_box, block, sems = rest[-7:]
    pairs = zip(
        (counts, coords, owner, obs, weight), (count_box, coord_box, owner_box, obs_box, weight_box)
    )
    copies = [
        pltpu.make_async_copy(source, target, sems.at[index])
        for index, (source, target) in enumerate(pairs)
    ]
    for copy in copies:
        copy.start()
    n_dom = counts.shape[1]
    slots = coords.shape[1]
    here = lax.axis_index("dom")
    block[...] = jnp.zeros(block.shape, F32)
    column = lax.broadcasted_iota(jnp.int32, (8, 2 * CAP), 1)
    for copy in copies:
        copy.wait()
    block[0:3, :] = coord_box[...]
    block[3:4, :] = owner_box[...].astype(F32)
    block[4:5, :] = obs_box[...]
    block[5:6, :] = weight_box[...]
    rows = block[...]

    def tile(target, half):
        start = jnp.int32(0)
        for other in range(n_dom):
            start = start + jnp.where(other < target, count_box[0, other], 0)
        count = count_box[0, target]
        turned = pltpu.roll(rows, lax.rem(half - start + slots, slots), axis=1)[:, : 2 * CAP]
        return jnp.where((column >= half) & (column < half + count), turned, 0.0)

    if paired:
        near = jnp.where(is_odd(paired) == 0, 1, 3)
        for out, bits, half in zip(outs, (0, near, 2), (0, CAP, 0)):
            out[...] = tile(jnp.bitwise_xor(here, bits), half)
    elif direct:
        for shift in range(n_dom):
            outs[shift][...] = tile(lax.rem(here + shift, n_dom), (shift % 2) * CAP)
    else:
        half = lax.rem(here, 2) * CAP

        def step(target, carry):
            outs[0][target] = tile(target, half)
            return carry

        lax.fori_loop(0, n_dom, step, 0)


def pick(refs, sensors, high, low):
    members, elements, nodes = refs[0].shape
    rows = jnp.concatenate([ref[...].reshape(members * elements, nodes) for ref in refs], axis=0)
    rows_high, rows_low = split(rows)
    both = jnp.dot(
        jnp.concatenate([rows_high, rows_low], axis=0), high, preferred_element_type=F32
    )
    partial = (
        both[: rows.shape[0]]
        + both[rows.shape[0] :]
        + jnp.dot(rows_high, low, preferred_element_type=F32)
    )
    ids = lax.broadcasted_iota(jnp.int32, (elements, sensors.shape[1]), 0).astype(F32)
    partial = partial.reshape(len(refs) * members, elements, partial.shape[1])
    return jnp.sum(jnp.where((ids == sensors[3:4, :])[None], partial, 0.0), axis=1)


def values_kernel(paired, tile_count, *refs):
    tiles, state_refs = refs[:tile_count], refs[tile_count:-4]
    sensors_out, high_out, low_out, values_out = refs[-4:]
    blocks = [ref[...] for ref in tiles]
    if paired:
        here, near, far, other = blocks
        odd = is_odd(paired) == 1
        blocks = [here, jnp.where(odd, other, near), far, jnp.where(odd, near, other)]
    pairs = []
    for first in range(0, tile_count, 2):
        pair = blocks[first]
        if first + 1 < tile_count:
            pair = pair + blocks[first + 1]
        pairs.append(pair)
    sensors = jnp.concatenate(pairs, axis=1) if len(pairs) > 1 else pairs[0]
    sensors_out[...] = sensors
    along_r = lagrange_rows(sensors[0:1, :])
    along_s = lagrange_rows(sensors[1:2, :])
    along_t = lagrange_rows(sensors[2:3, :])
    for t in range(ORDER):
        for s in range(0, ORDER, 2):
            rows = [along_r * (along_t[t : t + 1, :] * along_s[k : k + 1, :]) for k in (s, s + 1)]
            high, low = split(jnp.concatenate(rows, axis=0))
            base = ORDER * ORDER * t + ORDER * s
            high_out[base : base + 2 * ORDER, :] = high
            low_out[base : base + 2 * ORDER, :] = low
    values_out[...] = pick(state_refs, sensors, high_out[...], low_out[...])


def reach_kernel(sensors_ref, high_ref, low_ref, values_ref, *refs):
    state_refs, out = refs[:-1], refs[-1]
    first = values_ref.shape[0]
    out[:first, :] = values_ref[...]
    out[first:, :] = pick(state_refs, sensors_ref[...], high_ref[...], low_ref[...])


def cross_kernel(halves, sensors_ref, *refs):
    value_refs, out = refs[:-1], refs[-1]
    sensors = sensors_ref[...]
    values = jnp.concatenate([ref[...] for ref in value_refs], axis=0)
    total = values.shape[0]
    if halves:
        turned = jnp.concatenate([ref[...] for ref in value_refs[::-1]], axis=0)
        values = jnp.where(is_odd(halves) == 1, turned, values)
    mean_value = jnp.sum(values, axis=0, keepdims=True) * (1.0 / total)
    anomaly = values - mean_value
    weighted = anomaly * sensors[5:6, :]
    innovation = sensors[4:5, :] - mean_value
    pad = jnp.zeros((PROJECT_LANES - 1, values.shape[1]), F32)
    right = jnp.concatenate([anomaly, innovation, pad], axis=0)
    left_high, left_low = split(weighted)
    right_high, right_low = split(right)
    across = (((1,), (1,)), ((), ()))
    both = lax.dot_general(
        jnp.concatenate([left_high, left_low], axis=0),
        right_high,
        across,
        preferred_element_type=F32,
    )
    out[:, : total + PROJECT_LANES] = (
        both[:total]
        + both[total:]
        + lax.dot_general(left_high, right_low, across, preferred_element_type=F32)
    )
    trace_part = jnp.sum(jnp.sum(weighted * anomaly, axis=0, keepdims=True), axis=1, keepdims=True)
    out[:, TRACE_LANE:] = jnp.broadcast_to(trace_part, (total, LANES - TRACE_LANE))


def lane_gather(value, lanes):
    return jnp.take_along_axis(value, lanes, axis=1, mode="promise_in_bounds")


def sublane_total(value):
    for shift in (4, 2, 1):
        value = value + pltpu.roll(value, shift, axis=0)
    return value


def mix_kernel(halves, sum_count, *refs):
    sums, state_refs = refs[:sum_count], refs[sum_count:-4]
    out, staged, splats, sems = refs[-4:]
    local_members, elements, nodes = out.shape
    members = local_members * len(state_refs)
    tile = (8, LANES)
    sub = lax.broadcasted_iota(jnp.int32, tile, 0)
    lane = lax.broadcasted_iota(jnp.int32, tile, 1)
    left_lanes = [(lane // members) * members + (sub + 8 * g) for g in range(2)]
    right_lanes = sub * members + lane % members
    identity = [(lane // members + 8 * h == lane % members).astype(F32) for h in range(2)]

    def as_left(matrix):
        return [[lane_gather(matrix[h], left_lanes[g]) for g in range(2)] for h in range(2)]

    def as_right(matrix):
        return [lane_gather(matrix[g], right_lanes) for g in range(2)]

    def product(left, right):
        return [sublane_total(left[h][0] * right[0] + left[h][1] * right[1]) for h in range(2)]

    total_sum = sums[0][...]
    for ref in sums[1:]:
        total_sum = total_sum + ref[...]
    rows = [total_sum[8 * g : 8 * g + 8, :] for g in range(2)]
    project = [lane_gather(rows[g], jnp.full(tile, members, jnp.int32)) for g in range(2)]
    trace_value = lane_gather(rows[0], jnp.full(tile, TRACE_LANE, jnp.int32))
    scale = 1.0 / (trace_value + members * ((members - 1) / INFLATION))
    diagonal = (members - 1) / INFLATION
    unit_left = [[(lane // members + 8 * h == sub + 8 * g).astype(F32) for g in range(2)] for h in range(2)]
    unit_right = [(lane % members == sub + 8 * g).astype(F32) for g in range(2)]
    system_left = [
        [
            (lane_gather(rows[g], lane // members + 8 * h) + diagonal * unit_left[h][g]) * scale
            for g in range(2)
        ]
        for h in range(2)
    ]
    system_right = [
        (lane_gather(rows[g], lane % members) + diagonal * unit_right[g]) * scale for g in range(2)
    ]
    inverse_left = [
        [1.5 * unit_left[h][g] - 0.5 * system_left[h][g] for g in range(2)] for h in range(2)
    ]
    inverse_right = [1.5 * unit_right[g] - 0.5 * system_right[g] for g in range(2)]
    iterate = product(system_left, inverse_right)
    for sweep in range(1, NS_ITERS):
        step = product(inverse_left, as_right(iterate))
        middle = [1.5 * identity[h] - 0.5 * step[h] for h in range(2)]
        middle_left = as_left(middle)
        inverse_root = product(middle_left, inverse_right)
        if sweep + 1 < NS_ITERS:
            iterate = product(as_left(iterate), as_right(middle))
            inverse_left, inverse_right = as_left(inverse_root), as_right(inverse_root)
        else:
            solved = product(middle_left, as_right(product(inverse_left, project)))
    mean_weights = product(as_left(inverse_root), as_right(solved))
    root_scale = jnp.sqrt((members - 1) * scale)
    transform = [inverse_root[h] * root_scale + mean_weights[h] * scale for h in range(2)]
    transform_right = as_right(transform)
    column_mean = sublane_total(transform_right[0] + transform_right[1]) * (1.0 / members)
    mixing = [transform[h] - column_mean + 1.0 / members for h in range(2)]
    odd = is_odd(halves)
    order = key_order(len(state_refs))
    own_place = odd * order.index(1) if halves else 0
    for k in range(local_members):
        lanes = sub * members + (k + local_members * own_place)
        for h in range(2):
            column = lane_gather(mixing[h], lanes)
            for i in range(8):
                splats[(8 * h + i) * local_members + k] = jnp.broadcast_to(column[i : i + 1, :], tile)
    places = []
    for piece in range(len(state_refs)):
        place = order.index(piece)
        places.append(place + odd * (order.index(piece ^ 1) - place) if halves else place)
    copies = []
    for block in range(elements // 8):
        span = slice(8 * block, 8 * block + 8)
        for first in range(0, nodes, 2 * LANES):
            spans = [slice(first + LANES * u, first + LANES * (u + 1)) for u in range(2)]
            totals = [[None, None] for _ in range(local_members)]
            for j in range(members):
                piece, member = divmod(j, local_members)
                values = [state_refs[piece][member, span, lanes] for lanes in spans]
                for k in range(local_members):
                    factor = splats[(places[piece] * local_members + member) * local_members + k]
                    for u in range(2):
                        term = factor * values[u]
                        totals[k][u] = term if j == 0 else totals[k][u] + term
            for k in range(local_members):
                for u in range(2):
                    staged[k, span, spans[u]] = totals[k][u]
        place = pl.ds(8 * block, 8)
        copy = pltpu.make_async_copy(staged.at[:, place], out.at[:, place], sems.at[block])
        copy.start()
        copies.append(copy)
    for copy in copies:
        copy.wait()


def has_halves(n_ens):
    return n_ens > 1 and n_ens & (n_ens - 1) == 0


def is_paired(n_dom, n_ens):
    return n_dom == 4 and has_halves(n_ens)


def key_order(n_ens):
    if not has_halves(n_ens):
        return list(range(n_ens))
    return list(range(0, n_ens, 2)) + list(range(1, n_ens, 2))


def spread(values, n_dom, n_ens, bits=(1, 3, 2), crossing=0):
    if not is_paired(n_dom, n_ens):
        return [values[0]] + [
            lax.ppermute(values[s], "dom", [(d, (d + s) % n_dom) for d in range(n_dom)])
            for s in range(1, n_dom)
        ]
    here, near, far = values
    near_pairs, far_pairs = [], []
    for d in range(n_dom):
        for e in range(n_ens):
            near_pairs.append((d * n_ens + e, (d ^ bits[e % 2]) * n_ens + e))
            far_pairs.append((d * n_ens + e, (d ^ bits[2]) * n_ens + (e ^ crossing)))
    near = lax.ppermute(near, ("dom", "ens"), near_pairs)
    far = lax.ppermute(far, ("dom", "ens"), far_pairs)
    other = lax.ppermute(near, "ens", [(e, e ^ 1) for e in range(n_ens)])
    return [here, near, far, other]


def gather_members(state, own, n_ens):
    pieces = {0: state}
    if not has_halves(n_ens):
        for shift in range(1, n_ens):
            pairs = [(e, (e + shift) % n_ens) for e in range(n_ens)]
            pieces[shift] = lax.ppermute(state, "ens", pairs)
        pieces[0] = own
        return pieces
    bit = n_ens >> 1
    while bit:
        pairs = [(e, e ^ bit) for e in range(n_ens)]
        for key in list(pieces):
            pieces[key ^ bit] = lax.ppermute(pieces[key], "ens", pairs)
        bit >>= 1
        if bit == 1:
            pieces[0] = own
    pieces[0] = own
    return pieces


def make_on_device(n_dom, n_ens):
    vmem = pl.BlockSpec(memory_space=pltpu.VMEM)
    hbm = pl.BlockSpec(memory_space=pltpu.HBM)
    direct = n_dom <= DIRECT_DOM
    paired = is_paired(n_dom, n_ens)
    halves = has_halves(n_ens)
    limit = VMEM_LIMIT if direct else None

    def call(kernel, out_shape, operands, specs=None, scratch=(), out_spec=vmem):
        many = isinstance(out_shape, (list, tuple))
        return pl.pallas_call(
            kernel,
            out_shape=out_shape,
            in_specs=specs or [vmem] * len(operands),
            out_specs=[out_spec] * len(out_shape) if many else out_spec,
            scratch_shapes=list(scratch),
            compiler_params=pltpu.CompilerParams(vmem_limit_bytes=limit),
        )(*operands)

    def in_hbm(value):
        return pltpu.with_memory_space_constraint(value, pltpu.HBM)

    def shape(dims, dtype=F32):
        return jax.ShapeDtypeStruct(dims, dtype)

    def on_device(state, coords, owner_local, counts, obs_value, obs_weight):
        local_members, elements, nodes = state.shape
        slots = coords.shape[1]
        members = local_members * n_ens
        tile_shape = (8, 2 * CAP)
        inputs = [counts, coords, owner_local[None], obs_value[None], obs_weight[None]]
        tiles = call(
            lambda *refs: pack_kernel(direct, paired, *refs),
            [shape(tile_shape)] * (3 if paired else n_dom)
            if direct
            else [shape((n_dom,) + tile_shape)],
            [in_hbm(value) for value in inputs],
            [hbm] * len(inputs),
            [
                pltpu.SMEM(counts.shape, jnp.int32),
                pltpu.VMEM(coords.shape, F32),
                pltpu.VMEM((1, slots), jnp.int32),
                pltpu.VMEM((1, slots), F32),
                pltpu.VMEM((1, slots), F32),
                pltpu.VMEM((8, slots), F32),
                pltpu.SemaphoreType.DMA((5,)),
            ],
        )
        if direct:
            tiles = spread(tiles, n_dom, n_ens)
        else:
            moved = lax.all_to_all(tiles[0], "dom", split_axis=0, concat_axis=0, tiled=True)
            tiles = [moved[d] for d in range(n_dom)]
        own = call(
            fetch_kernel, shape(state.shape), [in_hbm(state)], [hbm], [pltpu.SemaphoreType.DMA(())]
        )
        pieces = gather_members(state, own, n_ens)
        sensor_count = CAP * (n_dom + n_dom % 2)
        order = key_order(n_ens)
        local = order[: n_ens // 2] if halves else order
        sensors, high, low, values = call(
            lambda *refs: values_kernel(paired, n_dom, *refs),
            [
                shape((8, sensor_count)),
                shape((nodes, sensor_count), BF16),
                shape((nodes, sensor_count), BF16),
                shape((local_members, sensor_count)),
            ],
            list(tiles) + [pieces[0]],
        )
        if len(local) > 1:
            values = call(
                reach_kernel,
                shape((len(local) * local_members, sensor_count)),
                [sensors, high, low, values] + [pieces[key] for key in local[1:]],
            )
        values = [values]
        if halves:
            pairs = [(e, e ^ 1) for e in range(n_ens)]
            values.append(lax.ppermute(values[0], "ens", pairs))
        partial_sum = call(
            lambda *refs: cross_kernel(halves, *refs), shape((members, LANES)), [sensors] + values
        )
        if direct:
            copies = [partial_sum] * (3 if paired else n_dom)
            sums = spread(copies, n_dom, n_ens, bits=(2, 3, 1), crossing=1)
        else:
            sums = [lax.psum(partial_sum, "dom")]
        return call(
            lambda *refs: mix_kernel(halves, len(sums), *refs),
            shape(state.shape),
            sums + [pieces[key] for key in range(n_ens)],
            None,
            [
                pltpu.VMEM(state.shape, F32),
                pltpu.VMEM((members * local_members, 8, 128), F32),
                pltpu.SemaphoreType.DMA((elements // 8,)),
            ],
            hbm,
        )

    return on_device


def solution(mesh):
    n_dom, n_ens = mesh.shape["dom"], mesh.shape["ens"]
    return jax.shard_map(
        make_on_device(n_dom, n_ens),
        mesh=mesh,
        in_specs=(
            P("ens", ("groups", "dom"), None),
            P(None, ("groups", "dom")),
            P(("groups", "dom")),
            P(("groups", "dom"), None),
            P(("groups", "dom")),
            P(("groups", "dom")),
        ),
        out_specs=P("ens", ("groups", "dom"), None),
        check_vma=False,
    )
```

```python
import jax
import jax.numpy as jnp
from jax import lax
from jax.experimental import pallas as pl
from jax.experimental.pallas import tpu as pltpu
from jax.sharding import PartitionSpec as P


CAP = 64
NS_ITERS = 8


GLL_POINTS = (
    -1.0,
    -0.8717401485096066,
    -0.5917001814331423,
    -0.2092992179024789,
    0.2092992179024789,
    0.5917001814331423,
    0.8717401485096066,
    1.0,
)
INFLATION = 1.1
ORDER = len(GLL_POINTS)
F32 = jnp.float32
BF16 = jnp.bfloat16
DIRECT_DOM = 8
VMEM_LIMIT = 8 * 1024 * 1024
LANES = 128
PROJECT_LANES = 8
TRACE_LANE = 64


def lagrange_scale(index):
    product = 1.0
    for other in range(ORDER):
        if other != index:
            product *= GLL_POINTS[index] - GLL_POINTS[other]
    return 1.0 / product


def lagrange_rows(position):
    shape = (ORDER, position.shape[1])
    node = lax.broadcasted_iota(jnp.int32, shape, 0)
    product = jnp.full(shape, lagrange_scale(0), F32)
    for index in range(1, ORDER):
        product = jnp.where(node == index, lagrange_scale(index), product)
    for other in range(ORDER):
        product = product * jnp.where(node == other, 1.0, position - GLL_POINTS[other])
    return product


def split(value):
    high = value.astype(BF16)
    low = (value - high.astype(F32)).astype(BF16)
    return high, low


def is_odd(halves):
    return lax.rem(lax.axis_index("ens"), 2) if halves else 0


def fetch_kernel(state, own, sem):
    copy = pltpu.make_async_copy(state, own, sem)
    copy.start()
    copy.wait()


def pack_kernel(direct, paired, counts, coords, owner, obs, weight, *rest):
    outs = rest[:-7]
    count_box, coord_box, owner_box, obs_box, weight_box, block, sems = rest[-7:]
    pairs = zip(
        (counts, coords, owner, obs, weight), (count_box, coord_box, owner_box, obs_box, weight_box)
    )
    copies = [
        pltpu.make_async_copy(source, target, sems.at[index])
        for index, (source, target) in enumerate(pairs)
    ]
    for copy in copies:
        copy.start()
    n_dom = counts.shape[1]
    slots = coords.shape[1]
    here = lax.axis_index("dom")
    block[...] = jnp.zeros(block.shape, F32)
    column = lax.broadcasted_iota(jnp.int32, (8, 2 * CAP), 1)
    for copy in copies:
        copy.wait()
    block[0:3, :] = coord_box[...]
    block[3:4, :] = owner_box[...].astype(F32)
    block[4:5, :] = obs_box[...]
    block[5:6, :] = weight_box[...]
    rows = block[...]

    def tile(target, half):
        start = jnp.int32(0)
        for other in range(n_dom):
            start = start + jnp.where(other < target, count_box[0, other], 0)
        count = count_box[0, target]
        turned = pltpu.roll(rows, lax.rem(half - start + slots, slots), axis=1)[:, : 2 * CAP]
        return jnp.where((column >= half) & (column < half + count), turned, 0.0)

    if paired:
        near = jnp.where(is_odd(paired) == 0, 1, 3)
        for out, bits, half in zip(outs, (0, near, 2), (0, CAP, 0)):
            out[...] = tile(jnp.bitwise_xor(here, bits), half)
    elif direct:
        for shift in range(n_dom):
            outs[shift][...] = tile(lax.rem(here + shift, n_dom), (shift % 2) * CAP)
    else:
        half = lax.rem(here, 2) * CAP

        def step(target, carry):
            outs[0][target] = tile(target, half)
            return carry

        lax.fori_loop(0, n_dom, step, 0)


def pick(refs, sensors, high, low):
    members, elements, nodes = refs[0].shape
    rows = jnp.concatenate([ref[...].reshape(members * elements, nodes) for ref in refs], axis=0)
    rows_high, rows_low = split(rows)
    both = jnp.dot(
        jnp.concatenate([rows_high, rows_low], axis=0), high, preferred_element_type=F32
    )
    partial = (
        both[: rows.shape[0]]
        + both[rows.shape[0] :]
        + jnp.dot(rows_high, low, preferred_element_type=F32)
    )
    ids = lax.broadcasted_iota(jnp.int32, (elements, sensors.shape[1]), 0).astype(F32)
    partial = partial.reshape(len(refs) * members, elements, partial.shape[1])
    return jnp.sum(jnp.where((ids == sensors[3:4, :])[None], partial, 0.0), axis=1)


def values_kernel(paired, tile_count, *refs):
    tiles, state_refs = refs[:tile_count], refs[tile_count:-4]
    sensors_out, high_out, low_out, values_out = refs[-4:]
    blocks = [ref[...] for ref in tiles]
    if paired:
        here, near, far, other = blocks
        odd = is_odd(paired) == 1
        blocks = [here, jnp.where(odd, other, near), far, jnp.where(odd, near, other)]
    pairs = []
    for first in range(0, tile_count, 2):
        pair = blocks[first]
        if first + 1 < tile_count:
            pair = pair + blocks[first + 1]
        pairs.append(pair)
    sensors = jnp.concatenate(pairs, axis=1) if len(pairs) > 1 else pairs[0]
    sensors_out[...] = sensors
    along_r = lagrange_rows(sensors[0:1, :])
    along_s = lagrange_rows(sensors[1:2, :])
    along_t = lagrange_rows(sensors[2:3, :])
    for t in range(ORDER):
        for s in range(0, ORDER, 2):
            rows = [along_r * (along_t[t : t + 1, :] * along_s[k : k + 1, :]) for k in (s, s + 1)]
            high, low = split(jnp.concatenate(rows, axis=0))
            base = ORDER * ORDER * t + ORDER * s
            high_out[base : base + 2 * ORDER, :] = high
            low_out[base : base + 2 * ORDER, :] = low
    values_out[...] = pick(state_refs, sensors, high_out[...], low_out[...])


def reach_kernel(sensors_ref, high_ref, low_ref, values_ref, *refs):
    state_refs, out = refs[:-1], refs[-1]
    first = values_ref.shape[0]
    out[:first, :] = values_ref[...]
    out[first:, :] = pick(state_refs, sensors_ref[...], high_ref[...], low_ref[...])


def cross_kernel(halves, sensors_ref, *refs):
    value_refs, out = refs[:-1], refs[-1]
    sensors = sensors_ref[...]
    values = jnp.concatenate([ref[...] for ref in value_refs], axis=0)
    total = values.shape[0]
    if halves:
        turned = jnp.concatenate([ref[...] for ref in value_refs[::-1]], axis=0)
        values = jnp.where(is_odd(halves) == 1, turned, values)
    mean_value = jnp.sum(values, axis=0, keepdims=True) * (1.0 / total)
    anomaly = values - mean_value
    weighted = anomaly * sensors[5:6, :]
    innovation = sensors[4:5, :] - mean_value
    pad = jnp.zeros((PROJECT_LANES - 1, values.shape[1]), F32)
    right = jnp.concatenate([anomaly, innovation, pad], axis=0)
    left_high, left_low = split(weighted)
    right_high, right_low = split(right)
    across = (((1,), (1,)), ((), ()))
    both = lax.dot_general(
        jnp.concatenate([left_high, left_low], axis=0),
        right_high,
        across,
        preferred_element_type=F32,
    )
    out[:, : total + PROJECT_LANES] = (
        both[:total]
        + both[total:]
        + lax.dot_general(left_high, right_low, across, preferred_element_type=F32)
    )
    trace_part = jnp.sum(jnp.sum(weighted * anomaly, axis=0, keepdims=True), axis=1, keepdims=True)
    out[:, TRACE_LANE:] = jnp.broadcast_to(trace_part, (total, LANES - TRACE_LANE))


def lane_gather(value, lanes):
    return jnp.take_along_axis(value, lanes, axis=1, mode="promise_in_bounds")


def sublane_total(value):
    for shift in (4, 2, 1):
        value = value + pltpu.roll(value, shift, axis=0)
    return value


def mix_kernel(halves, sum_count, *refs):
    sums, state_refs = refs[:sum_count], refs[sum_count:-4]
    out, staged, splats, sems = refs[-4:]
    local_members, elements, nodes = out.shape
    members = local_members * len(state_refs)
    tile = (8, LANES)
    sub = lax.broadcasted_iota(jnp.int32, tile, 0)
    lane = lax.broadcasted_iota(jnp.int32, tile, 1)
    left_lanes = [(lane // members) * members + (sub + 8 * g) for g in range(2)]
    right_lanes = sub * members + lane % members
    identity = [(lane // members + 8 * h == lane % members).astype(F32) for h in range(2)]

    def as_left(matrix):
        return [[lane_gather(matrix[h], left_lanes[g]) for g in range(2)] for h in range(2)]

    def as_right(matrix):
        return [lane_gather(matrix[g], right_lanes) for g in range(2)]

    def product(left, right):
        return [sublane_total(left[h][0] * right[0] + left[h][1] * right[1]) for h in range(2)]

    total_sum = sums[0][...]
    for ref in sums[1:]:
        total_sum = total_sum + ref[...]
    rows = [total_sum[8 * g : 8 * g + 8, :] for g in range(2)]
    project = [lane_gather(rows[g], jnp.full(tile, members, jnp.int32)) for g in range(2)]
    trace_value = lane_gather(rows[0], jnp.full(tile, TRACE_LANE, jnp.int32))
    scale = 1.0 / (trace_value + members * ((members - 1) / INFLATION))
    diagonal = (members - 1) / INFLATION
    unit_left = [[(lane // members + 8 * h == sub + 8 * g).astype(F32) for g in range(2)] for h in range(2)]
    unit_right = [(lane % members == sub + 8 * g).astype(F32) for g in range(2)]
    system_left = [
        [
            (lane_gather(rows[g], lane // members + 8 * h) + diagonal * unit_left[h][g]) * scale
            for g in range(2)
        ]
        for h in range(2)
    ]
    system_right = [
        (lane_gather(rows[g], lane % members) + diagonal * unit_right[g]) * scale for g in range(2)
    ]
    inverse_left = [
        [1.5 * unit_left[h][g] - 0.5 * system_left[h][g] for g in range(2)] for h in range(2)
    ]
    inverse_right = [1.5 * unit_right[g] - 0.5 * system_right[g] for g in range(2)]
    iterate = product(system_left, inverse_right)
    for sweep in range(1, NS_ITERS):
        step = product(inverse_left, as_right(iterate))
        middle = [1.5 * identity[h] - 0.5 * step[h] for h in range(2)]
        middle_left = as_left(middle)
        inverse_root = product(middle_left, inverse_right)
        if sweep + 1 < NS_ITERS:
            iterate = product(as_left(iterate), as_right(middle))
            inverse_left, inverse_right = as_left(inverse_root), as_right(inverse_root)
        else:
            solved = product(middle_left, as_right(product(inverse_left, project)))
    mean_weights = product(as_left(inverse_root), as_right(solved))
    root_scale = jnp.sqrt((members - 1) * scale)
    transform = [inverse_root[h] * root_scale + mean_weights[h] * scale for h in range(2)]
    transform_right = as_right(transform)
    column_mean = sublane_total(transform_right[0] + transform_right[1]) * (1.0 / members)
    mixing = [transform[h] - column_mean + 1.0 / members for h in range(2)]
    odd = is_odd(halves)
    order = key_order(len(state_refs))
    own_place = odd * order.index(1) if halves else 0
    for k in range(local_members):
        lanes = sub * members + (k + local_members * own_place)
        for h in range(2):
            column = lane_gather(mixing[h], lanes)
            for i in range(8):
                splats[(8 * h + i) * local_members + k] = jnp.broadcast_to(column[i : i + 1, :], tile)
    places = []
    for piece in range(len(state_refs)):
        place = order.index(piece)
        places.append(place + odd * (order.index(piece ^ 1) - place) if halves else place)
    copies = []
    for block in range(elements // 8):
        span = slice(8 * block, 8 * block + 8)
        for first in range(0, nodes, 2 * LANES):
            spans = [slice(first + LANES * u, first + LANES * (u + 1)) for u in range(2)]
            totals = [[None, None] for _ in range(local_members)]
            for j in range(members):
                piece, member = divmod(j, local_members)
                values = [state_refs[piece][member, span, lanes] for lanes in spans]
                for k in range(local_members):
                    factor = splats[(places[piece] * local_members + member) * local_members + k]
                    for u in range(2):
                        term = factor * values[u]
                        totals[k][u] = term if j == 0 else totals[k][u] + term
            for k in range(local_members):
                for u in range(2):
                    staged[k, span, spans[u]] = totals[k][u]
        place = pl.ds(8 * block, 8)
        copy = pltpu.make_async_copy(staged.at[:, place], out.at[:, place], sems.at[block])
        copy.start()
        copies.append(copy)
    for copy in copies:
        copy.wait()


def has_halves(n_ens):
    return n_ens > 1 and n_ens & (n_ens - 1) == 0


def is_paired(n_dom, n_ens):
    return n_dom == 4 and has_halves(n_ens)


def key_order(n_ens):
    if not has_halves(n_ens):
        return list(range(n_ens))
    local = [0] + [key + 1 for key in range(2, n_ens, 2)]
    return local + [key ^ 1 for key in local]


def spread(values, n_dom, n_ens, bits=(1, 3, 2), crossing=0):
    if not is_paired(n_dom, n_ens):
        return [values[0]] + [
            lax.ppermute(values[s], "dom", [(d, (d + s) % n_dom) for d in range(n_dom)])
            for s in range(1, n_dom)
        ]
    here, near, far = values
    near_pairs, far_pairs = [], []
    for d in range(n_dom):
        for e in range(n_ens):
            near_pairs.append((d * n_ens + e, (d ^ bits[e % 2]) * n_ens + e))
            far_pairs.append((d * n_ens + e, (d ^ bits[2]) * n_ens + (e ^ crossing)))
    near = lax.ppermute(near, ("dom", "ens"), near_pairs)
    far = lax.ppermute(far, ("dom", "ens"), far_pairs)
    other = lax.ppermute(near, "ens", [(e, e ^ 1) for e in range(n_ens)])
    return [here, near, far, other]


def gather_members(state, own, n_ens):
    pieces = {0: state}
    if not has_halves(n_ens):
        for shift in range(1, n_ens):
            pairs = [(e, (e + shift) % n_ens) for e in range(n_ens)]
            pieces[shift] = lax.ppermute(state, "ens", pairs)
        pieces[0] = own
        return pieces
    for key in key_order(n_ens)[1 : n_ens // 2]:
        pairs = [(e, e ^ key) for e in range(n_ens)]
        pieces[key] = lax.ppermute(state, "ens", pairs)
    pieces[0] = own
    for key in list(pieces):
        pairs = [(e, e ^ 1) for e in range(n_ens)]
        pieces[key ^ 1] = lax.ppermute(pieces[key], "ens", pairs)
    return pieces


def make_on_device(n_dom, n_ens):
    vmem = pl.BlockSpec(memory_space=pltpu.VMEM)
    hbm = pl.BlockSpec(memory_space=pltpu.HBM)
    direct = n_dom <= DIRECT_DOM
    paired = is_paired(n_dom, n_ens)
    halves = has_halves(n_ens)
    limit = VMEM_LIMIT if direct else None

    def call(kernel, out_shape, operands, specs=None, scratch=(), out_spec=vmem):
        many = isinstance(out_shape, (list, tuple))
        return pl.pallas_call(
            kernel,
            out_shape=out_shape,
            in_specs=specs or [vmem] * len(operands),
            out_specs=[out_spec] * len(out_shape) if many else out_spec,
            scratch_shapes=list(scratch),
            compiler_params=pltpu.CompilerParams(vmem_limit_bytes=limit),
        )(*operands)

    def in_hbm(value):
        return pltpu.with_memory_space_constraint(value, pltpu.HBM)

    def shape(dims, dtype=F32):
        return jax.ShapeDtypeStruct(dims, dtype)

    def on_device(state, coords, owner_local, counts, obs_value, obs_weight):
        local_members, elements, nodes = state.shape
        slots = coords.shape[1]
        members = local_members * n_ens
        tile_shape = (8, 2 * CAP)
        inputs = [counts, coords, owner_local[None], obs_value[None], obs_weight[None]]
        tiles = call(
            lambda *refs: pack_kernel(direct, paired, *refs),
            [shape(tile_shape)] * (3 if paired else n_dom)
            if direct
            else [shape((n_dom,) + tile_shape)],
            [in_hbm(value) for value in inputs],
            [hbm] * len(inputs),
            [
                pltpu.SMEM(counts.shape, jnp.int32),
                pltpu.VMEM(coords.shape, F32),
                pltpu.VMEM((1, slots), jnp.int32),
                pltpu.VMEM((1, slots), F32),
                pltpu.VMEM((1, slots), F32),
                pltpu.VMEM((8, slots), F32),
                pltpu.SemaphoreType.DMA((5,)),
            ],
        )
        if direct:
            tiles = spread(tiles, n_dom, n_ens)
        else:
            moved = lax.all_to_all(tiles[0], "dom", split_axis=0, concat_axis=0, tiled=True)
            tiles = [moved[d] for d in range(n_dom)]
        own = call(
            fetch_kernel, shape(state.shape), [in_hbm(state)], [hbm], [pltpu.SemaphoreType.DMA(())]
        )
        pieces = gather_members(state, own, n_ens)
        sensor_count = CAP * (n_dom + n_dom % 2)
        order = key_order(n_ens)
        local = order[: n_ens // 2] if halves else order
        sensors, high, low, values = call(
            lambda *refs: values_kernel(paired, n_dom, *refs),
            [
                shape((8, sensor_count)),
                shape((nodes, sensor_count), BF16),
                shape((nodes, sensor_count), BF16),
                shape((local_members, sensor_count)),
            ],
            list(tiles) + [pieces[0]],
        )
        if len(local) > 1:
            values = call(
                reach_kernel,
                shape((len(local) * local_members, sensor_count)),
                [sensors, high, low, values] + [pieces[key] for key in local[1:]],
            )
        values = [values]
        if halves:
            pairs = [(e, e ^ 1) for e in range(n_ens)]
            values.append(lax.ppermute(values[0], "ens", pairs))
        partial_sum = call(
            lambda *refs: cross_kernel(halves, *refs), shape((members, LANES)), [sensors] + values
        )
        if direct:
            copies = [partial_sum] * (3 if paired else n_dom)
            sums = spread(copies, n_dom, n_ens, bits=(2, 3, 1), crossing=1)
        else:
            sums = [lax.psum(partial_sum, "dom")]
        return call(
            lambda *refs: mix_kernel(halves, len(sums), *refs),
            shape(state.shape),
            sums + [pieces[key] for key in range(n_ens)],
            None,
            [
                pltpu.VMEM(state.shape, F32),
                pltpu.VMEM((members * local_members, 8, 128), F32),
                pltpu.SemaphoreType.DMA((elements // 8,)),
            ],
            hbm,
        )

    return on_device


def solution(mesh):
    n_dom, n_ens = mesh.shape["dom"], mesh.shape["ens"]
    return jax.shard_map(
        make_on_device(n_dom, n_ens),
        mesh=mesh,
        in_specs=(
            P("ens", ("groups", "dom"), None),
            P(None, ("groups", "dom")),
            P(("groups", "dom")),
            P(("groups", "dom"), None),
            P(("groups", "dom")),
            P(("groups", "dom")),
        ),
        out_specs=P("ens", ("groups", "dom"), None),
        check_vma=False,
    )
```

```python
import jax
import jax.numpy as jnp
from jax import lax
from jax.experimental import pallas as pl
from jax.experimental.pallas import tpu as pltpu
from jax.sharding import PartitionSpec as P


CAP = 64
NS_ITERS = 8


GLL_POINTS = (
    -1.0,
    -0.8717401485096066,
    -0.5917001814331423,
    -0.2092992179024789,
    0.2092992179024789,
    0.5917001814331423,
    0.8717401485096066,
    1.0,
)
INFLATION = 1.1
ORDER = len(GLL_POINTS)
F32 = jnp.float32
BF16 = jnp.bfloat16
DIRECT_DOM = 8
VMEM_LIMIT = 8 * 1024 * 1024
LANES = 128
PROJECT_LANES = 8
TRACE_LANE = 64


def lagrange_scale(index):
    product = 1.0
    for other in range(ORDER):
        if other != index:
            product *= GLL_POINTS[index] - GLL_POINTS[other]
    return 1.0 / product


def lagrange_rows(position):
    shape = (ORDER, position.shape[1])
    node = lax.broadcasted_iota(jnp.int32, shape, 0)
    product = jnp.full(shape, lagrange_scale(0), F32)
    for index in range(1, ORDER):
        product = jnp.where(node == index, lagrange_scale(index), product)
    for other in range(ORDER):
        product = product * jnp.where(node == other, 1.0, position - GLL_POINTS[other])
    return product


def split(value):
    high = value.astype(BF16)
    low = (value - high.astype(F32)).astype(BF16)
    return high, low


def is_odd(halves):
    return lax.rem(lax.axis_index("ens"), 2) if halves else 0


def fetch_kernel(state, own, sem):
    copy = pltpu.make_async_copy(state, own, sem)
    copy.start()
    copy.wait()


def pack_kernel(direct, paired, counts, coords, owner, obs, weight, *rest):
    outs = rest[:-7]
    count_box, coord_box, owner_box, obs_box, weight_box, block, sems = rest[-7:]
    pairs = zip(
        (counts, coords, owner, obs, weight), (count_box, coord_box, owner_box, obs_box, weight_box)
    )
    copies = [
        pltpu.make_async_copy(source, target, sems.at[index])
        for index, (source, target) in enumerate(pairs)
    ]
    for copy in copies:
        copy.start()
    n_dom = counts.shape[1]
    slots = coords.shape[1]
    here = lax.axis_index("dom")
    block[...] = jnp.zeros(block.shape, F32)
    column = lax.broadcasted_iota(jnp.int32, (8, 2 * CAP), 1)
    for copy in copies:
        copy.wait()
    block[0:3, :] = coord_box[...]
    block[3:4, :] = owner_box[...].astype(F32)
    block[4:5, :] = obs_box[...]
    block[5:6, :] = weight_box[...]
    rows = block[...]

    def tile(target, half):
        start = jnp.int32(0)
        for other in range(n_dom):
            start = start + jnp.where(other < target, count_box[0, other], 0)
        count = count_box[0, target]
        turned = pltpu.roll(rows, lax.rem(half - start + slots, slots), axis=1)[:, : 2 * CAP]
        return jnp.where((column >= half) & (column < half + count), turned, 0.0)

    if paired:
        near = jnp.where(is_odd(paired) == 0, 1, 3)
        for out, bits, half in zip(outs, (0, near, 2), (0, CAP, 0)):
            out[...] = tile(jnp.bitwise_xor(here, bits), half)
    elif direct:
        for shift in range(n_dom):
            outs[shift][...] = tile(lax.rem(here + shift, n_dom), (shift % 2) * CAP)
    else:
        half = lax.rem(here, 2) * CAP

        def step(target, carry):
            outs[0][target] = tile(target, half)
            return carry

        lax.fori_loop(0, n_dom, step, 0)


def pick(refs, sensors, high, low):
    members, elements, nodes = refs[0].shape
    rows = jnp.concatenate([ref[...].reshape(members * elements, nodes) for ref in refs], axis=0)
    rows_high, rows_low = split(rows)
    both = jnp.dot(
        jnp.concatenate([rows_high, rows_low], axis=0), high, preferred_element_type=F32
    )
    partial = (
        both[: rows.shape[0]]
        + both[rows.shape[0] :]
        + jnp.dot(rows_high, low, preferred_element_type=F32)
    )
    ids = lax.broadcasted_iota(jnp.int32, (elements, sensors.shape[1]), 0).astype(F32)
    partial = partial.reshape(len(refs) * members, elements, partial.shape[1])
    return jnp.sum(jnp.where((ids == sensors[3:4, :])[None], partial, 0.0), axis=1)


def values_kernel(paired, tile_count, *refs):
    tiles, state_refs = refs[:tile_count], refs[tile_count:-4]
    sensors_out, high_out, low_out, values_out = refs[-4:]
    blocks = [ref[...] for ref in tiles]
    if paired:
        here, near, far, other = blocks
        odd = is_odd(paired) == 1
        blocks = [here, jnp.where(odd, other, near), far, jnp.where(odd, near, other)]
    pairs = []
    for first in range(0, tile_count, 2):
        pair = blocks[first]
        if first + 1 < tile_count:
            pair = pair + blocks[first + 1]
        pairs.append(pair)
    sensors = jnp.concatenate(pairs, axis=1) if len(pairs) > 1 else pairs[0]
    sensors_out[...] = sensors
    along_r = lagrange_rows(sensors[0:1, :])
    along_s = lagrange_rows(sensors[1:2, :])
    along_t = lagrange_rows(sensors[2:3, :])
    for t in range(ORDER):
        for s in range(0, ORDER, 2):
            rows = [along_r * (along_t[t : t + 1, :] * along_s[k : k + 1, :]) for k in (s, s + 1)]
            high, low = split(jnp.concatenate(rows, axis=0))
            base = ORDER * ORDER * t + ORDER * s
            high_out[base : base + 2 * ORDER, :] = high
            low_out[base : base + 2 * ORDER, :] = low
    values_out[...] = pick(state_refs, sensors, high_out[...], low_out[...])


def reach_kernel(sensors_ref, high_ref, low_ref, values_ref, *refs):
    state_refs, out = refs[:-1], refs[-1]
    first = values_ref.shape[0]
    out[:first, :] = values_ref[...]
    out[first:, :] = pick(state_refs, sensors_ref[...], high_ref[...], low_ref[...])


def cross_kernel(halves, sensors_ref, *refs):
    value_refs, out = refs[:-1], refs[-1]
    sensors = sensors_ref[...]
    values = jnp.concatenate([ref[...] for ref in value_refs], axis=0)
    total = values.shape[0]
    if halves:
        turned = jnp.concatenate([ref[...] for ref in value_refs[::-1]], axis=0)
        values = jnp.where(is_odd(halves) == 1, turned, values)
    mean_value = jnp.sum(values, axis=0, keepdims=True) * (1.0 / total)
    anomaly = values - mean_value
    weighted = anomaly * sensors[5:6, :]
    innovation = sensors[4:5, :] - mean_value
    pad = jnp.zeros((PROJECT_LANES - 1, values.shape[1]), F32)
    right = jnp.concatenate([anomaly, innovation, pad], axis=0)
    left_high, left_low = split(weighted)
    right_high, right_low = split(right)
    across = (((1,), (1,)), ((), ()))
    both = lax.dot_general(
        jnp.concatenate([left_high, left_low], axis=0),
        right_high,
        across,
        preferred_element_type=F32,
    )
    out[:, : total + PROJECT_LANES] = (
        both[:total]
        + both[total:]
        + lax.dot_general(left_high, right_low, across, preferred_element_type=F32)
    )
    trace_part = jnp.sum(jnp.sum(weighted * anomaly, axis=0, keepdims=True), axis=1, keepdims=True)
    out[:, TRACE_LANE:] = jnp.broadcast_to(trace_part, (total, LANES - TRACE_LANE))


def lane_gather(value, lanes):
    return jnp.take_along_axis(value, lanes, axis=1, mode="promise_in_bounds")


def sublane_total(value):
    for shift in (4, 2, 1):
        value = value + pltpu.roll(value, shift, axis=0)
    return value


def mix_kernel(halves, sum_count, *refs):
    sums, state_refs = refs[:sum_count], refs[sum_count:-4]
    out, staged, splats, sems = refs[-4:]
    local_members, elements, nodes = out.shape
    members = local_members * len(state_refs)
    tile = (8, LANES)
    sub = lax.broadcasted_iota(jnp.int32, tile, 0)
    lane = lax.broadcasted_iota(jnp.int32, tile, 1)
    left_lanes = [(lane // members) * members + (sub + 8 * g) for g in range(2)]
    right_lanes = sub * members + lane % members
    identity = [(lane // members + 8 * h == lane % members).astype(F32) for h in range(2)]

    def as_left(matrix):
        return [[lane_gather(matrix[h], left_lanes[g]) for g in range(2)] for h in range(2)]

    def as_right(matrix):
        return [lane_gather(matrix[g], right_lanes) for g in range(2)]

    def product(left, right):
        return [sublane_total(left[h][0] * right[0] + left[h][1] * right[1]) for h in range(2)]

    total_sum = sums[0][...]
    for ref in sums[1:]:
        total_sum = total_sum + ref[...]
    rows = [total_sum[8 * g : 8 * g + 8, :] for g in range(2)]
    project = [lane_gather(rows[g], jnp.full(tile, members, jnp.int32)) for g in range(2)]
    trace_value = lane_gather(rows[0], jnp.full(tile, TRACE_LANE, jnp.int32))
    scale = 1.0 / (trace_value + members * ((members - 1) / INFLATION))
    diagonal = (members - 1) / INFLATION
    unit_left = [[(lane // members + 8 * h == sub + 8 * g).astype(F32) for g in range(2)] for h in range(2)]
    unit_right = [(lane % members == sub + 8 * g).astype(F32) for g in range(2)]
    system_left = [
        [
            (lane_gather(rows[g], lane // members + 8 * h) + diagonal * unit_left[h][g]) * scale
            for g in range(2)
        ]
        for h in range(2)
    ]
    system_right = [
        (lane_gather(rows[g], lane % members) + diagonal * unit_right[g]) * scale for g in range(2)
    ]
    inverse_left = [
        [1.5 * unit_left[h][g] - 0.5 * system_left[h][g] for g in range(2)] for h in range(2)
    ]
    inverse_right = [1.5 * unit_right[g] - 0.5 * system_right[g] for g in range(2)]
    iterate = product(system_left, inverse_right)
    for sweep in range(1, NS_ITERS):
        step = product(inverse_left, as_right(iterate))
        middle = [1.5 * identity[h] - 0.5 * step[h] for h in range(2)]
        middle_left = as_left(middle)
        inverse_root = product(middle_left, inverse_right)
        if sweep + 1 < NS_ITERS:
            iterate = product(as_left(iterate), as_right(middle))
            inverse_left, inverse_right = as_left(inverse_root), as_right(inverse_root)
        else:
            solved = product(middle_left, as_right(product(inverse_left, project)))
            ones = [jnp.ones(tile, F32)] * 2
            row_sums = product(middle_left, as_right(product(inverse_left, ones)))
    solved, row_sums, inverse_right = as_right(solved), as_right(row_sums), as_right(inverse_root)
    mean_weights = product(as_left(inverse_root), solved)
    root_scale = jnp.sqrt((members - 1) * scale)
    weights_mean = sublane_total(row_sums[0] * solved[0] + row_sums[1] * solved[1])
    column_sum = sublane_total(inverse_right[0] + inverse_right[1])
    shift = (1.0 - column_sum * root_scale - weights_mean * scale) * (1.0 / members)
    mixing = [
        inverse_root[h] * root_scale + mean_weights[h] * scale + shift for h in range(2)
    ]
    odd = is_odd(halves)
    order = key_order(len(state_refs))
    own_place = odd * order.index(1) if halves else 0
    for k in range(local_members):
        lanes = sub * members + (k + local_members * own_place)
        for h in range(2):
            column = lane_gather(mixing[h], lanes)
            for i in range(8):
                splats[(8 * h + i) * local_members + k] = jnp.broadcast_to(column[i : i + 1, :], tile)
    places = []
    for piece in range(len(state_refs)):
        place = order.index(piece)
        places.append(place + odd * (order.index(piece ^ 1) - place) if halves else place)

    def output_copy(block):
        place = pl.ds(pl.multiple_of(8 * block, 8), 8)
        return pltpu.make_async_copy(staged.at[:, place], out.at[:, place], sems.at[block])

    def mix_block(block, carry):
        span = pl.ds(pl.multiple_of(8 * block, 8), 8)
        for first in range(0, nodes, 2 * LANES):
            spans = [slice(first + LANES * u, first + LANES * (u + 1)) for u in range(2)]
            totals = [[None, None] for _ in range(local_members)]
            for j in range(members):
                piece, member = divmod(j, local_members)
                values = [state_refs[piece][member, span, lanes] for lanes in spans]
                for k in range(local_members):
                    factor = splats[(places[piece] * local_members + member) * local_members + k]
                    for u in range(2):
                        term = factor * values[u]
                        totals[k][u] = term if j == 0 else totals[k][u] + term
            for k in range(local_members):
                for u in range(2):
                    staged[k, span, spans[u]] = totals[k][u]
        output_copy(block).start()
        return carry

    def wait_block(block, carry):
        output_copy(block).wait()
        return carry

    lax.fori_loop(0, elements // 8, mix_block, 0)
    lax.fori_loop(0, elements // 8, wait_block, 0)


def has_halves(n_ens):
    return n_ens > 1 and n_ens & (n_ens - 1) == 0


def is_paired(n_dom, n_ens):
    return n_dom == 4 and has_halves(n_ens)


def key_order(n_ens):
    if not has_halves(n_ens):
        return list(range(n_ens))
    return list(range(0, n_ens, 2)) + list(range(1, n_ens, 2))


def spread(values, n_dom, n_ens, bits=(1, 3, 2), crossing=0):
    if not is_paired(n_dom, n_ens):
        return [values[0]] + [
            lax.ppermute(values[s], "dom", [(d, (d + s) % n_dom) for d in range(n_dom)])
            for s in range(1, n_dom)
        ]
    here, near, far = values
    near_pairs, far_pairs = [], []
    for d in range(n_dom):
        for e in range(n_ens):
            near_pairs.append((d * n_ens + e, (d ^ bits[e % 2]) * n_ens + e))
            far_pairs.append((d * n_ens + e, (d ^ bits[2]) * n_ens + (e ^ crossing)))
    near = lax.ppermute(near, ("dom", "ens"), near_pairs)
    far = lax.ppermute(far, ("dom", "ens"), far_pairs)
    other = lax.ppermute(near, "ens", [(e, e ^ 1) for e in range(n_ens)])
    return [here, near, far, other]


def gather_members(state, own, n_ens):
    pieces = {0: state}
    if not has_halves(n_ens):
        for shift in range(1, n_ens):
            pairs = [(e, (e + shift) % n_ens) for e in range(n_ens)]
            pieces[shift] = lax.ppermute(state, "ens", pairs)
        pieces[0] = own
        return pieces
    bit = n_ens >> 1
    while bit:
        pairs = [(e, e ^ bit) for e in range(n_ens)]
        for key in list(pieces):
            pieces[key ^ bit] = lax.ppermute(pieces[key], "ens", pairs)
        bit >>= 1
        if bit == 1:
            pieces[0] = own
    pieces[0] = own
    return pieces


def make_on_device(n_dom, n_ens):
    vmem = pl.BlockSpec(memory_space=pltpu.VMEM)
    hbm = pl.BlockSpec(memory_space=pltpu.HBM)
    direct = n_dom <= DIRECT_DOM
    paired = is_paired(n_dom, n_ens)
    halves = has_halves(n_ens)
    limit = VMEM_LIMIT if direct else None

    def call(kernel, out_shape, operands, specs=None, scratch=(), out_spec=vmem):
        many = isinstance(out_shape, (list, tuple))
        return pl.pallas_call(
            kernel,
            out_shape=out_shape,
            in_specs=specs or [vmem] * len(operands),
            out_specs=[out_spec] * len(out_shape) if many else out_spec,
            scratch_shapes=list(scratch),
            compiler_params=pltpu.CompilerParams(vmem_limit_bytes=limit),
        )(*operands)

    def in_hbm(value):
        return pltpu.with_memory_space_constraint(value, pltpu.HBM)

    def shape(dims, dtype=F32):
        return jax.ShapeDtypeStruct(dims, dtype)

    def on_device(state, coords, owner_local, counts, obs_value, obs_weight):
        local_members, elements, nodes = state.shape
        slots = coords.shape[1]
        members = local_members * n_ens
        tile_shape = (8, 2 * CAP)
        inputs = [counts, coords, owner_local[None], obs_value[None], obs_weight[None]]
        tiles = call(
            lambda *refs: pack_kernel(direct, paired, *refs),
            [shape(tile_shape)] * (3 if paired else n_dom)
            if direct
            else [shape((n_dom,) + tile_shape)],
            [in_hbm(value) for value in inputs],
            [hbm] * len(inputs),
            [
                pltpu.SMEM(counts.shape, jnp.int32),
                pltpu.VMEM(coords.shape, F32),
                pltpu.VMEM((1, slots), jnp.int32),
                pltpu.VMEM((1, slots), F32),
                pltpu.VMEM((1, slots), F32),
                pltpu.VMEM((8, slots), F32),
                pltpu.SemaphoreType.DMA((5,)),
            ],
        )
        if direct:
            tiles = spread(tiles, n_dom, n_ens)
        else:
            moved = lax.all_to_all(tiles[0], "dom", split_axis=0, concat_axis=0, tiled=True)
            tiles = [moved[d] for d in range(n_dom)]
        own = call(
            fetch_kernel, shape(state.shape), [in_hbm(state)], [hbm], [pltpu.SemaphoreType.DMA(())]
        )
        pieces = gather_members(state, own, n_ens)
        sensor_count = CAP * (n_dom + n_dom % 2)
        order = key_order(n_ens)
        local = order[: n_ens // 2] if halves else order
        sensors, high, low, values = call(
            lambda *refs: values_kernel(paired, n_dom, *refs),
            [
                shape((8, sensor_count)),
                shape((nodes, sensor_count), BF16),
                shape((nodes, sensor_count), BF16),
                shape((local_members, sensor_count)),
            ],
            list(tiles) + [pieces[0]],
        )
        if len(local) > 1:
            values = call(
                reach_kernel,
                shape((len(local) * local_members, sensor_count)),
                [sensors, high, low, values] + [pieces[key] for key in local[1:]],
            )
        values = [values]
        if halves:
            pairs = [(e, e ^ 1) for e in range(n_ens)]
            values.append(lax.ppermute(values[0], "ens", pairs))
        partial_sum = call(
            lambda *refs: cross_kernel(halves, *refs), shape((members, LANES)), [sensors] + values
        )
        if direct:
            copies = [partial_sum] * (3 if paired else n_dom)
            sums = spread(copies, n_dom, n_ens, bits=(2, 3, 1), crossing=0)
        else:
            sums = [lax.psum(partial_sum, "dom")]
        return call(
            lambda *refs: mix_kernel(halves, len(sums), *refs),
            shape(state.shape),
            sums + [pieces[key] for key in range(n_ens)],
            None,
            [
                pltpu.VMEM(state.shape, F32),
                pltpu.VMEM((members * local_members, 8, 128), F32),
                pltpu.SemaphoreType.DMA((elements // 8,)),
            ],
            hbm,
        )

    return on_device


def solution(mesh):
    n_dom, n_ens = mesh.shape["dom"], mesh.shape["ens"]
    return jax.shard_map(
        make_on_device(n_dom, n_ens),
        mesh=mesh,
        in_specs=(
            P("ens", ("groups", "dom"), None),
            P(None, ("groups", "dom")),
            P(("groups", "dom")),
            P(("groups", "dom"), None),
            P(("groups", "dom")),
            P(("groups", "dom")),
        ),
        out_specs=P("ens", ("groups", "dom"), None),
        check_vma=False,
    )
```

```python
import jax
import jax.numpy as jnp
from jax import lax
from jax.experimental import pallas as pl
from jax.experimental.pallas import tpu as pltpu
from jax.sharding import PartitionSpec as P


CAP = 64
NS_ITERS = 8


GLL_POINTS = (
    -1.0,
    -0.8717401485096066,
    -0.5917001814331423,
    -0.2092992179024789,
    0.2092992179024789,
    0.5917001814331423,
    0.8717401485096066,
    1.0,
)
INFLATION = 1.1
ORDER = len(GLL_POINTS)
F32 = jnp.float32
BF16 = jnp.bfloat16
DIRECT_DOM = 8
VMEM_LIMIT = 8 * 1024 * 1024
LANES = 128
PROJECT_LANES = 8
TRACE_LANE = 64


def lagrange_scale(index):
    product = 1.0
    for other in range(ORDER):
        if other != index:
            product *= GLL_POINTS[index] - GLL_POINTS[other]
    return 1.0 / product


def lagrange_rows(position):
    shape = (ORDER, position.shape[1])
    node = lax.broadcasted_iota(jnp.int32, shape, 0)
    product = jnp.full(shape, lagrange_scale(0), F32)
    for index in range(1, ORDER):
        product = jnp.where(node == index, lagrange_scale(index), product)
    for other in range(ORDER):
        product = product * jnp.where(node == other, 1.0, position - GLL_POINTS[other])
    return product


def split(value):
    high = value.astype(BF16)
    low = (value - high.astype(F32)).astype(BF16)
    return high, low


def is_odd(halves):
    return lax.rem(lax.axis_index("ens"), 2) if halves else 0


def fetch_kernel(state, own, sem):
    copy = pltpu.make_async_copy(state, own, sem)
    copy.start()
    copy.wait()


def pack_kernel(direct, paired, counts, coords, owner, obs, weight, *rest):
    outs = rest[:-7]
    count_box, coord_box, owner_box, obs_box, weight_box, block, sems = rest[-7:]
    pairs = zip(
        (counts, coords, owner, obs, weight), (count_box, coord_box, owner_box, obs_box, weight_box)
    )
    copies = [
        pltpu.make_async_copy(source, target, sems.at[index])
        for index, (source, target) in enumerate(pairs)
    ]
    for copy in copies:
        copy.start()
    n_dom = counts.shape[1]
    slots = coords.shape[1]
    here = lax.axis_index("dom")
    block[...] = jnp.zeros(block.shape, F32)
    column = lax.broadcasted_iota(jnp.int32, (8, 2 * CAP), 1)
    for copy in copies:
        copy.wait()
    block[0:3, :] = coord_box[...]
    block[3:4, :] = owner_box[...].astype(F32)
    block[4:5, :] = obs_box[...]
    block[5:6, :] = weight_box[...]
    rows = block[...]

    def tile(target, half):
        start = jnp.int32(0)
        for other in range(n_dom):
            start = start + jnp.where(other < target, count_box[0, other], 0)
        count = count_box[0, target]
        turned = pltpu.roll(rows, lax.rem(half - start + slots, slots), axis=1)[:, : 2 * CAP]
        return jnp.where((column >= half) & (column < half + count), turned, 0.0)

    if paired:
        near = jnp.where(is_odd(paired) == 0, 1, 3)
        for out, bits, half in zip(outs, (0, near, 2), (0, CAP, 0)):
            out[...] = tile(jnp.bitwise_xor(here, bits), half)
    elif direct:
        for shift in range(n_dom):
            outs[shift][...] = tile(lax.rem(here + shift, n_dom), (shift % 2) * CAP)
    else:
        half = lax.rem(here, 2) * CAP

        def step(target, carry):
            outs[0][target] = tile(target, half)
            return carry

        lax.fori_loop(0, n_dom, step, 0)


def pick(refs, sensors, high, low):
    members, elements, nodes = refs[0].shape
    rows = jnp.concatenate([ref[...].reshape(members * elements, nodes) for ref in refs], axis=0)
    rows_high, rows_low = split(rows)
    both = jnp.dot(
        jnp.concatenate([rows_high, rows_low], axis=0), high, preferred_element_type=F32
    )
    partial = (
        both[: rows.shape[0]]
        + both[rows.shape[0] :]
        + jnp.dot(rows_high, low, preferred_element_type=F32)
    )
    ids = lax.broadcasted_iota(jnp.int32, (elements, sensors.shape[1]), 0).astype(F32)
    partial = partial.reshape(len(refs) * members, elements, partial.shape[1])
    return jnp.sum(jnp.where((ids == sensors[3:4, :])[None], partial, 0.0), axis=1)


def values_kernel(paired, tile_count, *refs):
    tiles, state_refs = refs[:tile_count], refs[tile_count:-4]
    sensors_out, high_out, low_out, values_out = refs[-4:]
    blocks = [ref[...] for ref in tiles]
    if paired:
        here, near, far, other = blocks
        odd = is_odd(paired) == 1
        blocks = [here, jnp.where(odd, other, near), far, jnp.where(odd, near, other)]
    pairs = []
    for first in range(0, tile_count, 2):
        pair = blocks[first]
        if first + 1 < tile_count:
            pair = pair + blocks[first + 1]
        pairs.append(pair)
    sensors = jnp.concatenate(pairs, axis=1) if len(pairs) > 1 else pairs[0]
    sensors_out[...] = sensors
    along_r = lagrange_rows(sensors[0:1, :])
    along_s = lagrange_rows(sensors[1:2, :])
    along_t = lagrange_rows(sensors[2:3, :])
    for t in range(ORDER):
        for s in range(0, ORDER, 2):
            rows = [along_r * (along_t[t : t + 1, :] * along_s[k : k + 1, :]) for k in (s, s + 1)]
            high, low = split(jnp.concatenate(rows, axis=0))
            base = ORDER * ORDER * t + ORDER * s
            high_out[base : base + 2 * ORDER, :] = high
            low_out[base : base + 2 * ORDER, :] = low
    values_out[...] = pick(state_refs, sensors, high_out[...], low_out[...])


def reach_kernel(sensors_ref, high_ref, low_ref, values_ref, *refs):
    state_refs, out = refs[:-1], refs[-1]
    first = values_ref.shape[0]
    out[:first, :] = values_ref[...]
    out[first:, :] = pick(state_refs, sensors_ref[...], high_ref[...], low_ref[...])


def cross_kernel(halves, sensors_ref, *refs):
    value_refs, out = refs[:-1], refs[-1]
    sensors = sensors_ref[...]
    values = jnp.concatenate([ref[...] for ref in value_refs], axis=0)
    total = values.shape[0]
    if halves:
        turned = jnp.concatenate([ref[...] for ref in value_refs[::-1]], axis=0)
        values = jnp.where(is_odd(halves) == 1, turned, values)
    mean_value = jnp.sum(values, axis=0, keepdims=True) * (1.0 / total)
    anomaly = values - mean_value
    weighted = anomaly * sensors[5:6, :]
    innovation = sensors[4:5, :] - mean_value
    pad = jnp.zeros((PROJECT_LANES - 1, values.shape[1]), F32)
    right = jnp.concatenate([anomaly, innovation, pad], axis=0)
    left_high, left_low = split(weighted)
    right_high, right_low = split(right)
    across = (((1,), (1,)), ((), ()))
    both = lax.dot_general(
        jnp.concatenate([left_high, left_low], axis=0),
        right_high,
        across,
        preferred_element_type=F32,
    )
    out[:, : total + PROJECT_LANES] = (
        both[:total]
        + both[total:]
        + lax.dot_general(left_high, right_low, across, preferred_element_type=F32)
    )
    trace_part = jnp.sum(jnp.sum(weighted * anomaly, axis=0, keepdims=True), axis=1, keepdims=True)
    out[:, TRACE_LANE:] = jnp.broadcast_to(trace_part, (total, LANES - TRACE_LANE))


def lane_gather(value, lanes):
    return jnp.take_along_axis(value, lanes, axis=1, mode="promise_in_bounds")


def sublane_total(value):
    for shift in (4, 2, 1):
        value = value + pltpu.roll(value, shift, axis=0)
    return value


def mix_kernel(halves, sum_count, *refs):
    sums, state_refs = refs[:sum_count], refs[sum_count:-4]
    out, staged, splats, sems = refs[-4:]
    local_members, elements, nodes = out.shape
    members = local_members * len(state_refs)
    tile = (8, LANES)
    sub = lax.broadcasted_iota(jnp.int32, tile, 0)
    lane = lax.broadcasted_iota(jnp.int32, tile, 1)
    left_lanes = [(lane // members) * members + (sub + 8 * g) for g in range(2)]
    right_lanes = sub * members + lane % members
    identity = [(lane // members + 8 * h == lane % members).astype(F32) for h in range(2)]

    def as_left(matrix):
        return [[lane_gather(matrix[h], left_lanes[g]) for g in range(2)] for h in range(2)]

    def as_right(matrix):
        return [lane_gather(matrix[g], right_lanes) for g in range(2)]

    def product(left, right):
        return [sublane_total(left[h][0] * right[0] + left[h][1] * right[1]) for h in range(2)]

    total_sum = sums[0][...]
    for ref in sums[1:]:
        total_sum = total_sum + ref[...]
    rows = [total_sum[8 * g : 8 * g + 8, :] for g in range(2)]
    project = [lane_gather(rows[g], jnp.full(tile, members, jnp.int32)) for g in range(2)]
    trace_value = lane_gather(rows[0], jnp.full(tile, TRACE_LANE, jnp.int32))
    scale = 1.0 / (trace_value + members * ((members - 1) / INFLATION))
    diagonal = (members - 1) / INFLATION
    unit_left = [[(lane // members + 8 * h == sub + 8 * g).astype(F32) for g in range(2)] for h in range(2)]
    unit_right = [(lane % members == sub + 8 * g).astype(F32) for g in range(2)]
    system_left = [
        [
            (lane_gather(rows[g], lane // members + 8 * h) + diagonal * unit_left[h][g]) * scale
            for g in range(2)
        ]
        for h in range(2)
    ]
    system_right = [
        (lane_gather(rows[g], lane % members) + diagonal * unit_right[g]) * scale for g in range(2)
    ]
    inverse_left = [
        [1.5 * unit_left[h][g] - 0.5 * system_left[h][g] for g in range(2)] for h in range(2)
    ]
    inverse_right = [1.5 * unit_right[g] - 0.5 * system_right[g] for g in range(2)]
    iterate = product(system_left, inverse_right)
    for sweep in range(1, NS_ITERS):
        step = product(inverse_left, as_right(iterate))
        middle = [1.5 * identity[h] - 0.5 * step[h] for h in range(2)]
        middle_left = as_left(middle)
        inverse_root = product(middle_left, inverse_right)
        if sweep + 1 < NS_ITERS:
            iterate = product(as_left(iterate), as_right(middle))
            inverse_left, inverse_right = as_left(inverse_root), as_right(inverse_root)
        else:
            solved = product(middle_left, as_right(product(inverse_left, project)))
            ones = [jnp.ones(tile, F32)] * 2
            row_sums = product(middle_left, as_right(product(inverse_left, ones)))
    solved, row_sums, inverse_right = as_right(solved), as_right(row_sums), as_right(inverse_root)
    mean_weights = product(as_left(inverse_root), solved)
    root_scale = jnp.sqrt((members - 1) * scale)
    weights_mean = sublane_total(row_sums[0] * solved[0] + row_sums[1] * solved[1])
    column_sum = sublane_total(inverse_right[0] + inverse_right[1])
    shift = (1.0 - column_sum * root_scale - weights_mean * scale) * (1.0 / members)
    mixing = [
        inverse_root[h] * root_scale + mean_weights[h] * scale + shift for h in range(2)
    ]
    odd = is_odd(halves)
    order = key_order(len(state_refs))
    own_place = odd * order.index(1) if halves else 0
    for k in range(local_members):
        lanes = sub * members + (k + local_members * own_place)
        for h in range(2):
            column = lane_gather(mixing[h], lanes)
            for i in range(8):
                splats[(8 * h + i) * local_members + k] = jnp.broadcast_to(column[i : i + 1, :], tile)
    places = []
    for piece in range(len(state_refs)):
        place = order.index(piece)
        places.append(place + odd * (order.index(piece ^ 1) - place) if halves else place)

    def output_copies(block):
        place = pl.ds(pl.multiple_of(8 * block, 8), 8)
        return [
            pltpu.make_async_copy(staged.at[k, place], out.at[k, place], sems.at[block, k])
            for k in range(local_members)
        ]

    def mix_block(block, carry):
        span = pl.ds(pl.multiple_of(8 * block, 8), 8)
        for first in range(0, nodes, 2 * LANES):
            spans = [slice(first + LANES * u, first + LANES * (u + 1)) for u in range(2)]
            totals = [[None, None] for _ in range(local_members)]
            for j in range(members):
                piece, member = divmod(j, local_members)
                values = [state_refs[piece][member, span, lanes] for lanes in spans]
                for k in range(local_members):
                    factor = splats[(places[piece] * local_members + member) * local_members + k]
                    for u in range(2):
                        term = factor * values[u]
                        totals[k][u] = term if j == 0 else totals[k][u] + term
            for k in range(local_members):
                for u in range(2):
                    staged[k, span, spans[u]] = totals[k][u]
        for copy in output_copies(block):
            copy.start()
        return carry

    def wait_block(block, carry):
        for copy in output_copies(block):
            copy.wait()
        return carry

    lax.fori_loop(0, elements // 8, mix_block, 0)
    lax.fori_loop(0, elements // 8, wait_block, 0)


def has_halves(n_ens):
    return n_ens > 1 and n_ens & (n_ens - 1) == 0


def is_paired(n_dom, n_ens):
    return n_dom == 4 and has_halves(n_ens)


def key_order(n_ens):
    if not has_halves(n_ens):
        return list(range(n_ens))
    return list(range(0, n_ens, 2)) + list(range(1, n_ens, 2))


def spread(values, n_dom, n_ens, bits=(1, 3, 2), crossing=0):
    if not is_paired(n_dom, n_ens):
        return [values[0]] + [
            lax.ppermute(values[s], "dom", [(d, (d + s) % n_dom) for d in range(n_dom)])
            for s in range(1, n_dom)
        ]
    here, near, far = values
    near_pairs, far_pairs = [], []
    for d in range(n_dom):
        for e in range(n_ens):
            near_pairs.append((d * n_ens + e, (d ^ bits[e % 2]) * n_ens + e))
            far_pairs.append((d * n_ens + e, (d ^ bits[2]) * n_ens + (e ^ crossing)))
    near = lax.ppermute(near, ("dom", "ens"), near_pairs)
    far = lax.ppermute(far, ("dom", "ens"), far_pairs)
    other = lax.ppermute(near, "ens", [(e, e ^ 1) for e in range(n_ens)])
    return [here, near, far, other]


def gather_members(state, own, n_ens):
    pieces = {0: state}
    if not has_halves(n_ens):
        for shift in range(1, n_ens):
            pairs = [(e, (e + shift) % n_ens) for e in range(n_ens)]
            pieces[shift] = lax.ppermute(state, "ens", pairs)
        pieces[0] = own
        return pieces
    bit = n_ens >> 1
    while bit:
        pairs = [(e, e ^ bit) for e in range(n_ens)]
        for key in list(pieces):
            pieces[key ^ bit] = lax.ppermute(pieces[key], "ens", pairs)
        bit >>= 1
        if bit == 1:
            pieces[0] = own
    pieces[0] = own
    return pieces


def make_on_device(n_dom, n_ens):
    vmem = pl.BlockSpec(memory_space=pltpu.VMEM)
    hbm = pl.BlockSpec(memory_space=pltpu.HBM)
    direct = n_dom <= DIRECT_DOM
    paired = is_paired(n_dom, n_ens)
    halves = has_halves(n_ens)
    limit = VMEM_LIMIT if direct else None

    def call(kernel, out_shape, operands, specs=None, scratch=(), out_spec=vmem):
        many = isinstance(out_shape, (list, tuple))
        return pl.pallas_call(
            kernel,
            out_shape=out_shape,
            in_specs=specs or [vmem] * len(operands),
            out_specs=[out_spec] * len(out_shape) if many else out_spec,
            scratch_shapes=list(scratch),
            compiler_params=pltpu.CompilerParams(vmem_limit_bytes=limit),
        )(*operands)

    def in_hbm(value):
        return pltpu.with_memory_space_constraint(value, pltpu.HBM)

    def shape(dims, dtype=F32):
        return jax.ShapeDtypeStruct(dims, dtype)

    def on_device(state, coords, owner_local, counts, obs_value, obs_weight):
        local_members, elements, nodes = state.shape
        slots = coords.shape[1]
        members = local_members * n_ens
        tile_shape = (8, 2 * CAP)
        inputs = [counts, coords, owner_local[None], obs_value[None], obs_weight[None]]
        tiles = call(
            lambda *refs: pack_kernel(direct, paired, *refs),
            [shape(tile_shape)] * (3 if paired else n_dom)
            if direct
            else [shape((n_dom,) + tile_shape)],
            [in_hbm(value) for value in inputs],
            [hbm] * len(inputs),
            [
                pltpu.SMEM(counts.shape, jnp.int32),
                pltpu.VMEM(coords.shape, F32),
                pltpu.VMEM((1, slots), jnp.int32),
                pltpu.VMEM((1, slots), F32),
                pltpu.VMEM((1, slots), F32),
                pltpu.VMEM((8, slots), F32),
                pltpu.SemaphoreType.DMA((5,)),
            ],
        )
        if direct:
            tiles = spread(tiles, n_dom, n_ens)
        else:
            moved = lax.all_to_all(tiles[0], "dom", split_axis=0, concat_axis=0, tiled=True)
            tiles = [moved[d] for d in range(n_dom)]
        own = call(
            fetch_kernel, shape(state.shape), [in_hbm(state)], [hbm], [pltpu.SemaphoreType.DMA(())]
        )
        pieces = gather_members(state, own, n_ens)
        sensor_count = CAP * (n_dom + n_dom % 2)
        order = key_order(n_ens)
        local = order[: n_ens // 2] if halves else order
        sensors, high, low, values = call(
            lambda *refs: values_kernel(paired, n_dom, *refs),
            [
                shape((8, sensor_count)),
                shape((nodes, sensor_count), BF16),
                shape((nodes, sensor_count), BF16),
                shape((local_members, sensor_count)),
            ],
            list(tiles) + [pieces[0]],
        )
        if len(local) > 1:
            values = call(
                reach_kernel,
                shape((len(local) * local_members, sensor_count)),
                [sensors, high, low, values] + [pieces[key] for key in local[1:]],
            )
        values = [values]
        if halves:
            pairs = [(e, e ^ 1) for e in range(n_ens)]
            values.append(lax.ppermute(values[0], "ens", pairs))
        partial_sum = call(
            lambda *refs: cross_kernel(halves, *refs), shape((members, LANES)), [sensors] + values
        )
        if direct:
            copies = [partial_sum] * (3 if paired else n_dom)
            sums = spread(copies, n_dom, n_ens, bits=(2, 3, 1), crossing=1)
        else:
            sums = [lax.psum(partial_sum, "dom")]
        return call(
            lambda *refs: mix_kernel(halves, len(sums), *refs),
            shape(state.shape),
            sums + [pieces[key] for key in range(n_ens)],
            None,
            [
                pltpu.VMEM(state.shape, F32),
                pltpu.VMEM((members * local_members, 8, 128), F32),
                pltpu.SemaphoreType.DMA((elements // 8, local_members)),
            ],
            hbm,
        )

    return on_device


def solution(mesh):
    n_dom, n_ens = mesh.shape["dom"], mesh.shape["ens"]
    return jax.shard_map(
        make_on_device(n_dom, n_ens),
        mesh=mesh,
        in_specs=(
            P("ens", ("groups", "dom"), None),
            P(None, ("groups", "dom")),
            P(("groups", "dom")),
            P(("groups", "dom"), None),
            P(("groups", "dom")),
            P(("groups", "dom")),
        ),
        out_specs=P("ens", ("groups", "dom"), None),
        check_vma=False,
    )
```

```python
import jax
import jax.numpy as jnp
from jax import lax
from jax.experimental import pallas as pl
from jax.experimental.pallas import tpu as pltpu
from jax.sharding import PartitionSpec as P


CAP = 64
NS_ITERS = 8


GLL_POINTS = (
    -1.0,
    -0.8717401485096066,
    -0.5917001814331423,
    -0.2092992179024789,
    0.2092992179024789,
    0.5917001814331423,
    0.8717401485096066,
    1.0,
)
INFLATION = 1.1
ORDER = len(GLL_POINTS)
F32 = jnp.float32
BF16 = jnp.bfloat16
DIRECT_DOM = 8
VMEM_LIMIT = 8 * 1024 * 1024
LANES = 128
PROJECT_LANES = 8
TRACE_LANE = 64


def lagrange_scale(index):
    product = 1.0
    for other in range(ORDER):
        if other != index:
            product *= GLL_POINTS[index] - GLL_POINTS[other]
    return 1.0 / product


def lagrange_rows(position):
    shape = (ORDER, position.shape[1])
    node = lax.broadcasted_iota(jnp.int32, shape, 0)
    product = jnp.full(shape, lagrange_scale(0), F32)
    for index in range(1, ORDER):
        product = jnp.where(node == index, lagrange_scale(index), product)
    for other in range(ORDER):
        product = product * jnp.where(node == other, 1.0, position - GLL_POINTS[other])
    return product


def split(value):
    high = value.astype(BF16)
    low = (value - high.astype(F32)).astype(BF16)
    return high, low


def is_odd(halves):
    return lax.rem(lax.axis_index("ens"), 2) if halves else 0


def fetch_kernel(state, own, sem):
    copy = pltpu.make_async_copy(state, own, sem)
    copy.start()
    copy.wait()


def pack_kernel(direct, paired, counts, coords, owner, obs, weight, *rest):
    outs = rest[:-7]
    count_box, coord_box, owner_box, obs_box, weight_box, block, sems = rest[-7:]
    pairs = zip(
        (counts, coords, owner, obs, weight), (count_box, coord_box, owner_box, obs_box, weight_box)
    )
    copies = [
        pltpu.make_async_copy(source, target, sems.at[index])
        for index, (source, target) in enumerate(pairs)
    ]
    for copy in copies:
        copy.start()
    n_dom = counts.shape[1]
    slots = coords.shape[1]
    here = lax.axis_index("dom")
    block[...] = jnp.zeros(block.shape, F32)
    column = lax.broadcasted_iota(jnp.int32, (8, 2 * CAP), 1)
    for copy in copies:
        copy.wait()
    block[0:3, :] = coord_box[...]
    block[3:4, :] = owner_box[...].astype(F32)
    block[4:5, :] = obs_box[...]
    block[5:6, :] = weight_box[...]
    rows = block[...]

    def tile(target, half):
        start = jnp.int32(0)
        for other in range(n_dom):
            start = start + jnp.where(other < target, count_box[0, other], 0)
        count = count_box[0, target]
        turned = pltpu.roll(rows, lax.rem(half - start + slots, slots), axis=1)[:, : 2 * CAP]
        return jnp.where((column >= half) & (column < half + count), turned, 0.0)

    if paired:
        near = jnp.where(is_odd(paired) == 0, 2, 3)
        for out, bits, half in zip(outs, (0, near, 1), (0, CAP, 0)):
            out[...] = tile(jnp.bitwise_xor(here, bits), half)
    elif direct:
        for shift in range(n_dom):
            outs[shift][...] = tile(lax.rem(here + shift, n_dom), (shift % 2) * CAP)
    else:
        half = lax.rem(here, 2) * CAP

        def step(target, carry):
            outs[0][target] = tile(target, half)
            return carry

        lax.fori_loop(0, n_dom, step, 0)


def pick(refs, sensors, high, low):
    members, elements, nodes = refs[0].shape
    rows = jnp.concatenate([ref[...].reshape(members * elements, nodes) for ref in refs], axis=0)
    rows_high, rows_low = split(rows)
    both = jnp.dot(
        jnp.concatenate([rows_high, rows_low], axis=0), high, preferred_element_type=F32
    )
    partial = (
        both[: rows.shape[0]]
        + both[rows.shape[0] :]
        + jnp.dot(rows_high, low, preferred_element_type=F32)
    )
    ids = lax.broadcasted_iota(jnp.int32, (elements, sensors.shape[1]), 0).astype(F32)
    partial = partial.reshape(len(refs) * members, elements, partial.shape[1])
    return jnp.sum(jnp.where((ids == sensors[3:4, :])[None], partial, 0.0), axis=1)


def values_kernel(paired, tile_count, *refs):
    tiles, state_refs = refs[:tile_count], refs[tile_count:-4]
    sensors_out, high_out, low_out, values_out = refs[-4:]
    blocks = [ref[...] for ref in tiles]
    if paired:
        here, near, far, other = blocks
        odd = is_odd(paired) == 1
        blocks = [here, jnp.where(odd, other, near), far, jnp.where(odd, near, other)]
    pairs = []
    for first in range(0, tile_count, 2):
        pair = blocks[first]
        if first + 1 < tile_count:
            pair = pair + blocks[first + 1]
        pairs.append(pair)
    sensors = jnp.concatenate(pairs, axis=1) if len(pairs) > 1 else pairs[0]
    sensors_out[...] = sensors
    along_r = lagrange_rows(sensors[0:1, :])
    along_s = lagrange_rows(sensors[1:2, :])
    along_t = lagrange_rows(sensors[2:3, :])
    for t in range(ORDER):
        for s in range(0, ORDER, 2):
            rows = [along_r * (along_t[t : t + 1, :] * along_s[k : k + 1, :]) for k in (s, s + 1)]
            high, low = split(jnp.concatenate(rows, axis=0))
            base = ORDER * ORDER * t + ORDER * s
            high_out[base : base + 2 * ORDER, :] = high
            low_out[base : base + 2 * ORDER, :] = low
    values_out[...] = pick(state_refs, sensors, high_out[...], low_out[...])


def reach_kernel(sensors_ref, high_ref, low_ref, values_ref, *refs):
    state_refs, out = refs[:-1], refs[-1]
    first = values_ref.shape[0]
    out[:first, :] = values_ref[...]
    out[first:, :] = pick(state_refs, sensors_ref[...], high_ref[...], low_ref[...])


def cross_kernel(halves, sensors_ref, *refs):
    value_refs, out = refs[:-1], refs[-1]
    sensors = sensors_ref[...]
    values = jnp.concatenate([ref[...] for ref in value_refs], axis=0)
    total = values.shape[0]
    if halves:
        turned = jnp.concatenate([ref[...] for ref in value_refs[::-1]], axis=0)
        values = jnp.where(is_odd(halves) == 1, turned, values)
    mean_value = jnp.sum(values, axis=0, keepdims=True) * (1.0 / total)
    anomaly = values - mean_value
    weighted = anomaly * sensors[5:6, :]
    innovation = sensors[4:5, :] - mean_value
    pad = jnp.zeros((PROJECT_LANES - 1, values.shape[1]), F32)
    right = jnp.concatenate([anomaly, innovation, pad], axis=0)
    left_high, left_low = split(weighted)
    right_high, right_low = split(right)
    across = (((1,), (1,)), ((), ()))
    both = lax.dot_general(
        jnp.concatenate([left_high, left_low], axis=0),
        right_high,
        across,
        preferred_element_type=F32,
    )
    out[:, : total + PROJECT_LANES] = (
        both[:total]
        + both[total:]
        + lax.dot_general(left_high, right_low, across, preferred_element_type=F32)
    )
    trace_part = jnp.sum(jnp.sum(weighted * anomaly, axis=0, keepdims=True), axis=1, keepdims=True)
    out[:, TRACE_LANE:] = jnp.broadcast_to(trace_part, (total, LANES - TRACE_LANE))


def lane_gather(value, lanes):
    return jnp.take_along_axis(value, lanes, axis=1, mode="promise_in_bounds")


def sublane_total(value):
    for shift in (4, 2, 1):
        value = value + pltpu.roll(value, shift, axis=0)
    return value


def mix_kernel(halves, sum_count, *refs):
    sums, state_refs = refs[:sum_count], refs[sum_count:-4]
    out, staged, splats, sems = refs[-4:]
    local_members, elements, nodes = out.shape
    members = local_members * len(state_refs)
    tile = (8, LANES)
    sub = lax.broadcasted_iota(jnp.int32, tile, 0)
    lane = lax.broadcasted_iota(jnp.int32, tile, 1)
    left_lanes = [(lane // members) * members + (sub + 8 * g) for g in range(2)]
    right_lanes = sub * members + lane % members
    identity = [(lane // members + 8 * h == lane % members).astype(F32) for h in range(2)]

    def as_left(matrix):
        return [[lane_gather(matrix[h], left_lanes[g]) for g in range(2)] for h in range(2)]

    def as_right(matrix):
        return [lane_gather(matrix[g], right_lanes) for g in range(2)]

    def product(left, right):
        return [sublane_total(left[h][0] * right[0] + left[h][1] * right[1]) for h in range(2)]

    total_sum = sums[0][...]
    for ref in sums[1:]:
        total_sum = total_sum + ref[...]
    rows = [total_sum[8 * g : 8 * g + 8, :] for g in range(2)]
    project = [lane_gather(rows[g], jnp.full(tile, members, jnp.int32)) for g in range(2)]
    trace_value = lane_gather(rows[0], jnp.full(tile, TRACE_LANE, jnp.int32))
    scale = 1.0 / (trace_value + members * ((members - 1) / INFLATION))
    diagonal = (members - 1) / INFLATION
    unit_left = [[(lane // members + 8 * h == sub + 8 * g).astype(F32) for g in range(2)] for h in range(2)]
    unit_right = [(lane % members == sub + 8 * g).astype(F32) for g in range(2)]
    system_left = [
        [
            (lane_gather(rows[g], lane // members + 8 * h) + diagonal * unit_left[h][g]) * scale
            for g in range(2)
        ]
        for h in range(2)
    ]
    system_right = [
        (lane_gather(rows[g], lane % members) + diagonal * unit_right[g]) * scale for g in range(2)
    ]
    inverse_left = [
        [1.5 * unit_left[h][g] - 0.5 * system_left[h][g] for g in range(2)] for h in range(2)
    ]
    inverse_right = [1.5 * unit_right[g] - 0.5 * system_right[g] for g in range(2)]
    iterate = product(system_left, inverse_right)
    for sweep in range(1, NS_ITERS):
        step = product(inverse_left, as_right(iterate))
        middle = [1.5 * identity[h] - 0.5 * step[h] for h in range(2)]
        middle_left = as_left(middle)
        inverse_root = product(middle_left, inverse_right)
        if sweep + 1 < NS_ITERS:
            iterate = product(as_left(iterate), as_right(middle))
            inverse_left, inverse_right = as_left(inverse_root), as_right(inverse_root)
        else:
            solved = product(middle_left, as_right(product(inverse_left, project)))
            ones = [jnp.ones(tile, F32)] * 2
            row_sums = product(middle_left, as_right(product(inverse_left, ones)))
    solved, row_sums, inverse_right = as_right(solved), as_right(row_sums), as_right(inverse_root)
    mean_weights = product(as_left(inverse_root), solved)
    root_scale = jnp.sqrt((members - 1) * scale)
    weights_mean = sublane_total(row_sums[0] * solved[0] + row_sums[1] * solved[1])
    column_sum = sublane_total(inverse_right[0] + inverse_right[1])
    shift = (1.0 - column_sum * root_scale - weights_mean * scale) * (1.0 / members)
    mixing = [
        inverse_root[h] * root_scale + mean_weights[h] * scale + shift for h in range(2)
    ]
    odd = is_odd(halves)
    order = key_order(len(state_refs))
    own_place = odd * order.index(1) if halves else 0
    for k in range(local_members):
        lanes = sub * members + (k + local_members * own_place)
        for h in range(2):
            column = lane_gather(mixing[h], lanes)
            for i in range(8):
                splats[(8 * h + i) * local_members + k] = jnp.broadcast_to(column[i : i + 1, :], tile)
    places = []
    for piece in range(len(state_refs)):
        place = order.index(piece)
        places.append(place + odd * (order.index(piece ^ 1) - place) if halves else place)

    def output_copy(block):
        place = pl.ds(pl.multiple_of(8 * block, 8), 8)
        return pltpu.make_async_copy(staged.at[:, place], out.at[:, place], sems.at[block])

    def mix_block(block, carry):
        span = pl.ds(pl.multiple_of(8 * block, 8), 8)
        for first in range(0, nodes, 2 * LANES):
            spans = [slice(first + LANES * u, first + LANES * (u + 1)) for u in range(2)]
            totals = [[None, None] for _ in range(local_members)]
            for j in range(members):
                piece, member = divmod(j, local_members)
                values = [state_refs[piece][member, span, lanes] for lanes in spans]
                for k in range(local_members):
                    factor = splats[(places[piece] * local_members + member) * local_members + k]
                    for u in range(2):
                        term = factor * values[u]
                        totals[k][u] = term if j == 0 else totals[k][u] + term
            for k in range(local_members):
                for u in range(2):
                    staged[k, span, spans[u]] = totals[k][u]
        output_copy(block).start()
        return carry

    def wait_block(block, carry):
        output_copy(block).wait()
        return carry

    lax.fori_loop(0, elements // 8, mix_block, 0)
    lax.fori_loop(0, elements // 8, wait_block, 0)


def has_halves(n_ens):
    return n_ens > 1 and n_ens & (n_ens - 1) == 0


def is_paired(n_dom, n_ens):
    return n_dom == 4 and has_halves(n_ens)


def key_order(n_ens):
    if not has_halves(n_ens):
        return list(range(n_ens))
    return list(range(0, n_ens, 2)) + list(range(1, n_ens, 2))


def spread(values, n_dom, n_ens, bits=(1, 3, 2), crossing=0):
    if not is_paired(n_dom, n_ens):
        return [values[0]] + [
            lax.ppermute(values[s], "dom", [(d, (d + s) % n_dom) for d in range(n_dom)])
            for s in range(1, n_dom)
        ]
    here, near, far = values
    near_pairs, far_pairs = [], []
    for d in range(n_dom):
        for e in range(n_ens):
            near_pairs.append((d * n_ens + e, (d ^ bits[e % 2]) * n_ens + e))
            far_pairs.append((d * n_ens + e, (d ^ bits[2]) * n_ens + (e ^ crossing)))
    near = lax.ppermute(near, ("dom", "ens"), near_pairs)
    far = lax.ppermute(far, ("dom", "ens"), far_pairs)
    other = lax.ppermute(near, "ens", [(e, e ^ 1) for e in range(n_ens)])
    return [here, near, far, other]


def gather_members(state, own, n_ens):
    pieces = {0: state}
    if not has_halves(n_ens):
        for shift in range(1, n_ens):
            pairs = [(e, (e + shift) % n_ens) for e in range(n_ens)]
            pieces[shift] = lax.ppermute(state, "ens", pairs)
        pieces[0] = own
        return pieces
    bit = n_ens >> 1
    while bit:
        pairs = [(e, e ^ bit) for e in range(n_ens)]
        for key in list(pieces):
            pieces[key ^ bit] = lax.ppermute(pieces[key], "ens", pairs)
        bit >>= 1
        if bit == 1:
            pieces[0] = own
    pieces[0] = own
    return pieces


def make_on_device(n_dom, n_ens):
    vmem = pl.BlockSpec(memory_space=pltpu.VMEM)
    hbm = pl.BlockSpec(memory_space=pltpu.HBM)
    direct = n_dom <= DIRECT_DOM
    paired = is_paired(n_dom, n_ens)
    halves = has_halves(n_ens)
    limit = VMEM_LIMIT if direct else None

    def call(kernel, out_shape, operands, specs=None, scratch=(), out_spec=vmem):
        many = isinstance(out_shape, (list, tuple))
        return pl.pallas_call(
            kernel,
            out_shape=out_shape,
            in_specs=specs or [vmem] * len(operands),
            out_specs=[out_spec] * len(out_shape) if many else out_spec,
            scratch_shapes=list(scratch),
            compiler_params=pltpu.CompilerParams(vmem_limit_bytes=limit),
        )(*operands)

    def in_hbm(value):
        return pltpu.with_memory_space_constraint(value, pltpu.HBM)

    def shape(dims, dtype=F32):
        return jax.ShapeDtypeStruct(dims, dtype)

    def on_device(state, coords, owner_local, counts, obs_value, obs_weight):
        local_members, elements, nodes = state.shape
        slots = coords.shape[1]
        members = local_members * n_ens
        tile_shape = (8, 2 * CAP)
        inputs = [counts, coords, owner_local[None], obs_value[None], obs_weight[None]]
        tiles = call(
            lambda *refs: pack_kernel(direct, paired, *refs),
            [shape(tile_shape)] * (3 if paired else n_dom)
            if direct
            else [shape((n_dom,) + tile_shape)],
            [in_hbm(value) for value in inputs],
            [hbm] * len(inputs),
            [
                pltpu.SMEM(counts.shape, jnp.int32),
                pltpu.VMEM(coords.shape, F32),
                pltpu.VMEM((1, slots), jnp.int32),
                pltpu.VMEM((1, slots), F32),
                pltpu.VMEM((1, slots), F32),
                pltpu.VMEM((8, slots), F32),
                pltpu.SemaphoreType.DMA((5,)),
            ],
        )
        if direct:
            tiles = spread(tiles, n_dom, n_ens, bits=(2, 3, 1), crossing=1)
        else:
            moved = lax.all_to_all(tiles[0], "dom", split_axis=0, concat_axis=0, tiled=True)
            tiles = [moved[d] for d in range(n_dom)]
        own = call(
            fetch_kernel, shape(state.shape), [in_hbm(state)], [hbm], [pltpu.SemaphoreType.DMA(())]
        )
        pieces = gather_members(state, own, n_ens)
        sensor_count = CAP * (n_dom + n_dom % 2)
        order = key_order(n_ens)
        local = order[: n_ens // 2] if halves else order
        sensors, high, low, values = call(
            lambda *refs: values_kernel(paired, n_dom, *refs),
            [
                shape((8, sensor_count)),
                shape((nodes, sensor_count), BF16),
                shape((nodes, sensor_count), BF16),
                shape((local_members, sensor_count)),
            ],
            list(tiles) + [pieces[0]],
        )
        if len(local) > 1:
            values = call(
                reach_kernel,
                shape((len(local) * local_members, sensor_count)),
                [sensors, high, low, values] + [pieces[key] for key in local[1:]],
            )
        values = [values]
        if halves:
            pairs = [(e, e ^ 1) for e in range(n_ens)]
            values.append(lax.ppermute(values[0], "ens", pairs))
        partial_sum = call(
            lambda *refs: cross_kernel(halves, *refs), shape((members, LANES)), [sensors] + values
        )
        if direct:
            copies = [partial_sum] * (3 if paired else n_dom)
            sums = spread(copies, n_dom, n_ens, bits=(2, 3, 1), crossing=1)
        else:
            sums = [lax.psum(partial_sum, "dom")]
        return call(
            lambda *refs: mix_kernel(halves, len(sums), *refs),
            shape(state.shape),
            sums + [pieces[key] for key in range(n_ens)],
            None,
            [
                pltpu.VMEM(state.shape, F32),
                pltpu.VMEM((members * local_members, 8, 128), F32),
                pltpu.SemaphoreType.DMA((elements // 8,)),
            ],
            hbm,
        )

    return on_device


def solution(mesh):
    n_dom, n_ens = mesh.shape["dom"], mesh.shape["ens"]
    return jax.shard_map(
        make_on_device(n_dom, n_ens),
        mesh=mesh,
        in_specs=(
            P("ens", ("groups", "dom"), None),
            P(None, ("groups", "dom")),
            P(("groups", "dom")),
            P(("groups", "dom"), None),
            P(("groups", "dom")),
            P(("groups", "dom")),
        ),
        out_specs=P("ens", ("groups", "dom"), None),
        check_vma=False,
    )
```

```python
import jax
import jax.numpy as jnp
from jax import lax
from jax.experimental import pallas as pl
from jax.experimental.pallas import tpu as pltpu
from jax.sharding import PartitionSpec as P


CAP = 64
NS_ITERS = 8


GLL_POINTS = (
    -1.0,
    -0.8717401485096066,
    -0.5917001814331423,
    -0.2092992179024789,
    0.2092992179024789,
    0.5917001814331423,
    0.8717401485096066,
    1.0,
)
INFLATION = 1.1
ORDER = len(GLL_POINTS)
F32 = jnp.float32
BF16 = jnp.bfloat16
DIRECT_DOM = 8
VMEM_LIMIT = 8 * 1024 * 1024
LANES = 128
PROJECT_LANES = 8
TRACE_LANE = 64


def lagrange_scale(index):
    product = 1.0
    for other in range(ORDER):
        if other != index:
            product *= GLL_POINTS[index] - GLL_POINTS[other]
    return 1.0 / product


def lagrange_rows(position):
    shape = (ORDER, position.shape[1])
    node = lax.broadcasted_iota(jnp.int32, shape, 0)
    product = jnp.full(shape, lagrange_scale(0), F32)
    for index in range(1, ORDER):
        product = jnp.where(node == index, lagrange_scale(index), product)
    for other in range(ORDER):
        product = product * jnp.where(node == other, 1.0, position - GLL_POINTS[other])
    return product


def split(value):
    high = value.astype(BF16)
    low = (value - high.astype(F32)).astype(BF16)
    return high, low


def is_odd(halves):
    return lax.rem(lax.axis_index("ens"), 2) if halves else 0


def fetch_kernel(state, own, sem):
    copy = pltpu.make_async_copy(state, own, sem)
    copy.start()
    copy.wait()


def pack_kernel(direct, paired, counts, coords, owner, obs, weight, *rest):
    outs = rest[:-7]
    count_box, coord_box, owner_box, obs_box, weight_box, block, sems = rest[-7:]
    pairs = zip(
        (counts, coords, owner, obs, weight), (count_box, coord_box, owner_box, obs_box, weight_box)
    )
    copies = [
        pltpu.make_async_copy(source, target, sems.at[index])
        for index, (source, target) in enumerate(pairs)
    ]
    for copy in copies:
        copy.start()
    n_dom = counts.shape[1]
    slots = coords.shape[1]
    here = lax.axis_index("dom")
    block[...] = jnp.zeros(block.shape, F32)
    column = lax.broadcasted_iota(jnp.int32, (8, 2 * CAP), 1)
    for copy in copies:
        copy.wait()
    block[0:3, :] = coord_box[...]
    block[3:4, :] = owner_box[...].astype(F32)
    block[4:5, :] = obs_box[...]
    block[5:6, :] = weight_box[...]
    rows = block[...]

    def tile(target, half):
        start = jnp.int32(0)
        for other in range(n_dom):
            start = start + jnp.where(other < target, count_box[0, other], 0)
        count = count_box[0, target]
        turned = pltpu.roll(rows, lax.rem(half - start + slots, slots), axis=1)[:, : 2 * CAP]
        return jnp.where((column >= half) & (column < half + count), turned, 0.0)

    if paired:
        near = jnp.where(is_odd(paired) == 0, 1, 3)
        for out, bits, half in zip(outs, (0, near, 2), (0, CAP, 0)):
            out[...] = tile(jnp.bitwise_xor(here, bits), half)
    elif direct:
        for shift in range(n_dom):
            outs[shift][...] = tile(lax.rem(here + shift, n_dom), (shift % 2) * CAP)
    else:
        half = lax.rem(here, 2) * CAP

        def step(target, carry):
            outs[0][target] = tile(target, half)
            return carry

        lax.fori_loop(0, n_dom, step, 0)


def pick(refs, sensors, high, low):
    members, elements, nodes = refs[0].shape
    rows = jnp.concatenate([ref[...].reshape(members * elements, nodes) for ref in refs], axis=0)
    rows_high, rows_low = split(rows)
    both = jnp.dot(
        jnp.concatenate([rows_high, rows_low], axis=0), high, preferred_element_type=F32
    )
    partial = (
        both[: rows.shape[0]]
        + both[rows.shape[0] :]
        + jnp.dot(rows_high, low, preferred_element_type=F32)
    )
    ids = lax.broadcasted_iota(jnp.int32, (elements, sensors.shape[1]), 0).astype(F32)
    partial = partial.reshape(len(refs) * members, elements, partial.shape[1])
    return jnp.sum(jnp.where((ids == sensors[3:4, :])[None], partial, 0.0), axis=1)


def values_kernel(paired, tile_count, *refs):
    tiles, state_refs = refs[:tile_count], refs[tile_count:-4]
    sensors_out, high_out, low_out, values_out = refs[-4:]
    blocks = [ref[...] for ref in tiles]
    if paired:
        here, near, far, other = blocks
        odd = is_odd(paired) == 1
        blocks = [here, jnp.where(odd, other, near), far, jnp.where(odd, near, other)]
    pairs = []
    for first in range(0, tile_count, 2):
        pair = blocks[first]
        if first + 1 < tile_count:
            pair = pair + blocks[first + 1]
        pairs.append(pair)
    sensors = jnp.concatenate(pairs, axis=1) if len(pairs) > 1 else pairs[0]
    sensors_out[...] = sensors
    along_r = lagrange_rows(sensors[0:1, :])
    along_s = lagrange_rows(sensors[1:2, :])
    along_t = lagrange_rows(sensors[2:3, :])
    for t in range(ORDER):
        for s in range(0, ORDER, 2):
            rows = [along_r * (along_t[t : t + 1, :] * along_s[k : k + 1, :]) for k in (s, s + 1)]
            high, low = split(jnp.concatenate(rows, axis=0))
            base = ORDER * ORDER * t + ORDER * s
            high_out[base : base + 2 * ORDER, :] = high
            low_out[base : base + 2 * ORDER, :] = low
    values_out[...] = pick(state_refs, sensors, high_out[...], low_out[...])


def reach_kernel(sensors_ref, high_ref, low_ref, values_ref, *refs):
    state_refs, out = refs[:-1], refs[-1]
    first = values_ref.shape[0]
    out[:first, :] = values_ref[...]
    out[first:, :] = pick(state_refs, sensors_ref[...], high_ref[...], low_ref[...])


def cross_kernel(halves, sensors_ref, *refs):
    value_refs, out = refs[:-1], refs[-1]
    sensors = sensors_ref[...]
    values = jnp.concatenate([ref[...] for ref in value_refs], axis=0)
    total = values.shape[0]
    if halves:
        turned = jnp.concatenate([ref[...] for ref in value_refs[::-1]], axis=0)
        values = jnp.where(is_odd(halves) == 1, turned, values)
    mean_value = jnp.sum(values, axis=0, keepdims=True) * (1.0 / total)
    anomaly = values - mean_value
    weighted = anomaly * sensors[5:6, :]
    innovation = sensors[4:5, :] - mean_value
    pad = jnp.zeros((PROJECT_LANES - 1, values.shape[1]), F32)
    right = jnp.concatenate([anomaly, innovation, pad], axis=0)
    left_high, left_low = split(weighted)
    right_high, right_low = split(right)
    across = (((1,), (1,)), ((), ()))
    both = lax.dot_general(
        jnp.concatenate([left_high, left_low], axis=0),
        right_high,
        across,
        preferred_element_type=F32,
    )
    out[:, : total + PROJECT_LANES] = (
        both[:total]
        + both[total:]
        + lax.dot_general(left_high, right_low, across, preferred_element_type=F32)
    )
    trace_part = jnp.sum(jnp.sum(weighted * anomaly, axis=0, keepdims=True), axis=1, keepdims=True)
    out[:, TRACE_LANE:] = jnp.broadcast_to(trace_part, (total, LANES - TRACE_LANE))


def lane_gather(value, lanes):
    return jnp.take_along_axis(value, lanes, axis=1, mode="promise_in_bounds")


def sublane_total(value):
    for shift in (4, 2, 1):
        value = value + pltpu.roll(value, shift, axis=0)
    return value


def mix_kernel(halves, sum_count, *refs):
    sums, state_refs = refs[:sum_count], refs[sum_count:-4]
    out, staged, splats, sems = refs[-4:]
    local_members, elements, nodes = out.shape
    members = local_members * len(state_refs)
    tile = (8, LANES)
    sub = lax.broadcasted_iota(jnp.int32, tile, 0)
    lane = lax.broadcasted_iota(jnp.int32, tile, 1)
    left_lanes = [(lane // members) * members + (sub + 8 * g) for g in range(2)]
    right_lanes = sub * members + lane % members
    identity = [(lane // members + 8 * h == lane % members).astype(F32) for h in range(2)]

    def as_left(matrix):
        return [[lane_gather(matrix[h], left_lanes[g]) for g in range(2)] for h in range(2)]

    def as_right(matrix):
        return [lane_gather(matrix[g], right_lanes) for g in range(2)]

    def product(left, right):
        return [sublane_total(left[h][0] * right[0] + left[h][1] * right[1]) for h in range(2)]

    total_sum = sums[0][...]
    for ref in sums[1:]:
        total_sum = total_sum + ref[...]
    rows = [total_sum[8 * g : 8 * g + 8, :] for g in range(2)]
    project = [lane_gather(rows[g], jnp.full(tile, members, jnp.int32)) for g in range(2)]
    trace_value = lane_gather(rows[0], jnp.full(tile, TRACE_LANE, jnp.int32))
    scale = 1.0 / (trace_value + members * ((members - 1) / INFLATION))
    diagonal = (members - 1) / INFLATION
    unit_left = [[(lane // members + 8 * h == sub + 8 * g).astype(F32) for g in range(2)] for h in range(2)]
    unit_right = [(lane % members == sub + 8 * g).astype(F32) for g in range(2)]
    system_left = [
        [
            (lane_gather(rows[g], lane // members + 8 * h) + diagonal * unit_left[h][g]) * scale
            for g in range(2)
        ]
        for h in range(2)
    ]
    system_right = [
        (lane_gather(rows[g], lane % members) + diagonal * unit_right[g]) * scale for g in range(2)
    ]
    inverse_left = [
        [1.5 * unit_left[h][g] - 0.5 * system_left[h][g] for g in range(2)] for h in range(2)
    ]
    inverse_right = [1.5 * unit_right[g] - 0.5 * system_right[g] for g in range(2)]
    iterate = product(system_left, inverse_right)
    for sweep in range(1, NS_ITERS):
        step = product(inverse_left, as_right(iterate))
        middle = [1.5 * identity[h] - 0.5 * step[h] for h in range(2)]
        middle_left = as_left(middle)
        inverse_root = product(middle_left, inverse_right)
        if sweep + 1 < NS_ITERS:
            iterate = product(as_left(iterate), as_right(middle))
            inverse_left, inverse_right = as_left(inverse_root), as_right(inverse_root)
        else:
            solved = product(middle_left, as_right(product(inverse_left, project)))
            ones = [jnp.ones(tile, F32)] * 2
            row_sums = product(middle_left, as_right(product(inverse_left, ones)))
    solved, row_sums, inverse_right = as_right(solved), as_right(row_sums), as_right(inverse_root)
    mean_weights = product(as_left(inverse_root), solved)
    root_scale = jnp.sqrt((members - 1) * scale)
    weights_mean = sublane_total(row_sums[0] * solved[0] + row_sums[1] * solved[1])
    column_sum = sublane_total(inverse_right[0] + inverse_right[1])
    shift = (1.0 - column_sum * root_scale - weights_mean * scale) * (1.0 / members)
    mixing = [
        inverse_root[h] * root_scale + mean_weights[h] * scale + shift for h in range(2)
    ]
    odd = is_odd(halves)
    order = key_order(len(state_refs))
    own_place = odd * order.index(1) if halves else 0
    for k in range(local_members):
        lanes = sub * members + (k + local_members * own_place)
        for h in range(2):
            column = lane_gather(mixing[h], lanes)
            for i in range(8):
                splats[(8 * h + i) * local_members + k] = jnp.broadcast_to(column[i : i + 1, :], tile)
    places = []
    for piece in range(len(state_refs)):
        place = order.index(piece)
        places.append(place + odd * (order.index(piece ^ 1) - place) if halves else place)
    tall = 8 * (elements // 8 // sems.shape[0])

    def output_copy(block):
        place = pl.ds(tall * block, tall)
        return pltpu.make_async_copy(staged.at[:, place], out.at[:, place], sems.at[block])

    def mix_block(block, carry):
        span = pl.ds(pl.multiple_of(8 * block, 8), 8)
        for first in range(0, nodes, 2 * LANES):
            spans = [slice(first + LANES * u, first + LANES * (u + 1)) for u in range(2)]
            totals = [[None, None] for _ in range(local_members)]
            for j in range(members):
                piece, member = divmod(j, local_members)
                values = [state_refs[piece][member, span, lanes] for lanes in spans]
                for k in range(local_members):
                    factor = splats[(places[piece] * local_members + member) * local_members + k]
                    for u in range(2):
                        term = factor * values[u]
                        totals[k][u] = term if j == 0 else totals[k][u] + term
            for k in range(local_members):
                for u in range(2):
                    staged[k, span, spans[u]] = totals[k][u]
        return carry

    steps = tall // 8
    for part in range(sems.shape[0]):
        lax.fori_loop(part * steps, (part + 1) * steps, mix_block, 0)
        output_copy(part).start()
    for part in range(sems.shape[0]):
        output_copy(part).wait()


def has_halves(n_ens):
    return n_ens > 1 and n_ens & (n_ens - 1) == 0


def is_paired(n_dom, n_ens):
    return n_dom == 4 and has_halves(n_ens)


def key_order(n_ens):
    if not has_halves(n_ens):
        return list(range(n_ens))
    return list(range(0, n_ens, 2)) + list(range(1, n_ens, 2))


def spread(values, n_dom, n_ens, bits=(1, 3, 2), crossing=0):
    if not is_paired(n_dom, n_ens):
        return [values[0]] + [
            lax.ppermute(values[s], "dom", [(d, (d + s) % n_dom) for d in range(n_dom)])
            for s in range(1, n_dom)
        ]
    here, near, far = values
    near_pairs, far_pairs = [], []
    for d in range(n_dom):
        for e in range(n_ens):
            near_pairs.append((d * n_ens + e, (d ^ bits[e % 2]) * n_ens + e))
            far_pairs.append((d * n_ens + e, (d ^ bits[2]) * n_ens + (e ^ crossing)))
    near = lax.ppermute(near, ("dom", "ens"), near_pairs)
    far = lax.ppermute(far, ("dom", "ens"), far_pairs)
    other = lax.ppermute(near, "ens", [(e, e ^ 1) for e in range(n_ens)])
    return [here, near, far, other]


def gather_members(state, own, n_ens):
    pieces = {0: state}
    if not has_halves(n_ens):
        for shift in range(1, n_ens):
            pairs = [(e, (e + shift) % n_ens) for e in range(n_ens)]
            pieces[shift] = lax.ppermute(state, "ens", pairs)
        pieces[0] = own
        return pieces
    bit = n_ens >> 1
    while bit:
        pairs = [(e, e ^ bit) for e in range(n_ens)]
        for key in list(pieces):
            pieces[key ^ bit] = lax.ppermute(pieces[key], "ens", pairs)
        bit >>= 1
        if bit == 1:
            pieces[0] = own
    pieces[0] = own
    return pieces


def make_on_device(n_dom, n_ens):
    vmem = pl.BlockSpec(memory_space=pltpu.VMEM)
    hbm = pl.BlockSpec(memory_space=pltpu.HBM)
    direct = n_dom <= DIRECT_DOM
    paired = is_paired(n_dom, n_ens)
    halves = has_halves(n_ens)
    limit = VMEM_LIMIT if direct else None

    def call(kernel, out_shape, operands, specs=None, scratch=(), out_spec=vmem):
        many = isinstance(out_shape, (list, tuple))
        return pl.pallas_call(
            kernel,
            out_shape=out_shape,
            in_specs=specs or [vmem] * len(operands),
            out_specs=[out_spec] * len(out_shape) if many else out_spec,
            scratch_shapes=list(scratch),
            compiler_params=pltpu.CompilerParams(vmem_limit_bytes=limit),
        )(*operands)

    def in_hbm(value):
        return pltpu.with_memory_space_constraint(value, pltpu.HBM)

    def shape(dims, dtype=F32):
        return jax.ShapeDtypeStruct(dims, dtype)

    def on_device(state, coords, owner_local, counts, obs_value, obs_weight):
        local_members, _, nodes = state.shape
        slots = coords.shape[1]
        members = local_members * n_ens
        tile_shape = (8, 2 * CAP)
        inputs = [counts, coords, owner_local[None], obs_value[None], obs_weight[None]]
        tiles = call(
            lambda *refs: pack_kernel(direct, paired, *refs),
            [shape(tile_shape)] * (3 if paired else n_dom)
            if direct
            else [shape((n_dom,) + tile_shape)],
            [in_hbm(value) for value in inputs],
            [hbm] * len(inputs),
            [
                pltpu.SMEM(counts.shape, jnp.int32),
                pltpu.VMEM(coords.shape, F32),
                pltpu.VMEM((1, slots), jnp.int32),
                pltpu.VMEM((1, slots), F32),
                pltpu.VMEM((1, slots), F32),
                pltpu.VMEM((8, slots), F32),
                pltpu.SemaphoreType.DMA((5,)),
            ],
        )
        if direct:
            tiles = spread(tiles, n_dom, n_ens)
        else:
            moved = lax.all_to_all(tiles[0], "dom", split_axis=0, concat_axis=0, tiled=True)
            tiles = [moved[d] for d in range(n_dom)]
        own = call(
            fetch_kernel, shape(state.shape), [in_hbm(state)], [hbm], [pltpu.SemaphoreType.DMA(())]
        )
        pieces = gather_members(state, own, n_ens)
        sensor_count = CAP * (n_dom + n_dom % 2)
        order = key_order(n_ens)
        local = order[: n_ens // 2] if halves else order
        sensors, high, low, values = call(
            lambda *refs: values_kernel(paired, n_dom, *refs),
            [
                shape((8, sensor_count)),
                shape((nodes, sensor_count), BF16),
                shape((nodes, sensor_count), BF16),
                shape((local_members, sensor_count)),
            ],
            list(tiles) + [pieces[0]],
        )
        if len(local) > 1:
            values = call(
                reach_kernel,
                shape((len(local) * local_members, sensor_count)),
                [sensors, high, low, values] + [pieces[key] for key in local[1:]],
            )
        values = [values]
        if halves:
            pairs = [(e, e ^ 1) for e in range(n_ens)]
            values.append(lax.ppermute(values[0], "ens", pairs))
        partial_sum = call(
            lambda *refs: cross_kernel(halves, *refs), shape((members, LANES)), [sensors] + values
        )
        if direct:
            copies = [partial_sum] * (3 if paired else n_dom)
            sums = spread(copies, n_dom, n_ens, bits=(2, 3, 1), crossing=1)
        else:
            sums = [lax.psum(partial_sum, "dom")]
        return call(
            lambda *refs: mix_kernel(halves, len(sums), *refs),
            shape(state.shape),
            sums + [pieces[key] for key in range(n_ens)],
            None,
            [
                pltpu.VMEM(state.shape, F32),
                pltpu.VMEM((members * local_members, 8, 128), F32),
                pltpu.SemaphoreType.DMA((2,)),
            ],
            hbm,
        )

    return on_device


def solution(mesh):
    n_dom, n_ens = mesh.shape["dom"], mesh.shape["ens"]
    return jax.shard_map(
        make_on_device(n_dom, n_ens),
        mesh=mesh,
        in_specs=(
            P("ens", ("groups", "dom"), None),
            P(None, ("groups", "dom")),
            P(("groups", "dom")),
            P(("groups", "dom"), None),
            P(("groups", "dom")),
            P(("groups", "dom")),
        ),
        out_specs=P("ens", ("groups", "dom"), None),
        check_vma=False,
    )
```
